8 devices in a mesh: replica: 2 (over z, y), model: 4 (over x, core).
Axes of the slice: x: 2, y: 2, z: 1, core: 2. Of those that a mesh axis runs over, the one named last changes fastest.
Arguments:
- prompt: bfloat16 [128, 128, 3072], P('replica', 'model'), parts along dimension 0
- lengths: int32 [128], P('replica'), parts along dimension 0
- new_tok: bfloat16 [128, 3072], P('replica'), parts along dimension 0
- norm_attn: bfloat16 [1, 3072], replicated
- w_q: bfloat16 [1, 3072, 3072], P(None, None, 'model')
- w_k: bfloat16 [1, 3072, 1024], P(None, None, 'model')
- w_v: bfloat16 [1, 3072, 1024], P(None, None, 'model')
- w_o: bfloat16 [1, 3072, 3072], P(None, 'model')
- norm_mlp: bfloat16 [1, 3072], replicated
- w_gate: bfloat16 [1, 3072, 8192], P(None, None, 'model')
- w_up: bfloat16 [1, 3072, 8192], P(None, None, 'model')
- w_down: bfloat16 [1, 8192, 3072], P(None, 'model')
Outputs:
- output 1: bfloat16 [128, 3072], P('replica'), parts along dimension 0
- output 2: bfloat16 [128, 3072], P('replica'), parts along dimension 0
- output 3: bfloat16 [1, 128, 129, 8, 128], P(None, 'replica', None, 'model'), parts along dimension 1
- output 4: bfloat16 [1, 128, 129, 8, 128], P(None, 'replica', None, 'model'), parts along dimension 1
There are 2 independent parts. The reference program is written for one: setup_inputs(seed, part) draws one part's arguments, and reference() takes and returns one part's arrays. A program takes and returns all parts, laid end to end along the dimension named above; an argument that names none is the same for every part.
All inputs are finite; a program needn't handle non-finite values.
Results may differ from the reference program's by a relative error of at most 0.0108268.
Values are sent between devices in bfloat16 or wider.
A program may use at most 1 GiB of HBM per device.

```python
import jax
import jax.numpy as jnp
from jax import lax

BATCH_SIZE = 64
SEQ_LEN = 128
Q_BLOCK = 32
D_MODEL = 3072
NUM_HEADS = 24
KV_HEADS = 8
HEAD_DIM = 128
FF_DIM = 8192
N_LAYERS = 1

Q_WIDTH = NUM_HEADS * HEAD_DIM
KV_WIDTH = KV_HEADS * HEAD_DIM
GROUP_SIZE = NUM_HEADS // KV_HEADS
N_QBLOCKS = SEQ_LEN // Q_BLOCK
N_TOKENS = BATCH_SIZE * SEQ_LEN


def setup_inputs(seed: int = 0, part: int = 0) -> dict:
    part_keys = jax.random.split(jax.random.fold_in(jax.random.key(seed), part), 4)
    shared_keys = jax.random.split(jax.random.key(seed + 1), 9)
    qk_scale = (2.0 / D_MODEL) ** 0.5
    in_scale = D_MODEL ** -0.5

    def normal_bf16(rng_key, dims, scale_val):
        return (jax.random.normal(rng_key, dims, jnp.float32) * scale_val).astype(jnp.bfloat16)

    def gain_bf16(rng_key):
        return jax.random.uniform(rng_key, (N_LAYERS, D_MODEL), jnp.float32, 0.6, 1.4).astype(jnp.bfloat16)

    lengths = jax.random.randint(part_keys[1], (BATCH_SIZE,), SEQ_LEN // 2 + 1, SEQ_LEN + 1)
    full_row = jax.random.randint(part_keys[2], (), 0, BATCH_SIZE)
    lengths = jnp.where(jnp.arange(BATCH_SIZE) == full_row, SEQ_LEN, lengths).astype(jnp.int32)
    return {
        'prompt': normal_bf16(part_keys[0], (BATCH_SIZE, SEQ_LEN, D_MODEL), 1.0),
        'lengths': lengths,
        'new_tok': normal_bf16(part_keys[3], (BATCH_SIZE, D_MODEL), 1.0),
        'norm_attn': gain_bf16(shared_keys[0]),
        'w_q': normal_bf16(shared_keys[1], (N_LAYERS, D_MODEL, Q_WIDTH), qk_scale),
        'w_k': normal_bf16(shared_keys[2], (N_LAYERS, D_MODEL, KV_WIDTH), qk_scale),
        'w_v': normal_bf16(shared_keys[3], (N_LAYERS, D_MODEL, KV_WIDTH), in_scale),
        'w_o': normal_bf16(shared_keys[4], (N_LAYERS, Q_WIDTH, D_MODEL), Q_WIDTH ** -0.5),
        'norm_mlp': gain_bf16(shared_keys[5]),
        'w_gate': normal_bf16(shared_keys[6], (N_LAYERS, D_MODEL, FF_DIM), in_scale),
        'w_up': normal_bf16(shared_keys[7], (N_LAYERS, D_MODEL, FF_DIM), in_scale),
        'w_down': normal_bf16(shared_keys[8], (N_LAYERS, FF_DIM, D_MODEL), FF_DIM ** -0.5),
    }


def rms_norm(hidden, gain_vec):
    hid_f32 = hidden.astype(jnp.float32)
    inv_rms = lax.rsqrt(jnp.mean(hid_f32 * hid_f32, axis=-1, keepdims=True) + 1e-5)
    return (hid_f32 * inv_rms * gain_vec.astype(jnp.float32)).astype(jnp.bfloat16)


def rotary(heads_f32, positions):
    half_dim = HEAD_DIM // 2
    inv_freq = 10000.0 ** (-2.0 * jnp.arange(half_dim, dtype=jnp.float32) / HEAD_DIM)
    angles = positions.astype(jnp.float32)[..., None] * inv_freq
    cos_tab = jnp.cos(angles)[..., None, :]
    sin_tab = jnp.sin(angles)[..., None, :]
    lo_half = heads_f32[..., :half_dim]
    hi_half = heads_f32[..., half_dim:]
    return jnp.concatenate([lo_half * cos_tab - hi_half * sin_tab, hi_half * cos_tab + lo_half * sin_tab], axis=-1)


def prefill_attention(queries, key_rot, val_proj, lengths):
    q_blocks = jnp.moveaxis(queries.astype(jnp.float32).reshape(BATCH_SIZE, N_QBLOCKS, Q_BLOCK, KV_HEADS, GROUP_SIZE, HEAD_DIM), 1, 0)
    key_f32 = key_rot.astype(jnp.float32)
    val_f32 = val_proj.astype(jnp.float32)
    key_pos = jnp.arange(SEQ_LEN)
    key_valid = key_pos[None, :] < lengths[:, None]

    def one_block(block_args):
        q_blk, blk_idx = block_args
        q_pos = blk_idx * Q_BLOCK + jnp.arange(Q_BLOCK)
        scores = jnp.einsum('bqhgd,bkhd->bqhgk', q_blk, key_f32) * (HEAD_DIM ** -0.5)
        visible = (key_pos[None, None, :] <= q_pos[None, :, None]) & key_valid[:, None, :]
        scores = jnp.where(visible[:, :, None, None, :], scores, -1e30)
        attn_prob = jax.nn.softmax(scores, axis=-1)
        return jnp.einsum('bqhgk,bkhd->bqhgd', attn_prob, val_f32)

    blocks_out = lax.map(one_block, (q_blocks, jnp.arange(N_QBLOCKS)))
    return jnp.moveaxis(blocks_out, 0, 1).reshape(BATCH_SIZE, SEQ_LEN, Q_WIDTH).astype(jnp.bfloat16)


def decode_attention(q_new, key_cache, value_cache, lengths):
    q_f32 = q_new.astype(jnp.float32).reshape(BATCH_SIZE, KV_HEADS, GROUP_SIZE, HEAD_DIM)
    scores = jnp.einsum('bhgd,bkhd->bhgk', q_f32, key_cache.astype(jnp.float32)) * (HEAD_DIM ** -0.5)
    cache_pos = jnp.arange(SEQ_LEN + 1)
    visible = (cache_pos[None, :] < lengths[:, None]) | (cache_pos[None, :] == SEQ_LEN)
    scores = jnp.where(visible[:, None, None, :], scores, -1e30)
    attn_prob = jax.nn.softmax(scores, axis=-1)
    out_f32 = jnp.einsum('bhgk,bkhd->bhgd', attn_prob, value_cache.astype(jnp.float32))
    return out_f32.reshape(BATCH_SIZE, Q_WIDTH).astype(jnp.bfloat16)


def reference(prompt, lengths, new_tok, norm_attn, w_q, w_k, w_v, w_o, norm_mlp, w_gate, w_up, w_down):
    seq_pos = jnp.arange(SEQ_LEN)

    def layer_step(loop_state, layer_w):
        hidden, dec_hidden = loop_state
        g_attn, wq_l, wk_l, wv_l, wo_l, g_mlp, wg_l, wu_l, wd_l = layer_w
        normed = rms_norm(hidden, g_attn).reshape(N_TOKENS, D_MODEL)
        q_rot = rotary(jnp.dot(normed, wq_l, preferred_element_type=jnp.float32).reshape(BATCH_SIZE, SEQ_LEN, NUM_HEADS, HEAD_DIM), seq_pos).astype(jnp.bfloat16)
        k_rot = rotary(jnp.dot(normed, wk_l, preferred_element_type=jnp.float32).reshape(BATCH_SIZE, SEQ_LEN, KV_HEADS, HEAD_DIM), seq_pos).astype(jnp.bfloat16)
        v_proj = jnp.dot(normed, wv_l, preferred_element_type=jnp.float32).astype(jnp.bfloat16).reshape(BATCH_SIZE, SEQ_LEN, KV_HEADS, HEAD_DIM)
        attn_out = prefill_attention(q_rot, k_rot, v_proj, lengths).reshape(N_TOKENS, Q_WIDTH)
        hidden = (hidden.astype(jnp.float32) + jnp.dot(attn_out, wo_l, preferred_element_type=jnp.float32).reshape(BATCH_SIZE, SEQ_LEN, D_MODEL)).astype(jnp.bfloat16)
        normed = rms_norm(hidden, g_mlp).reshape(N_TOKENS, D_MODEL)
        mlp_mid = (jax.nn.silu(jnp.dot(normed, wg_l, preferred_element_type=jnp.float32)) * jnp.dot(normed, wu_l, preferred_element_type=jnp.float32)).astype(jnp.bfloat16)
        hidden = (hidden.astype(jnp.float32) + jnp.dot(mlp_mid, wd_l, preferred_element_type=jnp.float32).reshape(BATCH_SIZE, SEQ_LEN, D_MODEL)).astype(jnp.bfloat16)

        tok_norm = rms_norm(dec_hidden, g_attn)
        q_new = rotary(jnp.dot(tok_norm, wq_l, preferred_element_type=jnp.float32).reshape(BATCH_SIZE, NUM_HEADS, HEAD_DIM), lengths).astype(jnp.bfloat16)
        k_new = rotary(jnp.dot(tok_norm, wk_l, preferred_element_type=jnp.float32).reshape(BATCH_SIZE, KV_HEADS, HEAD_DIM), lengths).astype(jnp.bfloat16)
        v_new = jnp.dot(tok_norm, wv_l, preferred_element_type=jnp.float32).astype(jnp.bfloat16).reshape(BATCH_SIZE, KV_HEADS, HEAD_DIM)
        key_cache = jnp.concatenate([k_rot, k_new[:, None]], axis=1)
        value_cache = jnp.concatenate([v_proj, v_new[:, None]], axis=1)
        tok_attn = decode_attention(q_new, key_cache, value_cache, lengths)
        dec_hidden = (dec_hidden.astype(jnp.float32) + jnp.dot(tok_attn, wo_l, preferred_element_type=jnp.float32)).astype(jnp.bfloat16)
        tok_norm = rms_norm(dec_hidden, g_mlp)
        tok_mid = (jax.nn.silu(jnp.dot(tok_norm, wg_l, preferred_element_type=jnp.float32)) * jnp.dot(tok_norm, wu_l, preferred_element_type=jnp.float32)).astype(jnp.bfloat16)
        dec_hidden = (dec_hidden.astype(jnp.float32) + jnp.dot(tok_mid, wd_l, preferred_element_type=jnp.float32)).astype(jnp.bfloat16)
        return (hidden, dec_hidden), (key_cache, value_cache)

    (hidden, dec_hidden), (key_cache, value_cache) = lax.scan(layer_step, (prompt, new_tok), (norm_attn, w_q, w_k, w_v, w_o, norm_mlp, w_gate, w_up, w_down))
    last_sel = seq_pos[None, :] == (lengths - 1)[:, None]
    last_hidden = jnp.sum(jnp.where(last_sel[:, :, None], hidden.astype(jnp.float32), 0.0), axis=1).astype(jnp.bfloat16)
    return dec_hidden, last_hidden, key_cache, value_cache
```

```python
import jax
import jax.numpy as jnp
from jax import lax
from jax.sharding import PartitionSpec as P

HEAD_DIM = 128
NEG_BIG = -1e30


def rms_norm(hidden, gain_vec):
    hid_f32 = hidden.astype(jnp.float32)
    inv_rms = lax.rsqrt(jnp.mean(hid_f32 * hid_f32, axis=-1, keepdims=True) + 1e-5)
    return (hid_f32 * inv_rms * gain_vec.astype(jnp.float32)).astype(jnp.bfloat16)


def rotary(heads_f32, positions):
    half_dim = HEAD_DIM // 2
    inv_freq = 10000.0 ** (-2.0 * jnp.arange(half_dim, dtype=jnp.float32) / HEAD_DIM)
    angles = positions.astype(jnp.float32)[..., None] * inv_freq
    cos_tab = jnp.cos(angles)[..., None, :]
    sin_tab = jnp.sin(angles)[..., None, :]
    lo_half = heads_f32[..., :half_dim]
    hi_half = heads_f32[..., half_dim:]
    return jnp.concatenate([lo_half * cos_tab - hi_half * sin_tab, hi_half * cos_tab + lo_half * sin_tab], axis=-1)


def dot32(lhs, rhs):
    return jnp.dot(lhs, rhs, preferred_element_type=jnp.float32)


def solution(mesh):
    n_dev = mesh.shape['model']
    seq_spec = P('replica', 'model', None)
    col_spec = P(None, None, 'model')
    row_spec = P(None, 'model', None)
    gain_spec = P(None, None)
    tok_spec = P('replica', None)
    cache_spec = P(None, 'replica', None, 'model', None)
    in_specs = (seq_spec, P('replica'), tok_spec, gain_spec, col_spec, col_spec, col_spec, row_spec, gain_spec, col_spec, col_spec, row_spec)
    out_specs = (tok_spec, tok_spec, cache_spec, cache_spec)

    def per_device(prompt, lengths, new_tok, norm_attn, w_q, w_k, w_v, w_o, norm_mlp, w_gate, w_up, w_down):
        my_idx = lax.axis_index('model')
        n_batch, seq_loc, d_model = prompt.shape
        n_tok = n_batch * seq_loc
        kv_loc = w_k.shape[2] // HEAD_DIM
        q_loc = w_q.shape[2] // HEAD_DIM
        seq_len = seq_loc * n_dev
        seq_pos = my_idx * seq_loc + jnp.arange(seq_loc)
        w_kv = jnp.stack([w_k[0], w_v[0]])
        w_kv = lax.all_gather(w_kv, 'model', axis=0)
        normed = rms_norm(prompt, norm_attn[0]).reshape(n_tok, d_model)
        kv = jnp.einsum('td,nsdf->tnsf', normed, w_kv, preferred_element_type=jnp.float32)
        kv = kv.reshape(n_batch, seq_loc, n_dev, 2, kv_loc, HEAD_DIM)
        k_rot = rotary(kv[:, :, :, 0].reshape(n_batch, seq_loc, n_dev * kv_loc, HEAD_DIM), seq_pos).astype(jnp.bfloat16)
        k_rot = k_rot.reshape(n_batch, seq_loc, n_dev, kv_loc, HEAD_DIM)
        v_proj = kv[:, :, :, 1].astype(jnp.bfloat16)
        key_mine = lax.all_to_all(k_rot, 'model', 2, 1).reshape(n_batch, seq_len, kv_loc, HEAD_DIM)
        val_mine = lax.all_to_all(v_proj, 'model', 2, 1).reshape(n_batch, seq_len, kv_loc, HEAD_DIM)
        loc = lengths - 1 - my_idx * seq_loc
        rows = jnp.take_along_axis(prompt, jnp.clip(loc, 0, seq_loc - 1)[:, None, None], axis=1)[:, 0]
        rows = jnp.where(((loc >= 0) & (loc < seq_loc))[:, None], rows, 0).astype(jnp.float32)
        rows = lax.psum(rows, 'model').astype(jnp.bfloat16)
        hid = jnp.concatenate([rows, new_tok], axis=0)
        pos = jnp.concatenate([lengths - 1, lengths])
        n1 = rms_norm(hid, norm_attn[0])
        q = rotary(dot32(n1, w_q[0]).reshape(2 * n_batch, q_loc, HEAD_DIM), pos).astype(jnp.bfloat16)
        n_tok1 = n1[n_batch:]
        k_new = rotary(dot32(n_tok1, w_k[0]).reshape(n_batch, kv_loc, HEAD_DIM), lengths).astype(jnp.bfloat16)
        v_new = dot32(n_tok1, w_v[0]).astype(jnp.bfloat16).reshape(n_batch, kv_loc, HEAD_DIM)
        key_cache = jnp.concatenate([key_mine, k_new[:, None]], axis=1)
        val_cache = jnp.concatenate([val_mine, v_new[:, None]], axis=1)
        group = q_loc // kv_loc
        qg = q.reshape(2, n_batch, kv_loc, group, HEAD_DIM)
        scores = jnp.einsum('sbhgd,bkhd->bhsgk', qg, key_cache, preferred_element_type=jnp.float32) * (HEAD_DIM ** -0.5)
        cpos = jnp.arange(seq_len + 1)
        vis = cpos[None, :] < lengths[:, None]
        vis = jnp.stack([vis, vis | (cpos == seq_len)[None, :]], axis=1)
        scores = jnp.where(vis[:, None, :, None, :], scores, NEG_BIG)
        prob = jax.nn.softmax(scores, axis=-1).astype(jnp.bfloat16)
        att = jnp.einsum('bhsgk,bkhd->sbhgd', prob, val_cache, preferred_element_type=jnp.float32)
        att = att.reshape(2 * n_batch, q_loc * HEAD_DIM).astype(jnp.bfloat16)
        hid = (hid.astype(jnp.float32) + lax.psum(dot32(att, w_o[0]), 'model')).astype(jnp.bfloat16)
        n2 = rms_norm(hid, norm_mlp[0])
        mid = (jax.nn.silu(dot32(n2, w_gate[0])) * dot32(n2, w_up[0])).astype(jnp.bfloat16)
        hid = (hid.astype(jnp.float32) + lax.psum(dot32(mid, w_down[0]), 'model')).astype(jnp.bfloat16)
        return hid[n_batch:], hid[:n_batch], key_cache[None], val_cache[None]

    return jax.shard_map(per_device, mesh=mesh, in_specs=in_specs, out_specs=out_specs, check_vma=False)
```

```python
import functools

import jax
import jax.numpy as jnp
from jax import lax
from jax.experimental import pallas as pl
from jax.experimental.pallas import tpu as pltpu
from jax.sharding import PartitionSpec as P

HEAD_DIM = 128
NEG_BIG = -1e30
MESH = pl.DeviceIdType.MESH
F32 = jnp.float32
BF16 = jnp.bfloat16

NB = 64
SEQ_LOC = 32
D = 3072
FF = 2048
QW = 768
CH = 16
NCH = NB // CH
ROWS = CH * SEQ_LOC
WCH = 4
WROWS = D // WCH


def dot32(lhs, rhs):
    return jnp.dot(lhs, rhs, preferred_element_type=F32)


def rotate_tables(positions):
    half = HEAD_DIM // 2
    inv_freq = 10000.0 ** (-2.0 * jnp.arange(half, dtype=F32) / HEAD_DIM)
    angles = positions.astype(F32)[:, None] * inv_freq
    cos_tab, sin_tab = jnp.cos(angles), jnp.sin(angles)
    return jnp.concatenate([cos_tab, cos_tab], 1), jnp.concatenate([-sin_tab, sin_tab], 1)


def kernel(lens, tab_c, tab_s, rot_c, rot_s, g_attn, g_mlp, new_tok,
           prompt, w_q, w_k, w_v, w_o, w_g, w_u, w_d,
           o_hid, o_kv, o_new,
           buf_a, buf_b, buf_c, kv, stage, flat, q_buf, k_buf, v_buf, a_buf, att,
           sel_r1, sel_r2, hid, normed, part, r1, r2, n2, mid, hid2, out_buf, knv,
           ld_p, ld_w, ld_big, st_sem,
           wp_s, wp_r, wx_s, wx_r, wfx_s, wfx_r, wy_s, wy_r, wfy_s, wfy_r,
           sel_s, sel_r, kv_s, kv_r, ar_s, ar_r):
    y = lax.axis_index("replica")
    m = lax.axis_index("model")
    c = lax.rem(m, 2)
    x = m // 2
    xs_m = lax.rem(m + 2, 4)
    xo_m = 3 - m
    pt_m = m + 1 - 2 * c
    xs, xo, pt, yp = (y, xs_m), (y, xo_m), (y, pt_m), (1 - y, m)

    def remote(src, dst, ssem, rsem, dev):
        return pltpu.make_async_remote_copy(src_ref=src, dst_ref=dst, send_sem=ssem, recv_sem=rsem,
                                            device_id=dev, device_id_type=MESH)

    def load_w(i):
        src = (w_k, w_v)[i]
        return pltpu.make_async_copy(src, buf_b.at[:, pl.ds(pl.multiple_of(m * 512 + i * 256, 256), 256)], ld_w.at[i])

    def load_p(j):
        r = pl.ds(pl.multiple_of(j * ROWS, ROWS), ROWS)
        return pltpu.make_async_copy(prompt.at[r], buf_a.at[r], ld_p.at[j])

    for i in range(2):
        load_w(i).start()
    for j in range(NCH):
        load_p(j).start()
    load_q = pltpu.make_async_copy(w_q, buf_c.at[:, pl.ds(0, QW)], ld_big.at[0])
    load_q.start()

    def load_o(i):
        return pltpu.make_async_copy(w_o.at[:, pl.ds(i * QW, QW)], buf_c.at[pl.ds(i * QW, QW), pl.ds(QW, QW)], ld_big.at[1 + i])

    for i in range(4):
        load_o(i).start()
    load_g = pltpu.make_async_copy(w_g, buf_b, ld_big.at[5])
    load_u = pltpu.make_async_copy(w_u, buf_c, ld_big.at[6])
    load_d = pltpu.make_async_copy(w_d, buf_a, ld_big.at[7])

    barrier = pltpu.get_barrier_semaphore()
    for dev in (xs, xo, pt, yp):
        pl.semaphore_signal(barrier, inc=1, device_id=dev, device_id_type=MESH)
    pl.semaphore_wait(barrier, 4)

    def w_ref(owner, h, r):
        return buf_b.at[pl.ds(r * WROWS, WROWS), pl.ds(pl.multiple_of(owner * 512 + h * 256, 256), 256)]

    def wx(r):
        ref = w_ref(m, y, r)
        return remote(ref, ref, wx_s.at[r], wx_r.at[r], xs)

    def wfx(r):
        ref = w_ref(xs_m, y, r)
        return remote(ref, ref, wfx_s.at[r], wfx_r.at[r], pt)

    def wy(r):
        ref = w_ref(xs_m, y, r)
        return remote(ref, ref, wy_s.at[r], wy_r.at[r], yp)

    def wfy(r):
        ref = w_ref(xs_m, 1 - y, r)
        return remote(ref, ref, wfy_s.at[r], wfy_r.at[r], pt)

    own = buf_b.at[:, pl.ds(pl.multiple_of(m * 512, 512), 512)]
    wp = remote(own, own, wp_s, wp_r, pt)
    for i in range(2):
        load_w(i).wait()
    for r in range(WCH):
        wx(r).start()
    wp.start()

    def forward_x(r):
        wx(r).wait_recv()
        wfx(r).start()
        wy(r).start()

    def forward_y(r):
        wy(r).wait_recv()
        wfy(r).start()

    gain_a = g_attn[...].astype(F32)
    row_iota = lax.broadcasted_iota(jnp.int32, (SEQ_LOC, 1), 0)

    def norm_prompts(i, carry):
        parts = []
        for t in range(8):
            b = i * 8 + t
            rows = pl.ds(pl.multiple_of(b * SEQ_LOC, SEQ_LOC), SEQ_LOC)
            v = buf_a[rows, :].astype(F32)
            inv = lax.rsqrt(jnp.mean(v * v, axis=-1, keepdims=True) + 1e-5)
            hit = row_iota == lens[b] - 1 - m * SEQ_LOC
            parts.append(jnp.sum(jnp.where(hit, v, 0.0), axis=0, keepdims=True))
            buf_a[rows, :] = (buf_a[rows, :].astype(F32) * inv * gain_a).astype(BF16)
        part[pl.ds(pl.multiple_of(i * 8, 8), 8), :] = jnp.concatenate(parts, axis=0)
        return carry

    per = CH // 8
    for j in range(NCH):
        load_p(j).wait()
        lax.fori_loop(j * per, (j + 1) * per, norm_prompts, 0)

    sel_b = normed.at[pl.ds(0, NB)]
    sel_b[...] = part[0:NB, :].astype(BF16)
    s1 = remote(sel_b, sel_r1, sel_s.at[0], sel_r.at[0], pt)
    s1.start()

    def unit_chunk(owner, h, j):
        col = pl.ds(pl.multiple_of(owner * 512 + h * 256, 256), 256)
        acc = dot32(buf_a[pl.ds(pl.multiple_of(j * ROWS, ROWS), ROWS), :], buf_b[:, col])
        ct, st = tab_c[h], tab_s[h]
        for hd in range(2):
            a = acc[:, hd * HEAD_DIM:(hd + 1) * HEAD_DIM]
            turned = pltpu.roll(a, HEAD_DIM // 2, 1)
            res = a.reshape(CH, SEQ_LOC, HEAD_DIM) * ct[None] + turned.reshape(CH, SEQ_LOC, HEAD_DIM) * st[None]
            flat[pl.ds(hd, ROWS, stride=2), :] = res.reshape(ROWS, HEAD_DIM)
        return flat[...].astype(BF16).reshape(CH, 2 * SEQ_LOC, HEAD_DIM)

    def kv_ref(h, j):
        return kv.at[h, pl.ds(pl.multiple_of(j * CH, CH), CH), pl.ds(pl.multiple_of(m * 64, 64), 64)]

    def kv_send(kind, turn, j):
        dev = (pt, xs, xo)[kind]
        h = y if turn == 0 else 1 - y
        return remote(stage.at[kind, turn, j], kv_ref(h, j), kv_s.at[kind, turn, j], kv_r.at[kind, turn, j], dev)

    def run_unit(kind, turn, j):
        owner = (pt_m, xs_m, xo_m)[kind]
        h = y if turn == 0 else 1 - y
        stage[kind, turn, j] = unit_chunk(owner, h, j)
        kv_send(kind, turn, j).start()

    forward_x(0)

    def own_units(i, carry):
        h, j = i // NCH, lax.rem(i, NCH)
        kv[h, pl.ds(pl.multiple_of(j * CH, CH), CH), pl.ds(pl.multiple_of(m * 64, 64), 64)] = unit_chunk(m, h, j)
        return carry

    lax.fori_loop(0, 2 * NCH, own_units, 0)
    forward_x(1)

    s1.wait()
    sel_b[...] = (sel_b[...].astype(F32) + sel_r1[...].astype(F32)).astype(BF16)
    half = pl.ds(pl.multiple_of(c * 32, 32), 32)
    s2 = remote(normed.at[half], sel_r2, sel_s.at[1], sel_r.at[1], xs)
    s2.start()

    wp.wait_recv()

    def loop_unit(kind, turn):
        def body(j, carry):
            run_unit(kind, turn, j)
            return carry
        lax.fori_loop(0, NCH, body, 0)

    loop_unit(0, 0)
    forward_x(2)
    forward_y(0)
    loop_unit(0, 1)
    forward_x(3)
    loop_unit(1, 0)
    forward_y(1)
    for r in range(WCH):
        wfx(r).wait_recv()
    loop_unit(2, 0)
    forward_y(2)

    s2.wait()
    hid[half, :] = (normed[half, :].astype(F32) + sel_r2[...].astype(F32)).astype(BF16)
    s3 = remote(hid.at[half], hid.at[half], sel_s.at[2], sel_r.at[2], pt)
    s3.start()
    hid[pl.ds(NB, NB), :] = new_tok[...]
    forward_y(3)
    for r in range(WCH):
        wfy(r).wait_recv()

    def last_units(j, carry):
        run_unit(1, 1, j)
        run_unit(2, 1, j)
        return carry

    lax.fori_loop(0, NCH, last_units, 0)
    s3.wait()

    def norm_rows(src, gain):
        v = src.astype(F32)
        inv = lax.rsqrt(jnp.mean(v * v, axis=-1, keepdims=True) + 1e-5)
        return (v * inv * gain).astype(BF16)

    def norm_hid(i, carry):
        rows = pl.ds(pl.multiple_of(i * 32, 32), 32)
        normed[rows, :] = norm_rows(hid[rows, :], gain_a)
        return carry

    lax.fori_loop(0, 4, norm_hid, 0)
    load_q.wait()
    q_buf[...] = jnp.zeros_like(q_buf)
    k_buf[...] = jnp.zeros_like(k_buf)
    v_buf[...] = jnp.zeros_like(v_buf)

    def turn(a, ct, st):
        return (a * ct + pltpu.roll(a, HEAD_DIM // 2, 1) * st).astype(BF16).astype(F32)

    for pair in range(3):
        qs = dot32(normed[...], buf_c[:, pair * 256:(pair + 1) * 256])
        for i in range(2):
            hd = pair * 2 + i
            rot = turn(qs[:, i * HEAD_DIM:(i + 1) * HEAD_DIM], rot_c[...], rot_s[...])
            for t in range(2):
                q_buf[pl.ds(t * 8 + hd, NB, stride=16), :] = rot[t * NB:(t + 1) * NB]
    toks = normed[NB:2 * NB, :]
    k_new = dot32(toks, buf_b[:, pl.ds(pl.multiple_of(m * 512, 256), 256)])
    v_new = dot32(toks, buf_b[:, pl.ds(pl.multiple_of(m * 512 + 256, 256), 256)])
    for g in range(2):
        cols = slice(g * HEAD_DIM, (g + 1) * HEAD_DIM)
        k_g = turn(k_new[:, cols], rot_c[NB:, :], rot_s[NB:, :])
        v_g = v_new[:, cols].astype(BF16).astype(F32)
        flat[pl.ds(g, NB, stride=2), :] = k_g
        flat[pl.ds(2 * NB + g, NB, stride=2), :] = v_g
        for i in range(3):
            rows = pl.ds(8 + 3 * g + i, NB, stride=16)
            k_buf[rows, :] = k_g
            v_buf[rows, :] = v_g
    knv[0] = flat[0:2 * NB, :].astype(BF16)
    knv[1] = flat[2 * NB:4 * NB, :].astype(BF16)
    st_new = pltpu.make_async_copy(knv, o_new, st_sem.at[NCH])
    st_new.start()

    wp.wait_send()
    for r in range(WCH):
        wx(r).wait_send()
        wfx(r).wait_send()
        wy(r).wait_send()
        wfy(r).wait_send()
    load_g.start()
    load_d.start()

    r_io = lax.broadcasted_iota(jnp.int32, (16, 256), 0)
    c_io = lax.broadcasted_iota(jnp.int32, (16, 256), 1)
    same = ((r_io & 7) >= 3) == ((c_io & 1) == 1)
    k_pos = c_io >> 1
    is_new = lax.broadcasted_iota(jnp.int32, (16, 1), 0) >= 8
    scale = HEAD_DIM ** -0.5

    def attend(b):
        rows = pl.ds(pl.multiple_of(b * 16, 16), 16)
        q = q_buf[rows, :]
        s = lax.dot_general(q.astype(BF16), kv[0, b], (((1,), (1,)), ((), ())), preferred_element_type=F32) * scale
        s = jnp.where(same & (k_pos < lens[b]), s, NEG_BIG)
        s_new = jnp.where(is_new, jnp.sum(q * k_buf[rows, :], axis=-1, keepdims=True) * scale, NEG_BIG)
        top = jnp.maximum(jnp.max(s, axis=-1, keepdims=True), s_new)
        p = jnp.exp(s - top)
        p_new = jnp.exp(s_new - top)
        total = jnp.sum(p, axis=-1, keepdims=True) + p_new
        acc = dot32(p.astype(BF16), kv[1, b]) + p_new * v_buf[rows, :]
        a_buf[rows, :] = acc / total

    def attend_four(i, carry):
        for t in range(4):
            attend(i * 4 + t)
        return carry

    def store_kv(j):
        r = pl.ds(j * CH, CH)
        return pltpu.make_async_copy(kv.at[:, r], o_kv.at[:, r], st_sem.at[j])

    for j in range(NCH):
        for kind in range(3):
            for tn in range(2):
                kv_send(kind, tn, j).wait_recv()
        store_kv(j).start()
        lax.fori_loop(j * (CH // 4), (j + 1) * (CH // 4), attend_four, 0)

    for hd in range(6):
        for t in range(2):
            att[t * NB:(t + 1) * NB, hd * HEAD_DIM:(hd + 1) * HEAD_DIM] = a_buf[pl.ds(t * 8 + hd, NB, stride=16), :].astype(BF16)
    for i in range(4):
        load_o(i).wait()
        part[:, i * QW:(i + 1) * QW] = dot32(att[...], buf_c[i * QW:(i + 1) * QW, QW:2 * QW])

    my_half = pl.ds(pl.multiple_of(c * 64, 64), 64)
    ot_half = pl.ds(pl.multiple_of((1 - c) * 64, 64), 64)
    mine = pl.ds(pl.multiple_of(c * 64 + x * 32, 32), 32)
    away = pl.ds(pl.multiple_of(c * 64 + (1 - x) * 32, 32), 32)

    def reduce_rows(k):
        a1 = remote(part.at[ot_half], r1, ar_s.at[k, 0], ar_r.at[k, 0], pt)
        a1.start()
        if k == 0:
            load_u.start()
        a1.wait_recv()
        x_half = pl.ds(pl.multiple_of((1 - x) * 32, 32), 32)
        part[away, :] = part[away, :] + r1[x_half, :]
        a2 = remote(part.at[away], r2, ar_s.at[k, 1], ar_r.at[k, 1], xs)
        a2.start()
        m_half = pl.ds(pl.multiple_of(x * 32, 32), 32)
        part[mine, :] = part[mine, :] + r1[m_half, :]
        a2.wait_recv()
        a1.wait_send()
        a2.wait_send()
        return part[mine, :] + r2[...]

    def gather_rows(k, buf):
        a3 = remote(buf.at[mine], buf.at[mine], ar_s.at[k, 2], ar_r.at[k, 2], xs)
        a3.start()
        a4 = remote(buf.at[mine], buf.at[mine], ar_s.at[k, 3], ar_r.at[k, 3], pt)
        a4.start()
        a3.wait_recv()
        a5 = remote(buf.at[away], buf.at[away], ar_s.at[k, 4], ar_r.at[k, 4], pt)
        a5.start()
        a4.wait_recv()
        a5.wait_recv()
        a3.wait_send()
        a4.wait_send()
        a5.wait_send()

    hid2[...] = (hid[mine, :].astype(F32) + reduce_rows(0)).astype(BF16)
    n2[mine, :] = norm_rows(hid2[...], g_mlp[...].astype(F32))
    gather_rows(0, n2)

    load_g.wait()
    load_u.wait()

    def mlp_cols(i, carry):
        cols = pl.ds(pl.multiple_of(i * 256, 256), 256)
        gate = dot32(n2[...], buf_b[:, cols])
        up = dot32(n2[...], buf_c[:, cols])
        mid[:, cols] = (gate * (1.0 / (1.0 + jnp.exp(-gate))) * up).astype(BF16)
        return carry

    lax.fori_loop(0, FF // 256, mlp_cols, 0)
    load_d.wait()

    def down_cols(i, carry):
        cols = pl.ds(pl.multiple_of(i * 256, 256), 256)
        part[:, cols] = dot32(mid[...], buf_a[:, cols])
        return carry

    lax.fori_loop(0, D // 256, down_cols, 0)
    out_buf[mine, :] = (hid2[...].astype(F32) + reduce_rows(1)).astype(BF16)
    gather_rows(1, out_buf)
    st_hid = pltpu.make_async_copy(out_buf, o_hid, st_sem.at[NCH + 1])
    st_hid.start()

    for kind in range(3):
        for tn in range(2):
            for j in range(NCH):
                kv_send(kind, tn, j).wait_send()
    for j in range(NCH):
        store_kv(j).wait()
    st_new.wait()
    st_hid.wait()


def solution(mesh):
    seq_spec = P('replica', 'model', None)
    col_spec = P(None, None, 'model')
    row_spec = P(None, 'model', None)
    gain_spec = P(None, None)
    tok_spec = P('replica', None)
    cache_spec = P(None, 'replica', None, 'model', None)
    in_specs = (seq_spec, P('replica'), tok_spec, gain_spec, col_spec, col_spec, col_spec, row_spec, gain_spec, col_spec, col_spec, row_spec)
    out_specs = (tok_spec, tok_spec, cache_spec, cache_spec)

    def per_device(prompt, lengths, new_tok, norm_attn, w_q, w_k, w_v, w_o, norm_mlp, w_gate, w_up, w_down):
        my_idx = lax.axis_index('model')
        loc_c, loc_s = rotate_tables(my_idx * SEQ_LOC + jnp.arange(SEQ_LOC))
        tab_c = jnp.stack([loc_c, jnp.ones_like(loc_c)])
        tab_s = jnp.stack([loc_s, jnp.zeros_like(loc_s)])
        rot_c, rot_s = rotate_tables(jnp.concatenate([lengths - 1, lengths]))
        vmem = pl.BlockSpec(memory_space=pltpu.VMEM)
        hbm = pl.BlockSpec(memory_space=pl.ANY)
        smem = pl.BlockSpec(memory_space=pltpu.SMEM)
        dma = pltpu.SemaphoreType.DMA
        o_hid, o_kv, o_new = pl.pallas_call(
            kernel,
            out_shape=(jax.ShapeDtypeStruct((2 * NB, D), BF16), jax.ShapeDtypeStruct((2, NB, 256, HEAD_DIM), BF16),
                       jax.ShapeDtypeStruct((2, 2 * NB, HEAD_DIM), BF16)),
            in_specs=[smem] + [vmem] * 7 + [hbm] * 8,
            out_specs=(hbm, hbm, hbm),
            scratch_shapes=[
                pltpu.VMEM((NB * SEQ_LOC, D), BF16),
                pltpu.VMEM((D, FF), BF16),
                pltpu.VMEM((D, FF), BF16),
                pltpu.VMEM((2, NB, 256, HEAD_DIM), BF16),
                pltpu.VMEM((3, 2, NCH, CH, 64, HEAD_DIM), BF16),
                pltpu.VMEM((2 * ROWS, HEAD_DIM), F32),
                pltpu.VMEM((NB * 16, HEAD_DIM), F32),
                pltpu.VMEM((NB * 16, HEAD_DIM), F32),
                pltpu.VMEM((NB * 16, HEAD_DIM), F32),
                pltpu.VMEM((NB * 16, HEAD_DIM), F32),
                pltpu.VMEM((2 * NB, QW), BF16),
                pltpu.VMEM((NB, D), BF16),
                pltpu.VMEM((32, D), BF16),
                pltpu.VMEM((2 * NB, D), BF16),
                pltpu.VMEM((2 * NB, D), BF16),
                pltpu.VMEM((2 * NB, D), F32),
                pltpu.VMEM((NB, D), F32),
                pltpu.VMEM((32, D), F32),
                pltpu.VMEM((2 * NB, D), BF16),
                pltpu.VMEM((2 * NB, FF), BF16),
                pltpu.VMEM((32, D), BF16),
                pltpu.VMEM((2 * NB, D), BF16),
                pltpu.VMEM((2, 2 * NB, HEAD_DIM), BF16),
                dma((NCH,)), dma((2,)), dma((8,)), dma((NCH + 2,)),
                dma, dma, dma((WCH,)), dma((WCH,)), dma((WCH,)), dma((WCH,)),
                dma((WCH,)), dma((WCH,)), dma((WCH,)), dma((WCH,)),
                dma((3,)), dma((3,)), dma((3, 2, NCH)), dma((3, 2, NCH)), dma((2, 5)), dma((2, 5)),
            ],
            compiler_params=pltpu.CompilerParams(collective_id=0, has_side_effects=True, vmem_limit_bytes=67043328),
            name="layer",
        )(lengths, tab_c, tab_s, rot_c, rot_s, norm_attn, norm_mlp, new_tok,
          prompt.reshape(NB * SEQ_LOC, D), w_q[0], w_k[0], w_v[0], w_o[0], w_gate[0], w_up[0], w_down[0])
        caches = [jnp.concatenate([o_kv[i].reshape(NB, 128, 2, HEAD_DIM), o_new[i].reshape(NB, 1, 2, HEAD_DIM)], axis=1)[None]
                  for i in range(2)]
        return o_hid[NB:], o_hid[:NB], caches[0], caches[1]

    return jax.shard_map(per_device, mesh=mesh, in_specs=in_specs, out_specs=out_specs, check_vma=False)
```

```python
import functools

import jax
import jax.numpy as jnp
import numpy as np
from jax import lax
from jax.experimental import pallas as pl
from jax.experimental.pallas import tpu as pltpu
from jax.sharding import PartitionSpec as P

HEAD_DIM = 128
NEG_BIG = -1e30
MESH = pl.DeviceIdType.MESH
F32 = jnp.float32
BF16 = jnp.bfloat16

NB = 64
SEQ_LOC = 32
D = 3072
FF = 2048
QW = 768
CH = 16
NCH = NB // CH
ROWS = CH * SEQ_LOC
WCH = 4
WROWS = D // WCH


def dot32(lhs, rhs):
    return jnp.dot(lhs, rhs, preferred_element_type=F32)


def rotate_tables(n):
    half = HEAD_DIM // 2
    inv_freq = np.float32(10000.0) ** (np.float32(-2.0) * np.arange(half, dtype=np.float32) / np.float32(HEAD_DIM))
    angles = (np.arange(n, dtype=np.float32)[:, None] * inv_freq).astype(np.float32).astype(np.float64)
    cos_tab, sin_tab = np.cos(angles), np.sin(angles)
    return np.stack([np.concatenate([cos_tab, cos_tab], 1), np.concatenate([-sin_tab, sin_tab], 1)]).astype(np.float32)


def kernel(lens, tab, g_attn, g_mlp,
           new_tok, prompt, w_q, w_k, w_v, w_o, w_g, w_u, w_d,
           o_hid, o_kv,
           buf_a, buf_b, buf_c, kv, stage, flat, q_buf, k_buf, v_buf, a_buf, att,
           sel_r1, sel_r2, hid, normed, part, r1, r2, n2, mid, hid2, out_buf, knv, rot, o_buf,
           ld_p, ld_w, ld_big, st_sem,
           wp_s, wp_r, wx_s, wx_r, wfx_s, wfx_r, wy_s, wy_r, wfy_s, wfy_r,
           sel_s, sel_r, kv_s, kv_r, ar_s, ar_r):
    y = lax.axis_index("replica")
    m = lax.axis_index("model")
    c = lax.rem(m, 2)
    x = m // 2
    xs_m = lax.rem(m + 2, 4)
    xo_m = 3 - m
    pt_m = m + 1 - 2 * c
    xs, xo, pt, yp = (y, xs_m), (y, xo_m), (y, pt_m), (1 - y, m)

    def remote(src, dst, ssem, rsem, dev):
        return pltpu.make_async_remote_copy(src_ref=src, dst_ref=dst, send_sem=ssem, recv_sem=rsem,
                                            device_id=dev, device_id_type=MESH)

    def load_w(i):
        src = (w_k, w_v)[i]
        return pltpu.make_async_copy(src, buf_b.at[:, pl.ds(pl.multiple_of(m * 512 + i * 256, 256), 256)], ld_w.at[i])

    def load_p(j):
        r = pl.ds(pl.multiple_of(j * ROWS, ROWS), ROWS)
        return pltpu.make_async_copy(prompt.at[r], buf_a.at[r], ld_p.at[j])

    for i in range(2):
        load_w(i).start()
    for j in range(NCH):
        load_p(j).start()
    load_q = pltpu.make_async_copy(w_q, buf_c.at[:, pl.ds(0, QW)], ld_big.at[0])
    load_q.start()
    load_t = pltpu.make_async_copy(new_tok, hid.at[pl.ds(NB, NB)], ld_big.at[8])
    load_t.start()

    def load_o(i):
        return pltpu.make_async_copy(w_o.at[:, pl.ds(i * QW, QW)], buf_c.at[pl.ds(i * QW, QW), pl.ds(QW, QW)], ld_big.at[1 + i])

    for i in range(4):
        load_o(i).start()
    load_g = pltpu.make_async_copy(w_g, buf_b, ld_big.at[5])
    load_u = pltpu.make_async_copy(w_u, buf_c, ld_big.at[6])
    load_d = pltpu.make_async_copy(w_d, buf_a, ld_big.at[7])

    barrier = pltpu.get_barrier_semaphore()
    for dev in (xs, xo, pt, yp):
        pl.semaphore_signal(barrier, inc=1, device_id=dev, device_id_type=MESH)
    pl.semaphore_wait(barrier, 4)

    def w_ref(owner, h, r):
        return buf_b.at[pl.ds(r * WROWS, WROWS), pl.ds(pl.multiple_of(owner * 512 + h * 256, 256), 256)]

    def wx(r):
        ref = w_ref(m, y, r)
        return remote(ref, ref, wx_s.at[r], wx_r.at[r], xs)

    def wfx(r):
        ref = w_ref(xs_m, y, r)
        return remote(ref, ref, wfx_s.at[r], wfx_r.at[r], pt)

    def wy(r):
        ref = w_ref(xs_m, y, r)
        return remote(ref, ref, wy_s.at[r], wy_r.at[r], yp)

    def wfy(r):
        ref = w_ref(xs_m, 1 - y, r)
        return remote(ref, ref, wfy_s.at[r], wfy_r.at[r], pt)

    own = buf_b.at[:, pl.ds(pl.multiple_of(m * 512, 512), 512)]
    wp = remote(own, own, wp_s, wp_r, pt)
    for i in range(2):
        load_w(i).wait()
    for r in range(WCH):
        wx(r).start()
    wp.start()

    def forward_x(r):
        wx(r).wait_recv()
        wfx(r).start()
        wy(r).start()

    def forward_y(r):
        wy(r).wait_recv()
        wfy(r).start()

    gain_a = g_attn[...].astype(F32)
    row_iota = lax.broadcasted_iota(jnp.int32, (SEQ_LOC, 1), 0)

    def norm_prompts(i, carry):
        parts = []
        for t in range(8):
            b = i * 8 + t
            rows = pl.ds(pl.multiple_of(b * SEQ_LOC, SEQ_LOC), SEQ_LOC)
            v = buf_a[rows, :].astype(F32)
            inv = lax.rsqrt(jnp.mean(v * v, axis=-1, keepdims=True) + 1e-5)
            hit = row_iota == lens[b] - 1 - m * SEQ_LOC
            parts.append(jnp.sum(jnp.where(hit, v, 0.0), axis=0, keepdims=True))
            buf_a[rows, :] = (buf_a[rows, :].astype(F32) * inv * gain_a).astype(BF16)
        part[pl.ds(pl.multiple_of(i * 8, 8), 8), :] = jnp.concatenate(parts, axis=0)
        return carry

    per = CH // 8
    for j in range(NCH):
        load_p(j).wait()
        lax.fori_loop(j * per, (j + 1) * per, norm_prompts, 0)

    sel_b = normed.at[pl.ds(0, NB)]
    sel_b[...] = part[0:NB, :].astype(BF16)
    s1 = remote(sel_b, sel_r1, sel_s.at[0], sel_r.at[0], pt)
    s1.start()

    def unit_chunk(owner, h, j):
        col = pl.ds(pl.multiple_of(owner * 512 + h * 256, 256), 256)
        acc = dot32(buf_a[pl.ds(pl.multiple_of(j * ROWS, ROWS), ROWS), :], buf_b[:, col])
        here = pl.ds(pl.multiple_of(m * SEQ_LOC, SEQ_LOC), SEQ_LOC)
        ct = jnp.where(h == 0, tab[0, here, :], 1.0)
        st = jnp.where(h == 0, tab[1, here, :], 0.0)
        for hd in range(2):
            a = acc[:, hd * HEAD_DIM:(hd + 1) * HEAD_DIM]
            turned = pltpu.roll(a, HEAD_DIM // 2, 1)
            res = a.reshape(CH, SEQ_LOC, HEAD_DIM) * ct[None] + turned.reshape(CH, SEQ_LOC, HEAD_DIM) * st[None]
            flat[pl.ds(hd, ROWS, stride=2), :] = res.reshape(ROWS, HEAD_DIM)
        return flat[...].astype(BF16).reshape(CH, 2 * SEQ_LOC, HEAD_DIM)

    def kv_ref(h, j):
        return kv.at[h, pl.ds(pl.multiple_of(j * CH, CH), CH), pl.ds(pl.multiple_of(m * 64, 64), 64)]

    def kv_send(kind, turn, j):
        dev = (pt, xs, xo)[kind]
        h = y if turn == 0 else 1 - y
        return remote(stage.at[kind, turn, j], kv_ref(h, j), kv_s.at[kind, turn, j], kv_r.at[kind, turn, j], dev)

    def run_unit(kind, turn, j):
        owner = (pt_m, xs_m, xo_m)[kind]
        h = y if turn == 0 else 1 - y
        stage[kind, turn, j] = unit_chunk(owner, h, j)
        kv_send(kind, turn, j).start()

    forward_x(0)

    def own_units(i, carry):
        h, j = i // NCH, lax.rem(i, NCH)
        kv[h, pl.ds(pl.multiple_of(j * CH, CH), CH), pl.ds(pl.multiple_of(m * 64, 64), 64)] = unit_chunk(m, h, j)
        return carry

    lax.fori_loop(0, 2 * NCH, own_units, 0)
    forward_x(1)

    s1.wait()
    sel_b[...] = (sel_b[...].astype(F32) + sel_r1[...].astype(F32)).astype(BF16)
    half = pl.ds(pl.multiple_of(c * 32, 32), 32)
    s2 = remote(normed.at[half], sel_r2, sel_s.at[1], sel_r.at[1], xs)
    s2.start()

    wp.wait_recv()

    def loop_unit(kind, turn):
        def body(j, carry):
            run_unit(kind, turn, j)
            return carry
        lax.fori_loop(0, NCH, body, 0)

    loop_unit(0, 0)
    forward_x(2)
    forward_y(0)
    loop_unit(0, 1)
    forward_x(3)
    loop_unit(1, 0)
    forward_y(1)
    for r in range(WCH):
        wfx(r).wait_recv()
    loop_unit(2, 0)
    forward_y(2)

    s2.wait()
    hid[half, :] = (normed[half, :].astype(F32) + sel_r2[...].astype(F32)).astype(BF16)
    s3 = remote(hid.at[half], hid.at[half], sel_s.at[2], sel_r.at[2], pt)
    s3.start()
    forward_y(3)
    for r in range(WCH):
        wfy(r).wait_recv()

    def last_units(j, carry):
        run_unit(1, 1, j)
        run_unit(2, 1, j)
        return carry

    lax.fori_loop(0, NCH, last_units, 0)
    s3.wait()
    load_t.wait()

    def norm_rows(src, gain):
        v = src.astype(F32)
        inv = lax.rsqrt(jnp.mean(v * v, axis=-1, keepdims=True) + 1e-5)
        return (v * inv * gain).astype(BF16)

    def norm_hid(i, carry):
        rows = pl.ds(pl.multiple_of(i * 32, 32), 32)
        normed[rows, :] = norm_rows(hid[rows, :], gain_a)
        return carry

    lax.fori_loop(0, 4, norm_hid, 0)
    load_q.wait()
    q_buf[...] = jnp.zeros_like(q_buf)
    k_buf[...] = jnp.zeros_like(k_buf)
    v_buf[...] = jnp.zeros_like(v_buf)

    def pick(b, carry):
        pos = jnp.clip(lens[b], 1, 128)
        for i in range(2):
            rot[i, pl.ds(b, 1), :] = tab[i, pl.ds(pos - 1, 1), :]
            rot[i, pl.ds(NB + b, 1), :] = tab[i, pl.ds(pos, 1), :]
        return carry

    lax.fori_loop(0, NB, pick, 0)

    def turn(a, ct, st):
        return (a * ct + pltpu.roll(a, HEAD_DIM // 2, 1) * st).astype(BF16).astype(F32)

    for pair in range(3):
        qs = dot32(normed[...], buf_c[:, pair * 256:(pair + 1) * 256])
        for i in range(2):
            hd = pair * 2 + i
            q_h = turn(qs[:, i * HEAD_DIM:(i + 1) * HEAD_DIM], rot[0], rot[1])
            for t in range(2):
                q_buf[pl.ds(t * 8 + hd, NB, stride=16), :] = q_h[t * NB:(t + 1) * NB]
    toks = normed[NB:2 * NB, :]
    k_new = dot32(toks, buf_b[:, pl.ds(pl.multiple_of(m * 512, 256), 256)])
    v_new = dot32(toks, buf_b[:, pl.ds(pl.multiple_of(m * 512 + 256, 256), 256)])
    for g in range(2):
        cols = slice(g * HEAD_DIM, (g + 1) * HEAD_DIM)
        k_g = turn(k_new[:, cols], rot[0, NB:, :], rot[1, NB:, :])
        v_g = v_new[:, cols].astype(BF16).astype(F32)
        flat[pl.ds(g, NB, stride=2), :] = k_g
        flat[pl.ds(2 * NB + g, NB, stride=2), :] = v_g
        for i in range(3):
            rows = pl.ds(8 + 3 * g + i, NB, stride=16)
            k_buf[rows, :] = k_g
            v_buf[rows, :] = v_g
    knv[0] = flat[0:2 * NB, :].astype(BF16)
    knv[1] = flat[2 * NB:4 * NB, :].astype(BF16)

    wp.wait_send()
    for r in range(WCH):
        wx(r).wait_send()
        wfx(r).wait_send()
        wy(r).wait_send()
        wfy(r).wait_send()
    load_g.start()
    load_d.start()

    r_io = lax.broadcasted_iota(jnp.int32, (16, 256), 0)
    c_io = lax.broadcasted_iota(jnp.int32, (16, 256), 1)
    same = ((r_io & 7) >= 3) == ((c_io & 1) == 1)
    k_pos = c_io >> 1
    is_new = lax.broadcasted_iota(jnp.int32, (16, 1), 0) >= 8
    scale = HEAD_DIM ** -0.5

    def attend(b):
        rows = pl.ds(pl.multiple_of(b * 16, 16), 16)
        q = q_buf[rows, :]
        s = lax.dot_general(q.astype(BF16), kv[0, b], (((1,), (1,)), ((), ())), preferred_element_type=F32) * scale
        s = jnp.where(same & (k_pos < lens[b]), s, NEG_BIG)
        s_new = jnp.where(is_new, jnp.sum(q * k_buf[rows, :], axis=-1, keepdims=True) * scale, NEG_BIG)
        top = jnp.maximum(jnp.max(s, axis=-1, keepdims=True), s_new)
        p = jnp.exp(s - top)
        p_new = jnp.exp(s_new - top)
        total = jnp.sum(p, axis=-1, keepdims=True) + p_new
        acc = dot32(p.astype(BF16), kv[1, b]) + p_new * v_buf[rows, :]
        a_buf[rows, :] = acc / total

    def attend_four(i, carry):
        for t in range(4):
            attend(i * 4 + t)
        return carry

    def store_kv(h, g):
        rows = pl.ds(pl.multiple_of(g * 2064, 2064), 2064)
        return pltpu.make_async_copy(o_buf.at[h, pl.ds(0, 2064)], o_kv.at[h, rows], st_sem.at[h])

    def lay_out(g, carry):
        @pl.when(g > 0)
        def _():
            for h in range(2):
                store_kv(h, g - 1).wait()
        for h in range(2):
            for t in range(8):
                o_buf[h, t * 258:t * 258 + 256, :] = kv[h, g * 8 + t]
            new = knv[h, pl.ds(pl.multiple_of(g * 16, 16), 16), :]
            for t in range(8):
                o_buf[h, t * 258 + 256:t * 258 + 258, :] = new[2 * t:2 * t + 2]
            store_kv(h, g).start()
        return carry

    for j in range(NCH):
        for kind in range(3):
            for tn in range(2):
                kv_send(kind, tn, j).wait_recv()
        lax.fori_loop(j * (CH // 4), (j + 1) * (CH // 4), attend_four, 0)
        if j < NCH - 1:
            lax.fori_loop(j * (CH // 8), (j + 1) * (CH // 8), lay_out, 0)

    for hd in range(6):
        for t in range(2):
            att[t * NB:(t + 1) * NB, hd * HEAD_DIM:(hd + 1) * HEAD_DIM] = a_buf[pl.ds(t * 8 + hd, NB, stride=16), :].astype(BF16)
    for i in range(4):
        load_o(i).wait()
        part[:, i * QW:(i + 1) * QW] = dot32(att[...], buf_c[i * QW:(i + 1) * QW, QW:2 * QW])

    my_half = pl.ds(pl.multiple_of(c * 64, 64), 64)
    ot_half = pl.ds(pl.multiple_of((1 - c) * 64, 64), 64)
    mine = pl.ds(pl.multiple_of(c * 64 + x * 32, 32), 32)
    away = pl.ds(pl.multiple_of(c * 64 + (1 - x) * 32, 32), 32)

    def reduce_rows(k):
        a1 = remote(part.at[ot_half], r1, ar_s.at[k, 0], ar_r.at[k, 0], pt)
        a1.start()
        if k == 0:
            load_u.start()
        a1.wait_recv()
        x_half = pl.ds(pl.multiple_of((1 - x) * 32, 32), 32)
        part[away, :] = part[away, :] + r1[x_half, :]
        a2 = remote(part.at[away], r2, ar_s.at[k, 1], ar_r.at[k, 1], xs)
        a2.start()
        m_half = pl.ds(pl.multiple_of(x * 32, 32), 32)
        part[mine, :] = part[mine, :] + r1[m_half, :]
        if k == 0:
            lax.fori_loop((NCH - 1) * (CH // 8), NB // 8, lay_out, 0)
        a2.wait_recv()
        a1.wait_send()
        a2.wait_send()
        return part[mine, :] + r2[...]

    def gather_rows(k, buf):
        a3 = remote(buf.at[mine], buf.at[mine], ar_s.at[k, 2], ar_r.at[k, 2], xs)
        a3.start()
        a4 = remote(buf.at[mine], buf.at[mine], ar_s.at[k, 3], ar_r.at[k, 3], pt)
        a4.start()
        a3.wait_recv()
        a5 = remote(buf.at[away], buf.at[away], ar_s.at[k, 4], ar_r.at[k, 4], pt)
        a5.start()
        a4.wait_recv()
        a5.wait_recv()
        a3.wait_send()
        a4.wait_send()
        a5.wait_send()

    hid2[...] = (hid[mine, :].astype(F32) + reduce_rows(0)).astype(BF16)
    n2[mine, :] = norm_rows(hid2[...], g_mlp[...].astype(F32))
    gather_rows(0, n2)

    load_g.wait()
    load_u.wait()

    def mlp_cols(i, carry):
        cols = pl.ds(pl.multiple_of(i * 256, 256), 256)
        gate = dot32(n2[...], buf_b[:, cols])
        up = dot32(n2[...], buf_c[:, cols])
        mid[:, cols] = (gate * (1.0 / (1.0 + jnp.exp(-gate))) * up).astype(BF16)
        return carry

    lax.fori_loop(0, FF // 256, mlp_cols, 0)
    load_d.wait()

    def down_cols(i, carry):
        cols = pl.ds(pl.multiple_of(i * 256, 256), 256)
        part[:, cols] = dot32(mid[...], buf_a[:, cols])
        return carry

    lax.fori_loop(0, D // 256, down_cols, 0)
    out_buf[mine, :] = (hid2[...].astype(F32) + reduce_rows(1)).astype(BF16)
    gather_rows(1, out_buf)
    st_hid = pltpu.make_async_copy(out_buf, o_hid, st_sem.at[2])
    st_hid.start()

    for kind in range(3):
        for tn in range(2):
            for j in range(NCH):
                kv_send(kind, tn, j).wait_send()
    for h in range(2):
        store_kv(h, NB // 8 - 1).wait()
    st_hid.wait()


def solution(mesh):
    seq_spec = P('replica', 'model', None)
    col_spec = P(None, None, 'model')
    row_spec = P(None, 'model', None)
    gain_spec = P(None, None)
    tok_spec = P('replica', None)
    cache_spec = P(None, 'replica', None, 'model', None)
    in_specs = (seq_spec, P('replica'), tok_spec, gain_spec, col_spec, col_spec, col_spec, row_spec, gain_spec, col_spec, col_spec, row_spec)
    out_specs = (tok_spec, tok_spec, cache_spec, cache_spec)

    def per_device(prompt, lengths, new_tok, norm_attn, w_q, w_k, w_v, w_o, norm_mlp, w_gate, w_up, w_down):
        tab = jnp.asarray(rotate_tables(136))
        vmem = pl.BlockSpec(memory_space=pltpu.VMEM)
        hbm = pl.BlockSpec(memory_space=pl.ANY)
        smem = pl.BlockSpec(memory_space=pltpu.SMEM)
        dma = pltpu.SemaphoreType.DMA
        o_hid, o_kv = pl.pallas_call(
            kernel,
            out_shape=(jax.ShapeDtypeStruct((2 * NB, D), BF16), jax.ShapeDtypeStruct((2, NB * 258, HEAD_DIM), BF16)),
            in_specs=[smem] + [vmem] * 3 + [hbm] * 9,
            out_specs=(hbm, hbm),
            scratch_shapes=[
                pltpu.VMEM((NB * SEQ_LOC, D), BF16),
                pltpu.VMEM((D, FF), BF16),
                pltpu.VMEM((D, FF), BF16),
                pltpu.VMEM((2, NB, 256, HEAD_DIM), BF16),
                pltpu.VMEM((3, 2, NCH, CH, 64, HEAD_DIM), BF16),
                pltpu.VMEM((2 * ROWS, HEAD_DIM), F32),
                pltpu.VMEM((NB * 16, HEAD_DIM), F32),
                pltpu.VMEM((NB * 16, HEAD_DIM), F32),
                pltpu.VMEM((NB * 16, HEAD_DIM), F32),
                pltpu.VMEM((NB * 16, HEAD_DIM), F32),
                pltpu.VMEM((2 * NB, QW), BF16),
                pltpu.VMEM((NB, D), BF16),
                pltpu.VMEM((32, D), BF16),
                pltpu.VMEM((2 * NB, D), BF16),
                pltpu.VMEM((2 * NB, D), BF16),
                pltpu.VMEM((2 * NB, D), F32),
                pltpu.VMEM((NB, D), F32),
                pltpu.VMEM((32, D), F32),
                pltpu.VMEM((2 * NB, D), BF16),
                pltpu.VMEM((2 * NB, FF), BF16),
                pltpu.VMEM((32, D), BF16),
                pltpu.VMEM((2 * NB, D), BF16),
                pltpu.VMEM((2, 2 * NB, HEAD_DIM), BF16),
                pltpu.VMEM((2, 2 * NB, HEAD_DIM), F32),
                pltpu.VMEM((2, 8 * 258 + 32, HEAD_DIM), BF16),
                dma((NCH,)), dma((2,)), dma((9,)), dma((3,)),
                dma, dma, dma((WCH,)), dma((WCH,)), dma((WCH,)), dma((WCH,)),
                dma((WCH,)), dma((WCH,)), dma((WCH,)), dma((WCH,)),
                dma((3,)), dma((3,)), dma((3, 2, NCH)), dma((3, 2, NCH)), dma((2, 5)), dma((2, 5)),
            ],
            compiler_params=pltpu.CompilerParams(collective_id=0, has_side_effects=True, vmem_limit_bytes=67043328),
            name="layer",
        )(lengths, tab, norm_attn, norm_mlp, new_tok,
          prompt.reshape(NB * SEQ_LOC, D), w_q[0], w_k[0], w_v[0], w_o[0], w_gate[0], w_up[0], w_down[0])
        caches = o_kv.reshape(2, 1, NB, 129, 2, HEAD_DIM)
        return o_hid[NB:], o_hid[:NB], caches[0], caches[1]

    return jax.shard_map(per_device, mesh=mesh, in_specs=in_specs, out_specs=out_specs, check_vma=False)
```

```python
import functools

import jax
import jax.numpy as jnp
import numpy as np
from jax import lax
from jax.experimental import pallas as pl
from jax.experimental.pallas import tpu as pltpu
from jax.sharding import PartitionSpec as P

HEAD_DIM = 128
NEG_BIG = -1e30
MESH = pl.DeviceIdType.MESH
F32 = jnp.float32
BF16 = jnp.bfloat16

NB = 64
SEQ_LOC = 32
D = 3072
FF = 2048
QW = 768
CH = 16
NCH = NB // CH
ROWS = CH * SEQ_LOC
WCH = 4
WROWS = D // WCH


def dot32(lhs, rhs):
    return jnp.dot(lhs, rhs, preferred_element_type=F32)


def rotate_tables(n):
    half = HEAD_DIM // 2
    inv_freq = np.float32(10000.0) ** (np.float32(-2.0) * np.arange(half, dtype=np.float32) / np.float32(HEAD_DIM))
    angles = (np.arange(n, dtype=np.float32)[:, None] * inv_freq).astype(np.float32).astype(np.float64)
    cos_tab, sin_tab = np.cos(angles), np.sin(angles)
    return np.stack([np.concatenate([cos_tab, cos_tab], 1), np.concatenate([-sin_tab, sin_tab], 1)]).astype(np.float32)


def kernel(lens, tab, g_attn, g_mlp,
           new_tok, prompt, w_q, w_k, w_v, w_o, w_g, w_u, w_d,
           o_last, o_dec, o_k, o_v,
           buf_a, buf_b, buf_c, kv, stage, flat, q_buf, k_buf, v_buf, a_buf, att,
           sel_r1, sel_r2, hid, normed, part, r1, r2, x2, mid, p_buf, out_buf, knv, rot, o_buf,
           ld_p, ld_w, ld_big, st_sem,
           wp_s, wp_r, wx_s, wx_r, wfx_s, wfx_r, wy_s, wy_r, wfy_s, wfy_r,
           sel_s, sel_r, kv_s, kv_r, ar_s, ar_r):
    y = lax.axis_index("replica")
    m = lax.axis_index("model")
    c = lax.rem(m, 2)
    x = m // 2
    xs_m = lax.rem(m + 2, 4)
    xo_m = 3 - m
    pt_m = m + 1 - 2 * c
    xs, xo, pt, yp = (y, xs_m), (y, xo_m), (y, pt_m), (1 - y, m)

    def remote(src, dst, ssem, rsem, dev):
        return pltpu.make_async_remote_copy(src_ref=src, dst_ref=dst, send_sem=ssem, recv_sem=rsem,
                                            device_id=dev, device_id_type=MESH)

    def load_w(i):
        src = (w_k, w_v)[i]
        return pltpu.make_async_copy(src, buf_b.at[:, pl.ds(pl.multiple_of(m * 512 + i * 256, 256), 256)], ld_w.at[i])

    def load_p(j):
        r = pl.ds(pl.multiple_of(j * ROWS, ROWS), ROWS)
        return pltpu.make_async_copy(prompt.at[r], buf_a.at[r], ld_p.at[j])

    for i in range(2):
        load_w(i).start()
    for j in range(NCH):
        load_p(j).start()
    load_q = pltpu.make_async_copy(w_q, buf_c.at[:, pl.ds(0, QW)], ld_big.at[0])
    load_q.start()
    load_t = pltpu.make_async_copy(new_tok, hid.at[pl.ds(NB, NB)], ld_big.at[8])
    load_t.start()

    def load_o(i):
        return pltpu.make_async_copy(w_o.at[:, pl.ds(i * QW, QW)], buf_c.at[pl.ds(i * QW, QW), pl.ds(QW, QW)], ld_big.at[1 + i])

    for i in range(4):
        load_o(i).start()
    load_g = pltpu.make_async_copy(w_g, buf_b, ld_big.at[5])
    load_u = pltpu.make_async_copy(w_u, buf_c, ld_big.at[6])
    load_d = pltpu.make_async_copy(w_d, buf_a, ld_big.at[7])

    barrier = pltpu.get_barrier_semaphore()
    for dev in (xs, xo, pt, yp):
        pl.semaphore_signal(barrier, inc=1, device_id=dev, device_id_type=MESH)
    pl.semaphore_wait(barrier, 4)

    def w_ref(owner, half, r):
        rows = pl.ds(pl.multiple_of(half * (D // 2) + (r % 2) * WROWS, WROWS), WROWS)
        return buf_b.at[rows, pl.ds(pl.multiple_of(owner * 512 + (r // 2) * 256, 256), 256)]

    def wx(r):
        ref = w_ref(m, y, r)
        return remote(ref, ref, wx_s.at[r], wx_r.at[r], xs)

    def wfx(r):
        ref = w_ref(xs_m, y, r)
        return remote(ref, ref, wfx_s.at[r], wfx_r.at[r], pt)

    def wy(r):
        ref = w_ref(xs_m, y, r)
        return remote(ref, ref, wy_s.at[r], wy_r.at[r], yp)

    def wfy(r):
        ref = w_ref(xs_m, 1 - y, r)
        return remote(ref, ref, wfy_s.at[r], wfy_r.at[r], pt)

    own = buf_b.at[:, pl.ds(pl.multiple_of(m * 512, 512), 512)]
    wp = remote(own, own, wp_s, wp_r, pt)
    for i in range(2):
        load_w(i).wait()
    for r in range(WCH):
        wx(r).start()
    wp.start()

    def forward_x(r):
        wx(r).wait_recv()
        wfx(r).start()
        wy(r).start()

    def forward_y(r):
        wy(r).wait_recv()
        wfy(r).start()

    gain_a = g_attn[...].astype(F32)
    row_iota = lax.broadcasted_iota(jnp.int32, (SEQ_LOC, 1), 0)

    def norm_prompts(i, carry):
        parts = []
        for t in range(8):
            b = i * 8 + t
            rows = pl.ds(pl.multiple_of(b * SEQ_LOC, SEQ_LOC), SEQ_LOC)
            v = buf_a[rows, :].astype(F32)
            inv = lax.rsqrt(jnp.mean(v * v, axis=-1, keepdims=True) + 1e-5)
            hit = row_iota == lens[b] - 1 - m * SEQ_LOC
            parts.append(jnp.sum(jnp.where(hit, v, 0.0), axis=0, keepdims=True))
            buf_a[rows, :] = (buf_a[rows, :].astype(F32) * inv * gain_a).astype(BF16)
        part[pl.ds(pl.multiple_of(i * 8, 8), 8), :] = jnp.concatenate(parts, axis=0)
        return carry

    per = CH // 8
    for j in range(NCH):
        load_p(j).wait()
        lax.fori_loop(j * per, (j + 1) * per, norm_prompts, 0)

    sel_b = normed.at[pl.ds(0, NB)]
    sel_b[...] = part[0:NB, :].astype(BF16)
    s1 = remote(sel_b, sel_r1, sel_s.at[0], sel_r.at[0], pt)
    s1.start()

    def unit_chunk(owner, h, j):
        col = pl.ds(pl.multiple_of(owner * 512 + h * 256, 256), 256)
        acc = dot32(buf_a[pl.ds(pl.multiple_of(j * ROWS, ROWS), ROWS), :], buf_b[:, col])
        here = pl.ds(pl.multiple_of(m * SEQ_LOC, SEQ_LOC), SEQ_LOC)
        for hd in range(2):
            a = acc[:, hd * HEAD_DIM:(hd + 1) * HEAD_DIM]
            if h == 0:
                turned = pltpu.roll(a, HEAD_DIM // 2, 1).reshape(CH, SEQ_LOC, HEAD_DIM)
                a = a.reshape(CH, SEQ_LOC, HEAD_DIM) * tab[0, here, :][None] + turned * tab[1, here, :][None]
                a = a.reshape(ROWS, HEAD_DIM)
            flat[pl.ds(hd, ROWS, stride=2), :] = a
        return flat[...].astype(BF16).reshape(CH, 2 * SEQ_LOC, HEAD_DIM)

    def kv_ref(h, j):
        return kv.at[h, pl.ds(pl.multiple_of(j * CH, CH), CH), pl.ds(pl.multiple_of(m * 64, 64), 64)]

    def kv_send(kind, h, j):
        dev = (pt, xs, xo)[kind]
        return remote(stage.at[kind, h, j], kv_ref(h, j), kv_s.at[kind, h, j], kv_r.at[kind, h, j], dev)

    def run_unit(kind, h, j):
        owner = (pt_m, xs_m, xo_m)[kind]
        stage[kind, h, j] = unit_chunk(owner, h, j)
        kv_send(kind, h, j).start()

    def own_unit(h):
        def body(j, carry):
            kv[h, pl.ds(pl.multiple_of(j * CH, CH), CH), pl.ds(pl.multiple_of(m * 64, 64), 64)] = unit_chunk(m, h, j)
            return carry
        lax.fori_loop(0, NCH, body, 0)

    def loop_unit(kind, h):
        def body(j, carry):
            run_unit(kind, h, j)
            return carry
        lax.fori_loop(0, NCH, body, 0)

    forward_x(0)
    own_unit(0)
    s1.wait()
    sel_b[...] = (sel_b[...].astype(F32) + sel_r1[...].astype(F32)).astype(BF16)
    half = pl.ds(pl.multiple_of(c * 32, 32), 32)
    s2 = remote(normed.at[half], sel_r2, sel_s.at[1], sel_r.at[1], xs)
    s2.start()
    own_unit(1)
    forward_x(1)
    forward_y(0)
    wp.wait_recv()
    loop_unit(0, 0)
    forward_x(2)
    forward_y(1)
    loop_unit(1, 0)
    for r in range(2):
        wfx(r).wait_recv()
        wfy(r).wait_recv()
    loop_unit(2, 0)
    forward_x(3)
    forward_y(2)
    loop_unit(0, 1)

    s2.wait()
    hid[half, :] = (normed[half, :].astype(F32) + sel_r2[...].astype(F32)).astype(BF16)
    s3 = remote(hid.at[half], hid.at[half], sel_s.at[2], sel_r.at[2], pt)
    s3.start()
    forward_y(3)
    for r in range(2, WCH):
        wfx(r).wait_recv()
        wfy(r).wait_recv()

    def last_units(j, carry):
        run_unit(1, 1, j)
        run_unit(2, 1, j)
        return carry

    lax.fori_loop(0, NCH, last_units, 0)
    s3.wait()
    load_t.wait()

    def norm_rows(src, gain):
        v = src.astype(F32)
        inv = lax.rsqrt(jnp.mean(v * v, axis=-1, keepdims=True) + 1e-5)
        return (v * inv * gain).astype(BF16)

    def norm_hid(i, carry):
        rows = pl.ds(pl.multiple_of(i * 32, 32), 32)
        normed[rows, :] = norm_rows(hid[rows, :], gain_a)
        return carry

    lax.fori_loop(0, 4, norm_hid, 0)
    load_q.wait()
    q_buf[...] = jnp.zeros_like(q_buf)
    k_buf[...] = jnp.zeros_like(k_buf)
    v_buf[...] = jnp.zeros_like(v_buf)

    def pick(b, carry):
        pos = jnp.clip(lens[b], 1, 128)
        for i in range(2):
            rot[i, pl.ds(b, 1), :] = tab[i, pl.ds(pos - 1, 1), :]
            rot[i, pl.ds(NB + b, 1), :] = tab[i, pl.ds(pos, 1), :]
        return carry

    lax.fori_loop(0, NB, pick, 0)

    def turn(a, ct, st):
        return (a * ct + pltpu.roll(a, HEAD_DIM // 2, 1) * st).astype(BF16).astype(F32)

    for pair in range(3):
        qs = dot32(normed[...], buf_c[:, pair * 256:(pair + 1) * 256])
        for i in range(2):
            hd = pair * 2 + i
            q_h = turn(qs[:, i * HEAD_DIM:(i + 1) * HEAD_DIM], rot[0], rot[1])
            for t in range(2):
                q_buf[pl.ds(t * 8 + hd, NB, stride=16), :] = q_h[t * NB:(t + 1) * NB]
    toks = normed[NB:2 * NB, :]
    k_new = dot32(toks, buf_b[:, pl.ds(pl.multiple_of(m * 512, 256), 256)])
    v_new = dot32(toks, buf_b[:, pl.ds(pl.multiple_of(m * 512 + 256, 256), 256)])
    for g in range(2):
        cols = slice(g * HEAD_DIM, (g + 1) * HEAD_DIM)
        k_g = turn(k_new[:, cols], rot[0, NB:, :], rot[1, NB:, :])
        v_g = v_new[:, cols].astype(BF16).astype(F32)
        flat[pl.ds(g, NB, stride=2), :] = k_g
        flat[pl.ds(2 * NB + g, NB, stride=2), :] = v_g
        for i in range(3):
            rows = pl.ds(8 + 3 * g + i, NB, stride=16)
            k_buf[rows, :] = k_g
            v_buf[rows, :] = v_g
    knv[0] = flat[0:2 * NB, :].astype(BF16)
    knv[1] = flat[2 * NB:4 * NB, :].astype(BF16)

    wp.wait_send()
    for r in range(WCH):
        wx(r).wait_send()
        wfx(r).wait_send()
        wy(r).wait_send()
        wfy(r).wait_send()
    load_g.start()
    load_d.start()

    r_io = lax.broadcasted_iota(jnp.int32, (16, 256), 0)
    c_io = lax.broadcasted_iota(jnp.int32, (16, 256), 1)
    same = ((r_io & 7) >= 3) == ((c_io & 1) == 1)
    k_pos = c_io >> 1
    is_new = lax.broadcasted_iota(jnp.int32, (16, 1), 0) >= 8
    scale = HEAD_DIM ** -0.5

    def score(b):
        rows = pl.ds(pl.multiple_of(b * 16, 16), 16)
        q = q_buf[rows, :]
        s = lax.dot_general(q.astype(BF16), kv[0, b], (((1,), (1,)), ((), ())), preferred_element_type=F32) * scale
        s = jnp.where(same & (k_pos < lens[b]), s, NEG_BIG)
        s_new = jnp.where(is_new, jnp.sum(q * k_buf[rows, :], axis=-1, keepdims=True) * scale, NEG_BIG)
        top = jnp.maximum(jnp.max(s, axis=-1, keepdims=True), s_new)
        p = jnp.exp(s - top)
        p_new = jnp.exp(s_new - top)
        inv = 1.0 / (jnp.sum(p, axis=-1, keepdims=True) + p_new)
        p_buf[rows, :] = (p * inv).astype(BF16)
        a_buf[rows, :] = (p_new * inv) * v_buf[rows, :]

    def score_four(i, carry):
        for t in range(4):
            score(i * 4 + t)
        return carry

    def weigh_eight(i, carry):
        for t in range(8):
            b = i * 8 + t
            rows = pl.ds(pl.multiple_of(b * 16, 16), 16)
            a_buf[rows, :] = a_buf[rows, :] + dot32(p_buf[rows, :], kv[1, b])
        return carry

    def store_kv(h, g):
        rows = pl.ds(pl.multiple_of(g * 2064, 2064), 2064)
        return pltpu.make_async_copy(o_buf.at[h, pl.ds(0, 2064)], (o_k, o_v)[h].at[rows], st_sem.at[h])

    def lay_out(h):
        def body(g, carry):
            @pl.when(g > 0)
            def _():
                store_kv(h, g - 1).wait()
            for t in range(8):
                o_buf[h, t * 258:t * 258 + 256, :] = kv[h, g * 8 + t]
            new = knv[h, pl.ds(pl.multiple_of(g * 16, 16), 16), :]
            for t in range(8):
                o_buf[h, t * 258 + 256:t * 258 + 258, :] = new[2 * t:2 * t + 2]
            store_kv(h, g).start()
            return carry
        return body

    for j in range(NCH):
        for kind in range(3):
            kv_send(kind, 0, j).wait_recv()
        lax.fori_loop(j * (CH // 4), (j + 1) * (CH // 4), score_four, 0)
        lax.fori_loop(j * (CH // 8), (j + 1) * (CH // 8), lay_out(0), 0)
    for j in range(NCH):
        for kind in range(3):
            kv_send(kind, 1, j).wait_recv()
        lax.fori_loop(j * (CH // 8), (j + 1) * (CH // 8), weigh_eight, 0)
        if j < NCH - 1:
            lax.fori_loop(j * (CH // 8), (j + 1) * (CH // 8), lay_out(1), 0)

    for hd in range(6):
        for t in range(2):
            att[t * NB:(t + 1) * NB, hd * HEAD_DIM:(hd + 1) * HEAD_DIM] = a_buf[pl.ds(t * 8 + hd, NB, stride=16), :].astype(BF16)
    ot_half = pl.ds(pl.multiple_of((1 - c) * 64, 64), 64)
    mine = pl.ds(pl.multiple_of(c * 64 + x * 32, 32), 32)
    away = pl.ds(pl.multiple_of(c * 64 + (1 - x) * 32, 32), 32)
    mine_r1 = pl.ds(pl.multiple_of(x * 32, 32), 32)
    away_r1 = pl.ds(pl.multiple_of((1 - x) * 32, 32), 32)

    def reduce_all(k, produce, after, resid, buf):
        def msg(step, i, src, dst, dev):
            return remote(src, dst, ar_s.at[k, step, i], ar_r.at[k, step, i], dev)

        cols = [pl.ds(i * QW, QW) for i in range(4)]
        a1 = [msg(0, i, part.at[ot_half, cols[i]], r1.at[:, cols[i]], pt) for i in range(4)]
        a2 = [msg(1, i, part.at[away, cols[i]], r2.at[:, cols[i]], xs) for i in range(4)]
        a3 = [msg(2, i, buf.at[mine, cols[i]], buf.at[mine, cols[i]], xs) for i in range(4)]
        a4 = [msg(3, i, buf.at[mine, cols[i]], buf.at[mine, cols[i]], pt) for i in range(4)]
        a5 = [msg(4, i, buf.at[away, cols[i]], buf.at[away, cols[i]], pt) for i in range(4)]

        def over_x(i):
            a1[i].wait_recv()
            part[away, cols[i]] = part[away, cols[i]] + r1[away_r1, cols[i]]
            a2[i].start()
            part[mine, cols[i]] = part[mine, cols[i]] + r1[mine_r1, cols[i]]

        for i in range(4):
            produce(i)
            a1[i].start()
            if i:
                over_x(i - 1)
        over_x(3)
        after()
        for i in range(4):
            a2[i].wait_recv()
            total = part[mine, cols[i]] + r2[:, cols[i]]
            buf[mine, cols[i]] = (resid[mine, cols[i]].astype(F32) + total).astype(BF16)
            a3[i].start()
            a4[i].start()
        for i in range(4):
            a3[i].wait_recv()
            a5[i].start()
        for i in range(4):
            a4[i].wait_recv()
            a5[i].wait_recv()
        for step in (a1, a2, a3, a4, a5):
            for i in range(4):
                step[i].wait_send()

    def w_o_cols(i):
        load_o(i).wait()
        part[:, i * QW:(i + 1) * QW] = dot32(att[...], buf_c[i * QW:(i + 1) * QW, QW:2 * QW])

    def after_w_o():
        load_u.start()
        lax.fori_loop((NCH - 1) * (CH // 8), NB // 8, lay_out(1), 0)

    reduce_all(0, w_o_cols, after_w_o, hid, x2)
    gain_m = g_mlp[...].astype(F32)

    def norm_x2(i, carry):
        rows = pl.ds(pl.multiple_of(i * 32, 32), 32)
        normed[rows, :] = norm_rows(x2[rows, :], gain_m)
        return carry

    lax.fori_loop(0, 4, norm_x2, 0)
    load_g.wait()
    load_u.wait()

    def mlp_cols(i, carry):
        cols = pl.ds(pl.multiple_of(i * 256, 256), 256)
        gate = dot32(normed[...], buf_b[:, cols])
        up = dot32(normed[...], buf_c[:, cols])
        mid[:, cols] = (gate * (1.0 / (1.0 + jnp.exp(-gate))) * up).astype(BF16)
        return carry

    lax.fori_loop(0, FF // 256, mlp_cols, 0)
    load_d.wait()

    def down_cols(i):
        def body(t, carry):
            cols = pl.ds(pl.multiple_of(i * QW + t * 256, 256), 256)
            part[:, cols] = dot32(mid[...], buf_a[:, cols])
            return carry
        lax.fori_loop(0, QW // 256, body, 0)

    reduce_all(1, down_cols, lambda: None, x2, out_buf)
    st_last = pltpu.make_async_copy(out_buf.at[pl.ds(0, NB)], o_last, st_sem.at[2])
    st_dec = pltpu.make_async_copy(out_buf.at[pl.ds(NB, NB)], o_dec, st_sem.at[3])
    st_last.start()
    st_dec.start()

    for kind in range(3):
        for tn in range(2):
            for j in range(NCH):
                kv_send(kind, tn, j).wait_send()
    for h in range(2):
        store_kv(h, NB // 8 - 1).wait()
    st_last.wait()
    st_dec.wait()


def solution(mesh):
    seq_spec = P('replica', 'model', None)
    col_spec = P(None, None, 'model')
    row_spec = P(None, 'model', None)
    gain_spec = P(None, None)
    tok_spec = P('replica', None)
    cache_spec = P(None, 'replica', None, 'model', None)
    in_specs = (seq_spec, P('replica'), tok_spec, gain_spec, col_spec, col_spec, col_spec, row_spec, gain_spec, col_spec, col_spec, row_spec)
    out_specs = (tok_spec, tok_spec, cache_spec, cache_spec)

    def per_device(prompt, lengths, new_tok, norm_attn, w_q, w_k, w_v, w_o, norm_mlp, w_gate, w_up, w_down):
        tab = jnp.asarray(rotate_tables(136))
        vmem = pl.BlockSpec(memory_space=pltpu.VMEM)
        hbm = pl.BlockSpec(memory_space=pl.ANY)
        smem = pl.BlockSpec(memory_space=pltpu.SMEM)
        dma = pltpu.SemaphoreType.DMA
        o_last, o_dec, o_k, o_v = pl.pallas_call(
            kernel,
            out_shape=(jax.ShapeDtypeStruct((NB, D), BF16),) * 2 + (jax.ShapeDtypeStruct((NB * 258, HEAD_DIM), BF16),) * 2,
            in_specs=[smem] + [vmem] * 3 + [hbm] * 9,
            out_specs=(hbm,) * 4,
            scratch_shapes=[
                pltpu.VMEM((NB * SEQ_LOC, D), BF16),
                pltpu.VMEM((D, FF), BF16),
                pltpu.VMEM((D, FF), BF16),
                pltpu.VMEM((2, NB, 256, HEAD_DIM), BF16),
                pltpu.VMEM((3, 2, NCH, CH, 64, HEAD_DIM), BF16),
                pltpu.VMEM((2 * ROWS, HEAD_DIM), F32),
                pltpu.VMEM((NB * 16, HEAD_DIM), F32),
                pltpu.VMEM((NB * 16, HEAD_DIM), F32),
                pltpu.VMEM((NB * 16, HEAD_DIM), F32),
                pltpu.VMEM((NB * 16, HEAD_DIM), F32),
                pltpu.VMEM((2 * NB, QW), BF16),
                pltpu.VMEM((NB, D), BF16),
                pltpu.VMEM((32, D), BF16),
                pltpu.VMEM((2 * NB, D), BF16),
                pltpu.VMEM((2 * NB, D), BF16),
                pltpu.VMEM((2 * NB, D), F32),
                pltpu.VMEM((NB, D), F32),
                pltpu.VMEM((32, D), F32),
                pltpu.VMEM((2 * NB, D), BF16),
                pltpu.VMEM((2 * NB, FF), BF16),
                pltpu.VMEM((NB * 16, 256), BF16),
                pltpu.VMEM((2 * NB, D), BF16),
                pltpu.VMEM((2, 2 * NB, HEAD_DIM), BF16),
                pltpu.VMEM((2, 2 * NB, HEAD_DIM), F32),
                pltpu.VMEM((2, 8 * 258 + 32, HEAD_DIM), BF16),
                dma((NCH,)), dma((2,)), dma((9,)), dma((4,)),
                dma, dma, dma((WCH,)), dma((WCH,)), dma((WCH,)), dma((WCH,)),
                dma((WCH,)), dma((WCH,)), dma((WCH,)), dma((WCH,)),
                dma((3,)), dma((3,)), dma((3, 2, NCH)), dma((3, 2, NCH)), dma((2, 5, 4)), dma((2, 5, 4)),
            ],
            compiler_params=pltpu.CompilerParams(collective_id=0, has_side_effects=True, vmem_limit_bytes=67043328),
            name="layer",
        )(lengths, tab, norm_attn, norm_mlp, new_tok,
          prompt.reshape(NB * SEQ_LOC, D), w_q[0], w_k[0], w_v[0], w_o[0], w_gate[0], w_up[0], w_down[0])
        caches = [o.reshape(1, NB, 129, 2, HEAD_DIM) for o in (o_k, o_v)]
        return o_dec, o_last, caches[0], caches[1]

    return jax.shard_map(per_device, mesh=mesh, in_specs=in_specs, out_specs=out_specs, check_vma=False)
```

```python
import functools

import jax
import jax.numpy as jnp
import numpy as np
from jax import lax
from jax.experimental import pallas as pl
from jax.experimental.pallas import tpu as pltpu
from jax.sharding import PartitionSpec as P

HEAD_DIM = 128
NEG_BIG = -1e30
MESH = pl.DeviceIdType.MESH
F32 = jnp.float32
BF16 = jnp.bfloat16

NB = 64
SEQ_LOC = 32
D = 3072
FF = 2048
QW = 768
CH = 16
NCH = NB // CH
ROWS = CH * SEQ_LOC
LATE = NCH - 1
N_GAP = 3
WCH = 4
WROWS = D // WCH


def dot32(lhs, rhs):
    return jnp.dot(lhs, rhs, preferred_element_type=F32)


def rotate_tables(n):
    half = HEAD_DIM // 2
    inv_freq = np.float32(10000.0) ** (np.float32(-2.0) * np.arange(half, dtype=np.float32) / np.float32(HEAD_DIM))
    angles = (np.arange(n, dtype=np.float32)[:, None] * inv_freq).astype(np.float32).astype(np.float64)
    cos_tab, sin_tab = np.cos(angles), np.sin(angles)
    return np.stack([np.concatenate([cos_tab, cos_tab], 1), np.concatenate([-sin_tab, sin_tab], 1)]).astype(np.float32)


def kernel(lens, tab, g_attn, g_mlp,
           new_tok, prompt, w_q, w_k, w_v, w_o, w_g, w_u, w_d,
           o_last, o_dec, o_k, o_v,
           buf_a, buf_b, buf_c, kv, stage, stage_p, flat, q_buf, k_buf, v_buf, a_buf, att,
           sel_r1, sel_r2, hid, normed, part, r1, r2, x2, mid, p_buf, knv, rot, o_buf,
           rb, qb, qb_r, m_buf, l_buf, pb, pb_r,
           ld_p, ld_w, ld_big, st_sem,
           wp_s, wp_r, wx_s, wx_r, wfx_s, wfx_r, wy_s, wy_r, wfy_s, wfy_r,
           sel_s, sel_r, kv_s, kv_r, ar_s, ar_r, rb_s, rb_r, late_s, late_r, qp_s, qp_r):
    y = lax.axis_index("replica")
    m = lax.axis_index("model")
    c = lax.rem(m, 2)
    x = m // 2
    xs_m = lax.rem(m + 2, 4)
    xo_m = 3 - m
    pt_m = m + 1 - 2 * c
    xs, xo, pt, yp = (y, xs_m), (y, xo_m), (y, pt_m), (1 - y, m)

    def remote(src, dst, ssem, rsem, dev):
        return pltpu.make_async_remote_copy(src_ref=src, dst_ref=dst, send_sem=ssem, recv_sem=rsem,
                                            device_id=dev, device_id_type=MESH)

    def load_w(i):
        src = (w_k, w_v)[i]
        return pltpu.make_async_copy(src, buf_b.at[:, pl.ds(pl.multiple_of(m * 512 + i * 256, 256), 256)], ld_w.at[i])

    def load_p(j):
        r = pl.ds(pl.multiple_of(j * ROWS, ROWS), ROWS)
        return pltpu.make_async_copy(prompt.at[r], buf_a.at[r], ld_p.at[j])

    for i in range(2):
        load_w(i).start()
    for j in range(NCH):
        load_p(j).start()
    load_q = pltpu.make_async_copy(w_q, buf_c.at[:, pl.ds(0, QW)], ld_big.at[0])
    load_q.start()
    load_t = pltpu.make_async_copy(new_tok, hid.at[pl.ds(NB, NB)], ld_big.at[8])
    load_t.start()

    def load_o(i):
        return pltpu.make_async_copy(w_o.at[:, pl.ds(i * QW, QW)], buf_c.at[pl.ds(i * QW, QW), pl.ds(QW, QW)], ld_big.at[1 + i])

    for i in range(4):
        load_o(i).start()
    load_g = pltpu.make_async_copy(w_g, buf_b, ld_big.at[5])
    load_u = pltpu.make_async_copy(w_u, buf_c, ld_big.at[6])
    load_d = pltpu.make_async_copy(w_d, buf_a, ld_big.at[7])

    barrier = pltpu.get_barrier_semaphore()
    for dev in (xs, xo, pt, yp):
        pl.semaphore_signal(barrier, inc=1, device_id=dev, device_id_type=MESH)
    pl.semaphore_wait(barrier, 4)

    def w_ref(owner, half, r):
        rows = pl.ds(pl.multiple_of(half * (D // 2) + (r % 2) * WROWS, WROWS), WROWS)
        return buf_b.at[rows, pl.ds(pl.multiple_of(owner * 512 + (r // 2) * 256, 256), 256)]

    def wx(r):
        ref = w_ref(m, y, r)
        return remote(ref, ref, wx_s.at[r], wx_r.at[r], xs)

    def wfx(r):
        ref = w_ref(xs_m, y, r)
        return remote(ref, ref, wfx_s.at[r], wfx_r.at[r], pt)

    def wy(r):
        ref = w_ref(xs_m, y, r)
        return remote(ref, ref, wy_s.at[r], wy_r.at[r], yp)

    def wfy(r):
        ref = w_ref(xs_m, 1 - y, r)
        return remote(ref, ref, wfy_s.at[r], wfy_r.at[r], pt)

    own = buf_b.at[:, pl.ds(pl.multiple_of(m * 512, 512), 512)]
    wp = remote(own, own, wp_s, wp_r, pt)
    for i in range(2):
        load_w(i).wait()
    for r in range(WCH):
        wx(r).start()
    wp.start()

    def forward_x(r):
        wx(r).wait_recv()
        wfx(r).start()
        wy(r).start()

    def forward_y(r):
        wy(r).wait_recv()
        wfy(r).start()

    gain_a = g_attn[...].astype(F32)
    row_iota = lax.broadcasted_iota(jnp.int32, (SEQ_LOC, 1), 0)

    def norm_prompts(i, carry):
        parts = []
        for t in range(8):
            b = i * 8 + t
            rows = pl.ds(pl.multiple_of(b * SEQ_LOC, SEQ_LOC), SEQ_LOC)
            v = buf_a[rows, :].astype(F32)
            inv = lax.rsqrt(jnp.mean(v * v, axis=-1, keepdims=True) + 1e-5)
            hit = row_iota == lens[b] - 1 - m * SEQ_LOC
            parts.append(jnp.sum(jnp.where(hit, v, 0.0), axis=0, keepdims=True))
            buf_a[rows, :] = (buf_a[rows, :].astype(F32) * inv * gain_a).astype(BF16)
        part[pl.ds(pl.multiple_of(i * 8, 8), 8), :] = jnp.concatenate(parts, axis=0)
        return carry

    per = CH // 8
    for j in range(NCH):
        load_p(j).wait()
        lax.fori_loop(j * per, (j + 1) * per, norm_prompts, 0)

    sel_b = normed.at[pl.ds(0, NB)]
    sel_b[...] = part[0:NB, :].astype(BF16)
    s1 = remote(sel_b, sel_r1, sel_s.at[0], sel_r.at[0], pt)
    s1.start()

    def unit_chunk(owner, h, j):
        col = pl.ds(pl.multiple_of(owner * 512 + h * 256, 256), 256)
        acc = dot32(buf_a[pl.ds(pl.multiple_of(j * ROWS, ROWS), ROWS), :], buf_b[:, col])
        here = pl.ds(pl.multiple_of(m * SEQ_LOC, SEQ_LOC), SEQ_LOC)
        for hd in range(2):
            a = acc[:, hd * HEAD_DIM:(hd + 1) * HEAD_DIM]
            if h == 0:
                turned = pltpu.roll(a, HEAD_DIM // 2, 1).reshape(CH, SEQ_LOC, HEAD_DIM)
                a = a.reshape(CH, SEQ_LOC, HEAD_DIM) * tab[0, here, :][None] + turned * tab[1, here, :][None]
                a = a.reshape(ROWS, HEAD_DIM)
            flat[pl.ds(hd, ROWS, stride=2), :] = a
        return flat[...].astype(BF16).reshape(CH, 2 * SEQ_LOC, HEAD_DIM)

    def kv_ref(h, j):
        return kv.at[h, pl.ds(pl.multiple_of(j * CH, CH), CH), pl.ds(pl.multiple_of(m * 64, 64), 64)]

    def kv_send(kind, h, j):
        dev = (pt, xs, xo)[kind]
        return remote(stage_p.at[j] if kind == 0 else stage.at[kind - 1, h, j], kv_ref(h, j), kv_s.at[kind, h, j], kv_r.at[kind, h, j], dev)

    def late_send(i):
        kind, h, part8 = 1 + i % 2, (i // 2) % 2, i // 4
        src = stage.at[kind - 1, h, LATE, pl.ds(part8 * 8, 8)]
        dst = kv.at[h, pl.ds(LATE * CH + part8 * 8, 8), pl.ds(pl.multiple_of(m * 64, 64), 64)]
        return remote(src, dst, late_s.at[i], late_r.at[i], (xs, xo)[i % 2])

    my_rb = pl.ds(pl.multiple_of(c * 64, 64), 64)

    def rb_send(h):
        return remote(stage.at[1, h, LATE], rb.at[h, :, my_rb], rb_s.at[h], rb_r.at[h], pt)

    def late_unit(h):
        chunk = unit_chunk(xs_m, h, LATE)
        stage[0, h, LATE] = chunk
        rb[h, :, my_rb] = chunk
        stage[1, h, LATE] = unit_chunk(xo_m, h, LATE)
        rb_send(h).start()

    def run_unit(kind, h, j):
        owner = (pt_m, xs_m, xo_m)[kind]
        chunk = unit_chunk(owner, h, j)
        if kind == 0:
            if h == 1:
                kv_send(0, 0, j).wait_send()
            stage_p[j] = chunk
        else:
            stage[kind - 1, h, j] = chunk
        kv_send(kind, h, j).start()

    def own_unit(h):
        def body(j, carry):
            kv[h, pl.ds(pl.multiple_of(j * CH, CH), CH), pl.ds(pl.multiple_of(m * 64, 64), 64)] = unit_chunk(m, h, j)
            return carry
        lax.fori_loop(0, NCH, body, 0)

    def loop_unit(kind, h):
        def body(j, carry):
            run_unit(kind, h, j)
            return carry
        lax.fori_loop(0, NCH if kind == 0 else LATE, body, 0)

    forward_x(0)
    own_unit(0)
    s1.wait()
    sel_b[...] = (sel_b[...].astype(F32) + sel_r1[...].astype(F32)).astype(BF16)
    half = pl.ds(pl.multiple_of(c * 32, 32), 32)
    s2 = remote(normed.at[half], sel_r2, sel_s.at[1], sel_r.at[1], xs)
    s2.start()
    own_unit(1)
    forward_x(1)
    forward_y(0)
    wp.wait_recv()
    loop_unit(0, 0)
    forward_x(2)
    forward_y(1)
    loop_unit(1, 0)
    for r in range(2):
        wfx(r).wait_recv()
        wfy(r).wait_recv()
    loop_unit(2, 0)
    late_unit(0)
    forward_x(3)
    forward_y(2)
    loop_unit(0, 1)

    s2.wait()
    hid[half, :] = (normed[half, :].astype(F32) + sel_r2[...].astype(F32)).astype(BF16)
    s3 = remote(hid.at[half], hid.at[half], sel_s.at[2], sel_r.at[2], pt)
    s3.start()
    forward_y(3)
    s3.wait()
    load_t.wait()

    def norm_rows(src, gain):
        v = src.astype(F32)
        inv = lax.rsqrt(jnp.mean(v * v, axis=-1, keepdims=True) + 1e-5)
        return (v * inv * gain).astype(BF16)

    def norm_hid(i, carry):
        rows = pl.ds(pl.multiple_of(i * 32, 32), 32)
        normed[rows, :] = norm_rows(hid[rows, :], gain_a)
        return carry

    lax.fori_loop(0, 4, norm_hid, 0)
    load_q.wait()
    q_buf[...] = jnp.zeros_like(q_buf)
    k_buf[...] = jnp.zeros_like(k_buf)
    v_buf[...] = jnp.zeros_like(v_buf)

    def pick(b, carry):
        pos = jnp.clip(lens[b], 1, 128)
        for i in range(2):
            rot[i, pl.ds(b, 1), :] = tab[i, pl.ds(pos - 1, 1), :]
            rot[i, pl.ds(NB + b, 1), :] = tab[i, pl.ds(pos, 1), :]
        return carry

    lax.fori_loop(0, NB, pick, 0)

    def turn(a, ct, st):
        return (a * ct + pltpu.roll(a, HEAD_DIM // 2, 1) * st).astype(BF16).astype(F32)

    for pair in range(3):
        qs = dot32(normed[...], buf_c[:, pair * 256:(pair + 1) * 256])
        for i in range(2):
            hd = pair * 2 + i
            q_h = turn(qs[:, i * HEAD_DIM:(i + 1) * HEAD_DIM], rot[0], rot[1])
            for t in range(2):
                q_buf[pl.ds(t * 8 + hd, NB, stride=16), :] = q_h[t * NB:(t + 1) * NB]
    toks = normed[NB:2 * NB, :]
    k_new = dot32(toks, buf_b[:, pl.ds(pl.multiple_of(m * 512, 256), 256)])
    v_new = dot32(toks, buf_b[:, pl.ds(pl.multiple_of(m * 512 + 256, 256), 256)])
    for g in range(2):
        cols = slice(g * HEAD_DIM, (g + 1) * HEAD_DIM)
        k_g = turn(k_new[:, cols], rot[0, NB:, :], rot[1, NB:, :])
        v_g = v_new[:, cols].astype(BF16).astype(F32)
        flat[pl.ds(g, NB, stride=2), :] = k_g
        flat[pl.ds(2 * NB + g, NB, stride=2), :] = v_g
        for i in range(3):
            rows = pl.ds(8 + 3 * g + i, NB, stride=16)
            k_buf[rows, :] = k_g
            v_buf[rows, :] = v_g
    knv[0] = flat[0:2 * NB, :].astype(BF16)
    knv[1] = flat[2 * NB:4 * NB, :].astype(BF16)

    qb[...] = q_buf[LATE * CH * 16:, :].astype(BF16)
    q_msg = remote(qb, qb_r, qp_s.at[0], qp_r.at[0], xs)
    q_msg.start()

    for r in range(2, WCH):
        wfx(r).wait_recv()
        wfy(r).wait_recv()

    def last_units(j, carry):
        run_unit(1, 1, j)
        run_unit(2, 1, j)
        return carry

    lax.fori_loop(0, LATE, last_units, 0)
    late_unit(1)
    wp.wait_send()
    for r in range(WCH):
        wx(r).wait_send()
        wfx(r).wait_send()
        wy(r).wait_send()
        wfy(r).wait_send()
    load_g.start()
    load_d.start()

    r_io = lax.broadcasted_iota(jnp.int32, (16, 256), 0)
    c_io = lax.broadcasted_iota(jnp.int32, (16, 256), 1)
    same = ((r_io & 7) >= 3) == ((c_io & 1) == 1)
    k_pos = c_io >> 1
    is_new = lax.broadcasted_iota(jnp.int32, (16, 1), 0) >= 8
    scale = HEAD_DIM ** -0.5

    def score(b):
        rows = pl.ds(pl.multiple_of(b * 16, 16), 16)
        q = q_buf[rows, :]
        s = lax.dot_general(q.astype(BF16), kv[0, b], (((1,), (1,)), ((), ())), preferred_element_type=F32) * scale
        s = jnp.where(same & (k_pos < lens[b]), s, NEG_BIG)
        s_new = jnp.where(is_new, jnp.sum(q * k_buf[rows, :], axis=-1, keepdims=True) * scale, NEG_BIG)
        top = jnp.maximum(jnp.max(s, axis=-1, keepdims=True), s_new)
        p = jnp.exp(s - top)
        p_new = jnp.exp(s_new - top)
        inv = 1.0 / (jnp.sum(p, axis=-1, keepdims=True) + p_new)
        p_buf[rows, :] = (p * inv).astype(BF16)
        a_buf[rows, :] = (p_new * inv) * v_buf[rows, :]

    def score_four(i, carry):
        for t in range(4):
            score(i * 4 + t)
        return carry

    def weigh_eight(i, carry):
        for t in range(8):
            b = i * 8 + t
            rows = pl.ds(pl.multiple_of(b * 16, 16), 16)
            a_buf[rows, :] = a_buf[rows, :] + dot32(p_buf[rows, :], kv[1, b])
        return carry

    def store_kv(h, g):
        rows = pl.ds(pl.multiple_of(g * 2064, 2064), 2064)
        return pltpu.make_async_copy(o_buf.at[h, pl.ds(0, 2064)], (o_k, o_v)[h].at[rows], st_sem.at[h])

    def lay_out(h):
        def body(g, carry):
            @pl.when(g > 0)
            def _():
                store_kv(h, g - 1).wait()
            for t in range(8):
                o_buf[h, t * 258:t * 258 + 256, :] = kv[h, g * 8 + t]
            new = knv[h, pl.ds(pl.multiple_of(g * 16, 16), 16), :]
            for t in range(8):
                o_buf[h, t * 258 + 256:t * 258 + 258, :] = new[2 * t:2 * t + 2]
            store_kv(h, g).start()
            return carry
        return body

    c_half = lax.broadcasted_iota(jnp.int32, (16, 128), 1)
    r_half = lax.broadcasted_iota(jnp.int32, (16, 128), 0)
    same_half = ((r_half & 7) >= 3) == ((c_half & 1) == 1)
    pos_half = x * 64 + (c_half >> 1)
    on_diag = c_half == r_half
    chip_rows = pl.ds(pl.multiple_of(x * 128, 128), 128)

    def partial_scores(q, keys, b):
        s = lax.dot_general(q, keys, (((1,), (1,)), ((), ())), preferred_element_type=F32) * scale
        return jnp.where(same_half & (pos_half < lens[b]), s, NEG_BIG)

    def late_local(p):
        b = LATE * CH + p
        rows = pl.ds(pl.multiple_of(b * 16, 16), 16)
        out = pl.ds(pl.multiple_of(p * 16, 16), 16)
        q = q_buf[rows, :]
        s = partial_scores(q.astype(BF16), kv[0, b, chip_rows, :], b)
        s_new = jnp.where(is_new, jnp.sum(q * k_buf[rows, :], axis=-1, keepdims=True) * scale, NEG_BIG)
        top = jnp.maximum(jnp.max(s, axis=-1, keepdims=True), s_new)
        w = jnp.exp(s - top)
        w_new = jnp.exp(s_new - top)
        m_buf[out, :] = jnp.broadcast_to(top, (16, HEAD_DIM))
        l_buf[out, :] = jnp.broadcast_to(jnp.sum(w, axis=-1, keepdims=True) + w_new, (16, HEAD_DIM))
        a_buf[rows, :] = dot32(w.astype(BF16), kv[1, b, chip_rows, :]) + w_new * v_buf[rows, :]

    def late_peer(p):
        out = pl.ds(pl.multiple_of(p * 16, 16), 16)
        s = partial_scores(qb_r[out, :], rb[0, p], LATE * CH + p)
        top = jnp.max(s, axis=-1, keepdims=True)
        w = jnp.exp(s - top)
        acc = dot32(w.astype(BF16), rb[1, p])
        tops = jnp.sum(jnp.where(on_diag, top, 0.0), axis=0, keepdims=True)
        sums = jnp.sum(jnp.where(on_diag, jnp.sum(w, axis=-1, keepdims=True), 0.0), axis=0, keepdims=True)
        pb[out, :] = jnp.where(r_half == 6, tops, jnp.where(r_half == 7, sums, acc))

    def late_merge(p):
        rows = pl.ds(pl.multiple_of((LATE * CH + p) * 16, 16), 16)
        out = pl.ds(pl.multiple_of(p * 16, 16), 16)
        other = pb_r[out, :]
        o_top = jnp.sum(jnp.where(on_diag, other[6:7, :], 0.0), axis=-1, keepdims=True)
        o_sum = jnp.sum(jnp.where(on_diag, other[7:8, :], 0.0), axis=-1, keepdims=True)
        top = jnp.maximum(m_buf[out, :], o_top)
        w, o_w = jnp.exp(m_buf[out, :] - top), jnp.exp(o_top - top)
        a_buf[rows, :] = (a_buf[rows, :] * w + other * o_w) / (l_buf[out, :] * w + o_sum * o_w)

    def by_four(f):
        def body(i, carry):
            for t in range(4):
                f(i * 4 + t)
            return carry
        lax.fori_loop(0, CH // 4, body, 0)

    for j in range(LATE):
        for kind in range(3):
            kv_send(kind, 0, j).wait_recv()
        lax.fori_loop(j * (CH // 4), (j + 1) * (CH // 4), score_four, 0)
        lax.fori_loop(j * (CH // 8), (j + 1) * (CH // 8), lay_out(0), 0)
    for h in range(2):
        kv_send(0, h, LATE).wait_recv()
        rb_send(h).wait_recv()
    by_four(late_local)
    q_msg.wait_recv()
    by_four(late_peer)
    p_msg = remote(pb, pb_r, qp_s.at[1], qp_r.at[1], xs)
    p_msg.start()
    for i in range(N_GAP):
        late_send(i).start()

    for j in range(LATE):
        for kind in range(3):
            kv_send(kind, 1, j).wait_recv()
        lax.fori_loop(j * (CH // 8), (j + 1) * (CH // 8), weigh_eight, 0)
        if j < LATE - 1:
            lax.fori_loop(j * (CH // 8), (j + 1) * (CH // 8), lay_out(1), 0)
    p_msg.wait_recv()
    by_four(late_merge)

    for hd in range(6):
        for t in range(2):
            att[t * NB:(t + 1) * NB, hd * HEAD_DIM:(hd + 1) * HEAD_DIM] = a_buf[pl.ds(t * 8 + hd, NB, stride=16), :].astype(BF16)
    ot_half = pl.ds(pl.multiple_of((1 - c) * 64, 64), 64)
    mine = pl.ds(pl.multiple_of(c * 64 + x * 32, 32), 32)
    away = pl.ds(pl.multiple_of(c * 64 + (1 - x) * 32, 32), 32)
    mine_r1 = pl.ds(pl.multiple_of(x * 32, 32), 32)
    away_r1 = pl.ds(pl.multiple_of((1 - x) * 32, 32), 32)

    def reduce_all(k, produce, after, last, resid, buf):
        def msg(step, i, src, dst, dev):
            return remote(src, dst, ar_s.at[k, step, i], ar_r.at[k, step, i], dev)

        cols = [pl.ds(i * QW, QW) for i in range(4)]
        a1 = [msg(0, i, part.at[ot_half, cols[i]], r1.at[:, cols[i]], pt) for i in range(4)]
        a2 = [msg(1, i, part.at[away, cols[i]], r2.at[:, cols[i]], xs) for i in range(4)]
        a3 = [msg(2, i, buf.at[mine, cols[i]], buf.at[mine, cols[i]], xs) for i in range(4)]
        a4 = [msg(3, i, buf.at[mine, cols[i]], buf.at[mine, cols[i]], pt) for i in range(4)]
        a5 = [msg(4, i, buf.at[away, cols[i]], buf.at[away, cols[i]], pt) for i in range(4)]

        def over_x(i):
            a1[i].wait_recv()
            part[away, cols[i]] = part[away, cols[i]] + r1[away_r1, cols[i]]
            a2[i].start()
            part[mine, cols[i]] = part[mine, cols[i]] + r1[mine_r1, cols[i]]

        for i in range(4):
            produce(i)
            a1[i].start()
            if i:
                over_x(i - 1)
        over_x(3)
        after()
        for i in range(4):
            a2[i].wait_recv()
            total = part[mine, cols[i]] + r2[:, cols[i]]
            buf[mine, cols[i]] = (resid[mine, cols[i]].astype(F32) + total).astype(BF16)
            a3[i].start()
            a4[i].start()
        last()
        for i in range(4):
            a3[i].wait_recv()
            a5[i].start()
        for i in range(4):
            a4[i].wait_recv()
            a5[i].wait_recv()
        for step in (a1, a2, a3, a4, a5):
            for i in range(4):
                step[i].wait_send()

    def w_o_cols(i):
        load_o(i).wait()
        part[:, i * QW:(i + 1) * QW] = dot32(att[...], buf_c[i * QW:(i + 1) * QW, QW:2 * QW])

    def after_w_o():
        load_u.start()
        lax.fori_loop((LATE - 1) * (CH // 8), LATE * (CH // 8), lay_out(1), 0)

    def send_late():
        for i in range(N_GAP, 8):
            late_send(i).start()

    def keep_late():
        for i in range(8):
            late_send(i).wait_recv()
        for h in range(2):
            lax.fori_loop(LATE * (CH // 8), NB // 8, lay_out(h), 0)

    reduce_all(0, w_o_cols, after_w_o, send_late, hid, x2)
    gain_m = g_mlp[...].astype(F32)

    def norm_x2(i, carry):
        rows = pl.ds(pl.multiple_of(i * 32, 32), 32)
        normed[rows, :] = norm_rows(x2[rows, :], gain_m)
        return carry

    lax.fori_loop(0, 4, norm_x2, 0)
    load_g.wait()
    load_u.wait()

    def mlp_cols(i, carry):
        cols = pl.ds(pl.multiple_of(i * 256, 256), 256)
        gate = dot32(normed[...], buf_b[:, cols])
        up = dot32(normed[...], buf_c[:, cols])
        mid[:, cols] = (gate * (1.0 / (1.0 + jnp.exp(-gate))) * up).astype(BF16)
        return carry

    lax.fori_loop(0, FF // 256, mlp_cols, 0)
    load_d.wait()

    def down_cols(i):
        def body(t, carry):
            cols = pl.ds(pl.multiple_of(i * QW + t * 256, 256), 256)
            part[:, cols] = dot32(mid[...], buf_a[:, cols])
            return carry
        lax.fori_loop(0, QW // 256, body, 0)

    reduce_all(1, down_cols, keep_late, lambda: None, x2, hid)
    st_last = pltpu.make_async_copy(hid.at[pl.ds(0, NB)], o_last, st_sem.at[2])
    st_dec = pltpu.make_async_copy(hid.at[pl.ds(NB, NB)], o_dec, st_sem.at[3])
    st_last.start()
    st_dec.start()

    for kind in range(3):
        for tn in range(2):
            for j in range(NCH if kind == 0 else LATE):
                if kind or tn:
                    kv_send(kind, tn, j).wait_send()
    for i in range(8):
        late_send(i).wait_send()
    for h in range(2):
        rb_send(h).wait_send()
    q_msg.wait_send()
    p_msg.wait_send()
    for h in range(2):
        store_kv(h, NB // 8 - 1).wait()
    st_last.wait()
    st_dec.wait()


def copy_out(k_in, v_in, last_in, dec_in, k_out, v_out, last_out, dec_out, k_buf, v_buf, last_buf, dec_buf, rd, wr):
    step = 8 * 258
    moves = []
    for i in range(NB // 8):
        rows = pl.ds(i * step, step)
        for src, buf, dst in ((k_in, k_buf, k_out), (v_in, v_buf, v_out)):
            moves.append((src.at[rows], buf.at[rows], dst.at[rows]))
    moves.append((last_in, last_buf, last_out))
    moves.append((dec_in, dec_buf, dec_out))
    reads = [pltpu.make_async_copy(a, b, rd.at[i]) for i, (a, b, _) in enumerate(moves)]
    writes = [pltpu.make_async_copy(b, c, wr.at[i]) for i, (_, b, c) in enumerate(moves)]
    for r in reads:
        r.start()
    for r, w in zip(reads, writes):
        r.wait()
        w.start()
    for w in writes:
        w.wait()


def solution(mesh):
    seq_spec = P('replica', 'model', None)
    col_spec = P(None, None, 'model')
    row_spec = P(None, 'model', None)
    gain_spec = P(None, None)
    tok_spec = P('replica', None)
    cache_spec = P(None, 'replica', None, 'model', None)
    in_specs = (seq_spec, P('replica'), tok_spec, gain_spec, col_spec, col_spec, col_spec, row_spec, gain_spec, col_spec, col_spec, row_spec)
    out_specs = (tok_spec, tok_spec, cache_spec, cache_spec)

    def per_device(prompt, lengths, new_tok, norm_attn, w_q, w_k, w_v, w_o, norm_mlp, w_gate, w_up, w_down):
        tab = jnp.asarray(rotate_tables(136))
        vmem = pl.BlockSpec(memory_space=pltpu.VMEM)
        hbm = pl.BlockSpec(memory_space=pl.ANY)
        smem = pl.BlockSpec(memory_space=pltpu.SMEM)
        dma = pltpu.SemaphoreType.DMA
        o_last, o_dec, o_k, o_v = pl.pallas_call(
            kernel,
            out_shape=(jax.ShapeDtypeStruct((NB, D), BF16),) * 2 + (jax.ShapeDtypeStruct((NB * 258, HEAD_DIM), BF16),) * 2,
            in_specs=[smem] + [vmem] * 3 + [hbm] * 9,
            out_specs=(hbm,) * 4,
            scratch_shapes=[
                pltpu.VMEM((NB * SEQ_LOC, D), BF16),
                pltpu.VMEM((D, FF), BF16),
                pltpu.VMEM((D, FF), BF16),
                pltpu.VMEM((2, NB, 256, HEAD_DIM), BF16),
                pltpu.VMEM((2, 2, NCH, CH, 64, HEAD_DIM), BF16),
                pltpu.VMEM((NCH, CH, 64, HEAD_DIM), BF16),
                pltpu.VMEM((2 * ROWS, HEAD_DIM), F32),
                pltpu.VMEM((NB * 16, HEAD_DIM), F32),
                pltpu.VMEM((NB * 16, HEAD_DIM), F32),
                pltpu.VMEM((NB * 16, HEAD_DIM), F32),
                pltpu.VMEM((NB * 16, HEAD_DIM), F32),
                pltpu.VMEM((2 * NB, QW), BF16),
                pltpu.VMEM((NB, D), BF16),
                pltpu.VMEM((32, D), BF16),
                pltpu.VMEM((2 * NB, D), BF16),
                pltpu.VMEM((2 * NB, D), BF16),
                pltpu.VMEM((2 * NB, D), F32),
                pltpu.VMEM((NB, D), F32),
                pltpu.VMEM((32, D), F32),
                pltpu.VMEM((2 * NB, D), BF16),
                pltpu.VMEM((2 * NB, FF), BF16),
                pltpu.VMEM((NB * 16, 256), BF16),
                pltpu.VMEM((2, 2 * NB, HEAD_DIM), BF16),
                pltpu.VMEM((2, 2 * NB, HEAD_DIM), F32),
                pltpu.VMEM((2, 8 * 258 + 32, HEAD_DIM), BF16),
                pltpu.VMEM((2, CH, 128, HEAD_DIM), BF16),
                pltpu.VMEM((CH * 16, HEAD_DIM), BF16),
                pltpu.VMEM((CH * 16, HEAD_DIM), BF16),
                pltpu.VMEM((CH * 16, HEAD_DIM), F32),
                pltpu.VMEM((CH * 16, HEAD_DIM), F32),
                pltpu.VMEM((CH * 16, HEAD_DIM), F32),
                pltpu.VMEM((CH * 16, HEAD_DIM), F32),
                dma((NCH,)), dma((2,)), dma((9,)), dma((4,)),
                dma, dma, dma((WCH,)), dma((WCH,)), dma((WCH,)), dma((WCH,)),
                dma((WCH,)), dma((WCH,)), dma((WCH,)), dma((WCH,)),
                dma((3,)), dma((3,)), dma((3, 2, NCH)), dma((3, 2, NCH)), dma((2, 5, 4)), dma((2, 5, 4)),
                dma((2,)), dma((2,)), dma((8,)), dma((8,)), dma((2,)), dma((2,)),
            ],
            compiler_params=pltpu.CompilerParams(collective_id=0, has_side_effects=True, vmem_limit_bytes=67043328),
            name="layer",
        )(lengths, tab, norm_attn, norm_mlp, new_tok,
          prompt.reshape(NB * SEQ_LOC, D), w_q[0], w_k[0], w_v[0], w_o[0], w_gate[0], w_up[0], w_down[0])
        rows, slots = jax.ShapeDtypeStruct((NB, D), BF16), jax.ShapeDtypeStruct((NB * 258, HEAD_DIM), BF16)
        n_moves = 2 * (NB // 8) + 2
        o_k, o_v, o_last, o_dec = pl.pallas_call(
            copy_out,
            out_shape=(slots, slots, rows, rows),
            in_specs=[hbm] * 4,
            out_specs=(hbm,) * 4,
            scratch_shapes=[pltpu.VMEM(slots.shape, BF16), pltpu.VMEM(slots.shape, BF16), pltpu.VMEM(rows.shape, BF16),
                            pltpu.VMEM(rows.shape, BF16), dma((n_moves,)), dma((n_moves,))],
            compiler_params=pltpu.CompilerParams(vmem_limit_bytes=60 * 1024 * 1024),
            name="copy_out",
        )(o_k, o_v, o_last, o_dec)
        caches = [o.reshape(1, NB, 129, 2, HEAD_DIM) for o in (o_k, o_v)]
        return o_dec, o_last, caches[0], caches[1]

    return jax.shard_map(per_device, mesh=mesh, in_specs=in_specs, out_specs=out_specs, check_vma=False)
```

```python
import functools

import jax
import jax.numpy as jnp
import numpy as np
from jax import lax
from jax.experimental import pallas as pl
from jax.experimental.pallas import tpu as pltpu
from jax.sharding import PartitionSpec as P

HEAD_DIM = 128
NEG_BIG = -1e30
MESH = pl.DeviceIdType.MESH
F32 = jnp.float32
BF16 = jnp.bfloat16

NB = 64
SEQ_LOC = 32
D = 3072
FF = 2048
QW = 768
CH = 16
NCH = NB // CH
ROWS = CH * SEQ_LOC
VMEM_LAYER = 67043328 - (10 << 20)
LATE = NCH - 1
N_GAP = 3
WCH = 4
WROWS = D // WCH


def dot32(lhs, rhs):
    return jnp.dot(lhs, rhs, preferred_element_type=F32)


def rotate_tables(n):
    half = HEAD_DIM // 2
    inv_freq = np.float32(10000.0) ** (np.float32(-2.0) * np.arange(half, dtype=np.float32) / np.float32(HEAD_DIM))
    angles = (np.arange(n, dtype=np.float32)[:, None] * inv_freq).astype(np.float32).astype(np.float64)
    cos_tab, sin_tab = np.cos(angles), np.sin(angles)
    return np.stack([np.concatenate([cos_tab, cos_tab], 1), np.concatenate([-sin_tab, sin_tab], 1)]).astype(np.float32)


def kernel(lens, tab, g_attn, g_mlp,
           new_tok, prompt, w_q, w_k, w_v, w_o, w_g, w_u, w_d,
           kv, knv, hid,
           buf_a, buf_b, buf_c, stage, stage_p, flat, q_buf, k_buf, v_buf, a_buf, att,
           sel_r1, sel_r2, normed, part, r1, r2, x2, mid, p_buf, rot,
           rb, qb, qb_r, m_buf, l_buf, pb, pb_r,
           ld_p, ld_w, ld_big,
           wp_s, wp_r, wx_s, wx_r, wfx_s, wfx_r, wy_s, wy_r, wfy_s, wfy_r,
           sel_s, sel_r, kv_s, kv_r, ar_s, ar_r, rb_s, rb_r, late_s, late_r, qp_s, qp_r):
    y = lax.axis_index("replica")
    m = lax.axis_index("model")
    c = lax.rem(m, 2)
    x = m // 2
    xs_m = lax.rem(m + 2, 4)
    xo_m = 3 - m
    pt_m = m + 1 - 2 * c
    xs, xo, pt, yp = (y, xs_m), (y, xo_m), (y, pt_m), (1 - y, m)

    def remote(src, dst, ssem, rsem, dev):
        return pltpu.make_async_remote_copy(src_ref=src, dst_ref=dst, send_sem=ssem, recv_sem=rsem,
                                            device_id=dev, device_id_type=MESH)

    def load_w(i):
        src = (w_k, w_v)[i]
        return pltpu.make_async_copy(src, buf_b.at[:, pl.ds(pl.multiple_of(m * 512 + i * 256, 256), 256)], ld_w.at[i])

    def load_p(j):
        r = pl.ds(pl.multiple_of(j * ROWS, ROWS), ROWS)
        return pltpu.make_async_copy(prompt.at[r], buf_a.at[r], ld_p.at[j])

    for i in range(2):
        load_w(i).start()
    for j in range(NCH):
        load_p(j).start()
    load_q = pltpu.make_async_copy(w_q, buf_c.at[:, pl.ds(0, QW)], ld_big.at[0])
    load_q.start()
    load_t = pltpu.make_async_copy(new_tok, hid.at[pl.ds(NB, NB)], ld_big.at[8])
    load_t.start()

    def load_o(i):
        return pltpu.make_async_copy(w_o.at[:, pl.ds(i * QW, QW)], buf_c.at[pl.ds(i * QW, QW), pl.ds(QW, QW)], ld_big.at[1 + i])

    for i in range(4):
        load_o(i).start()
    load_g = pltpu.make_async_copy(w_g, buf_b, ld_big.at[5])
    load_u = pltpu.make_async_copy(w_u, buf_c, ld_big.at[6])
    load_d = pltpu.make_async_copy(w_d, buf_a, ld_big.at[7])

    barrier = pltpu.get_barrier_semaphore()
    for dev in (xs, xo, pt, yp):
        pl.semaphore_signal(barrier, inc=1, device_id=dev, device_id_type=MESH)
    pl.semaphore_wait(barrier, 4)

    def w_ref(owner, half, r):
        rows = pl.ds(pl.multiple_of(half * (D // 2) + (r % 2) * WROWS, WROWS), WROWS)
        return buf_b.at[rows, pl.ds(pl.multiple_of(owner * 512 + (r // 2) * 256, 256), 256)]

    def wx(r):
        ref = w_ref(m, y, r)
        return remote(ref, ref, wx_s.at[r], wx_r.at[r], xs)

    def wfx(r):
        ref = w_ref(xs_m, y, r)
        return remote(ref, ref, wfx_s.at[r], wfx_r.at[r], pt)

    def wy(r):
        ref = w_ref(xs_m, y, r)
        return remote(ref, ref, wy_s.at[r], wy_r.at[r], yp)

    def wfy(r):
        ref = w_ref(xs_m, 1 - y, r)
        return remote(ref, ref, wfy_s.at[r], wfy_r.at[r], pt)

    own = buf_b.at[:, pl.ds(pl.multiple_of(m * 512, 512), 512)]
    wp = remote(own, own, wp_s, wp_r, pt)
    for i in range(2):
        load_w(i).wait()
    for r in range(WCH):
        wx(r).start()
    wp.start()

    def forward_x(r):
        wx(r).wait_recv()
        wfx(r).start()
        wy(r).start()

    def forward_y(r):
        wy(r).wait_recv()
        wfy(r).start()

    gain_a = g_attn[...].astype(F32)
    row_iota = lax.broadcasted_iota(jnp.int32, (SEQ_LOC, 1), 0)

    def norm_prompts(i, carry):
        parts = []
        for t in range(8):
            b = i * 8 + t
            rows = pl.ds(pl.multiple_of(b * SEQ_LOC, SEQ_LOC), SEQ_LOC)
            v = buf_a[rows, :].astype(F32)
            inv = lax.rsqrt(jnp.mean(v * v, axis=-1, keepdims=True) + 1e-5)
            hit = row_iota == lens[b] - 1 - m * SEQ_LOC
            parts.append(jnp.sum(jnp.where(hit, v, 0.0), axis=0, keepdims=True))
            buf_a[rows, :] = (buf_a[rows, :].astype(F32) * inv * gain_a).astype(BF16)
        part[pl.ds(pl.multiple_of(i * 8, 8), 8), :] = jnp.concatenate(parts, axis=0)
        return carry

    per = CH // 8
    for j in range(NCH):
        load_p(j).wait()
        lax.fori_loop(j * per, (j + 1) * per, norm_prompts, 0)

    sel_b = normed.at[pl.ds(0, NB)]
    sel_b[...] = part[0:NB, :].astype(BF16)
    s1 = remote(sel_b, sel_r1, sel_s.at[0], sel_r.at[0], pt)
    s1.start()

    def unit_chunk(owner, h, j):
        col = pl.ds(pl.multiple_of(owner * 512 + h * 256, 256), 256)
        acc = dot32(buf_a[pl.ds(pl.multiple_of(j * ROWS, ROWS), ROWS), :], buf_b[:, col])
        here = pl.ds(pl.multiple_of(m * SEQ_LOC, SEQ_LOC), SEQ_LOC)
        for hd in range(2):
            a = acc[:, hd * HEAD_DIM:(hd + 1) * HEAD_DIM]
            if h == 0:
                turned = pltpu.roll(a, HEAD_DIM // 2, 1).reshape(CH, SEQ_LOC, HEAD_DIM)
                a = a.reshape(CH, SEQ_LOC, HEAD_DIM) * tab[0, here, :][None] + turned * tab[1, here, :][None]
                a = a.reshape(ROWS, HEAD_DIM)
            flat[pl.ds(hd, ROWS, stride=2), :] = a
        return flat[...].astype(BF16).reshape(CH, 2 * SEQ_LOC, HEAD_DIM)

    def kv_ref(h, j):
        return kv.at[h, pl.ds(pl.multiple_of(j * CH, CH), CH), pl.ds(pl.multiple_of(m * 64, 64), 64)]

    def kv_send(kind, h, j):
        dev = (pt, xs, xo)[kind]
        return remote(stage_p.at[j] if kind == 0 else stage.at[kind - 1, h, j], kv_ref(h, j), kv_s.at[kind, h, j], kv_r.at[kind, h, j], dev)

    def late_send(i):
        kind, h, part8 = 1 + i % 2, (i // 2) % 2, i // 4
        src = stage.at[kind - 1, h, LATE, pl.ds(part8 * 8, 8)]
        dst = kv.at[h, pl.ds(LATE * CH + part8 * 8, 8), pl.ds(pl.multiple_of(m * 64, 64), 64)]
        return remote(src, dst, late_s.at[i], late_r.at[i], (xs, xo)[i % 2])

    my_rb = pl.ds(pl.multiple_of(c * 64, 64), 64)

    def rb_send(h):
        return remote(stage.at[1, h, LATE], rb.at[h, :, my_rb], rb_s.at[h], rb_r.at[h], pt)

    def late_unit(h):
        chunk = unit_chunk(xs_m, h, LATE)
        stage[0, h, LATE] = chunk
        rb[h, :, my_rb] = chunk
        stage[1, h, LATE] = unit_chunk(xo_m, h, LATE)
        rb_send(h).start()

    def run_unit(kind, h, j):
        owner = (pt_m, xs_m, xo_m)[kind]
        chunk = unit_chunk(owner, h, j)
        if kind == 0:
            if h == 1:
                kv_send(0, 0, j).wait_send()
            stage_p[j] = chunk
        else:
            stage[kind - 1, h, j] = chunk
        kv_send(kind, h, j).start()

    def own_unit(h):
        def body(j, carry):
            kv[h, pl.ds(pl.multiple_of(j * CH, CH), CH), pl.ds(pl.multiple_of(m * 64, 64), 64)] = unit_chunk(m, h, j)
            return carry
        lax.fori_loop(0, NCH, body, 0)

    def loop_unit(kind, h):
        def body(j, carry):
            run_unit(kind, h, j)
            return carry
        lax.fori_loop(0, NCH if kind == 0 else LATE, body, 0)

    forward_x(0)
    own_unit(0)
    s1.wait()
    sel_b[...] = (sel_b[...].astype(F32) + sel_r1[...].astype(F32)).astype(BF16)
    half = pl.ds(pl.multiple_of(c * 32, 32), 32)
    s2 = remote(normed.at[half], sel_r2, sel_s.at[1], sel_r.at[1], xs)
    s2.start()
    own_unit(1)
    forward_x(1)
    forward_y(0)
    wp.wait_recv()
    loop_unit(0, 0)
    forward_x(2)
    forward_y(1)
    loop_unit(1, 0)
    for r in range(2):
        wfx(r).wait_recv()
        wfy(r).wait_recv()
    loop_unit(2, 0)
    late_unit(0)
    forward_x(3)
    forward_y(2)
    loop_unit(0, 1)

    s2.wait()
    hid[half, :] = (normed[half, :].astype(F32) + sel_r2[...].astype(F32)).astype(BF16)
    s3 = remote(hid.at[half], hid.at[half], sel_s.at[2], sel_r.at[2], pt)
    s3.start()
    forward_y(3)
    s3.wait()
    load_t.wait()

    def norm_rows(src, gain):
        v = src.astype(F32)
        inv = lax.rsqrt(jnp.mean(v * v, axis=-1, keepdims=True) + 1e-5)
        return (v * inv * gain).astype(BF16)

    def norm_hid(i, carry):
        rows = pl.ds(pl.multiple_of(i * 32, 32), 32)
        normed[rows, :] = norm_rows(hid[rows, :], gain_a)
        return carry

    lax.fori_loop(0, 4, norm_hid, 0)
    load_q.wait()
    q_buf[...] = jnp.zeros_like(q_buf)
    k_buf[...] = jnp.zeros_like(k_buf)
    v_buf[...] = jnp.zeros_like(v_buf)

    def pick(b, carry):
        pos = jnp.clip(lens[b], 1, 128)
        for i in range(2):
            rot[i, pl.ds(b, 1), :] = tab[i, pl.ds(pos - 1, 1), :]
            rot[i, pl.ds(NB + b, 1), :] = tab[i, pl.ds(pos, 1), :]
        return carry

    lax.fori_loop(0, NB, pick, 0)

    def turn(a, ct, st):
        return (a * ct + pltpu.roll(a, HEAD_DIM // 2, 1) * st).astype(BF16).astype(F32)

    for pair in range(3):
        qs = dot32(normed[...], buf_c[:, pair * 256:(pair + 1) * 256])
        for i in range(2):
            hd = pair * 2 + i
            q_h = turn(qs[:, i * HEAD_DIM:(i + 1) * HEAD_DIM], rot[0], rot[1])
            for t in range(2):
                q_buf[pl.ds(t * 8 + hd, NB, stride=16), :] = q_h[t * NB:(t + 1) * NB]
    toks = normed[NB:2 * NB, :]
    k_new = dot32(toks, buf_b[:, pl.ds(pl.multiple_of(m * 512, 256), 256)])
    v_new = dot32(toks, buf_b[:, pl.ds(pl.multiple_of(m * 512 + 256, 256), 256)])
    for g in range(2):
        cols = slice(g * HEAD_DIM, (g + 1) * HEAD_DIM)
        k_g = turn(k_new[:, cols], rot[0, NB:, :], rot[1, NB:, :])
        v_g = v_new[:, cols].astype(BF16).astype(F32)
        flat[pl.ds(g, NB, stride=2), :] = k_g
        flat[pl.ds(2 * NB + g, NB, stride=2), :] = v_g
        for i in range(3):
            rows = pl.ds(8 + 3 * g + i, NB, stride=16)
            k_buf[rows, :] = k_g
            v_buf[rows, :] = v_g
    knv[0] = flat[0:2 * NB, :].astype(BF16)
    knv[1] = flat[2 * NB:4 * NB, :].astype(BF16)

    qb[...] = q_buf[LATE * CH * 16:, :].astype(BF16)
    q_msg = remote(qb, qb_r, qp_s.at[0], qp_r.at[0], xs)
    q_msg.start()

    for r in range(2, WCH):
        wfx(r).wait_recv()
        wfy(r).wait_recv()

    def last_units(j, carry):
        run_unit(1, 1, j)
        run_unit(2, 1, j)
        return carry

    lax.fori_loop(0, LATE, last_units, 0)
    late_unit(1)
    wp.wait_send()
    for r in range(WCH):
        wx(r).wait_send()
        wfx(r).wait_send()
        wy(r).wait_send()
        wfy(r).wait_send()
    load_g.start()
    load_d.start()

    r_io = lax.broadcasted_iota(jnp.int32, (16, 256), 0)
    c_io = lax.broadcasted_iota(jnp.int32, (16, 256), 1)
    same = ((r_io & 7) >= 3) == ((c_io & 1) == 1)
    k_pos = c_io >> 1
    is_new = lax.broadcasted_iota(jnp.int32, (16, 1), 0) >= 8
    scale = HEAD_DIM ** -0.5

    def score(b):
        rows = pl.ds(pl.multiple_of(b * 16, 16), 16)
        q = q_buf[rows, :]
        s = lax.dot_general(q.astype(BF16), kv[0, b], (((1,), (1,)), ((), ())), preferred_element_type=F32) * scale
        s = jnp.where(same & (k_pos < lens[b]), s, NEG_BIG)
        s_new = jnp.where(is_new, jnp.sum(q * k_buf[rows, :], axis=-1, keepdims=True) * scale, NEG_BIG)
        top = jnp.maximum(jnp.max(s, axis=-1, keepdims=True), s_new)
        p = jnp.exp(s - top)
        p_new = jnp.exp(s_new - top)
        inv = 1.0 / (jnp.sum(p, axis=-1, keepdims=True) + p_new)
        p_buf[rows, :] = (p * inv).astype(BF16)
        a_buf[rows, :] = (p_new * inv) * v_buf[rows, :]

    def score_four(i, carry):
        for t in range(4):
            score(i * 4 + t)
        return carry

    def weigh_eight(i, carry):
        for t in range(8):
            b = i * 8 + t
            rows = pl.ds(pl.multiple_of(b * 16, 16), 16)
            a_buf[rows, :] = a_buf[rows, :] + dot32(p_buf[rows, :], kv[1, b])
        return carry

    c_half = lax.broadcasted_iota(jnp.int32, (16, 128), 1)
    r_half = lax.broadcasted_iota(jnp.int32, (16, 128), 0)
    same_half = ((r_half & 7) >= 3) == ((c_half & 1) == 1)
    pos_half = x * 64 + (c_half >> 1)
    on_diag = c_half == r_half
    chip_rows = pl.ds(pl.multiple_of(x * 128, 128), 128)

    def partial_scores(q, keys, b):
        s = lax.dot_general(q, keys, (((1,), (1,)), ((), ())), preferred_element_type=F32) * scale
        return jnp.where(same_half & (pos_half < lens[b]), s, NEG_BIG)

    def late_local(p):
        b = LATE * CH + p
        rows = pl.ds(pl.multiple_of(b * 16, 16), 16)
        out = pl.ds(pl.multiple_of(p * 16, 16), 16)
        q = q_buf[rows, :]
        s = partial_scores(q.astype(BF16), kv[0, b, chip_rows, :], b)
        s_new = jnp.where(is_new, jnp.sum(q * k_buf[rows, :], axis=-1, keepdims=True) * scale, NEG_BIG)
        top = jnp.maximum(jnp.max(s, axis=-1, keepdims=True), s_new)
        w = jnp.exp(s - top)
        w_new = jnp.exp(s_new - top)
        m_buf[out, :] = jnp.broadcast_to(top, (16, HEAD_DIM))
        l_buf[out, :] = jnp.broadcast_to(jnp.sum(w, axis=-1, keepdims=True) + w_new, (16, HEAD_DIM))
        a_buf[rows, :] = dot32(w.astype(BF16), kv[1, b, chip_rows, :]) + w_new * v_buf[rows, :]

    def late_peer(p):
        out = pl.ds(pl.multiple_of(p * 16, 16), 16)
        s = partial_scores(qb_r[out, :], rb[0, p], LATE * CH + p)
        top = jnp.max(s, axis=-1, keepdims=True)
        w = jnp.exp(s - top)
        acc = dot32(w.astype(BF16), rb[1, p])
        tops = jnp.sum(jnp.where(on_diag, top, 0.0), axis=0, keepdims=True)
        sums = jnp.sum(jnp.where(on_diag, jnp.sum(w, axis=-1, keepdims=True), 0.0), axis=0, keepdims=True)
        pb[out, :] = jnp.where(r_half == 6, tops, jnp.where(r_half == 7, sums, acc))

    def late_merge(p):
        rows = pl.ds(pl.multiple_of((LATE * CH + p) * 16, 16), 16)
        out = pl.ds(pl.multiple_of(p * 16, 16), 16)
        other = pb_r[out, :]
        o_top = jnp.sum(jnp.where(on_diag, other[6:7, :], 0.0), axis=-1, keepdims=True)
        o_sum = jnp.sum(jnp.where(on_diag, other[7:8, :], 0.0), axis=-1, keepdims=True)
        top = jnp.maximum(m_buf[out, :], o_top)
        w, o_w = jnp.exp(m_buf[out, :] - top), jnp.exp(o_top - top)
        a_buf[rows, :] = (a_buf[rows, :] * w + other * o_w) / (l_buf[out, :] * w + o_sum * o_w)

    def by_four(f):
        def body(i, carry):
            for t in range(4):
                f(i * 4 + t)
            return carry
        lax.fori_loop(0, CH // 4, body, 0)

    for j in range(LATE):
        for kind in range(3):
            kv_send(kind, 0, j).wait_recv()
        lax.fori_loop(j * (CH // 4), (j + 1) * (CH // 4), score_four, 0)
    for h in range(2):
        kv_send(0, h, LATE).wait_recv()
        rb_send(h).wait_recv()
    by_four(late_local)
    q_msg.wait_recv()
    by_four(late_peer)
    p_msg = remote(pb, pb_r, qp_s.at[1], qp_r.at[1], xs)
    p_msg.start()
    for i in range(N_GAP):
        late_send(i).start()

    for j in range(LATE):
        for kind in range(3):
            kv_send(kind, 1, j).wait_recv()
        lax.fori_loop(j * (CH // 8), (j + 1) * (CH // 8), weigh_eight, 0)
    p_msg.wait_recv()
    by_four(late_merge)

    for hd in range(6):
        for t in range(2):
            att[t * NB:(t + 1) * NB, hd * HEAD_DIM:(hd + 1) * HEAD_DIM] = a_buf[pl.ds(t * 8 + hd, NB, stride=16), :].astype(BF16)
    ot_half = pl.ds(pl.multiple_of((1 - c) * 64, 64), 64)
    mine = pl.ds(pl.multiple_of(c * 64 + x * 32, 32), 32)
    away = pl.ds(pl.multiple_of(c * 64 + (1 - x) * 32, 32), 32)
    mine_r1 = pl.ds(pl.multiple_of(x * 32, 32), 32)
    away_r1 = pl.ds(pl.multiple_of((1 - x) * 32, 32), 32)

    def reduce_all(k, produce, after, last, resid, buf):
        def msg(step, i, src, dst, dev):
            return remote(src, dst, ar_s.at[k, step, i], ar_r.at[k, step, i], dev)

        cols = [pl.ds(i * QW, QW) for i in range(4)]
        a1 = [msg(0, i, part.at[ot_half, cols[i]], r1.at[:, cols[i]], pt) for i in range(4)]
        a2 = [msg(1, i, part.at[away, cols[i]], r2.at[:, cols[i]], xs) for i in range(4)]
        a3 = [msg(2, i, buf.at[mine, cols[i]], buf.at[mine, cols[i]], xs) for i in range(4)]
        a4 = [msg(3, i, buf.at[mine, cols[i]], buf.at[mine, cols[i]], pt) for i in range(4)]
        a5 = [msg(4, i, buf.at[away, cols[i]], buf.at[away, cols[i]], pt) for i in range(4)]

        def over_x(i):
            a1[i].wait_recv()
            part[away, cols[i]] = part[away, cols[i]] + r1[away_r1, cols[i]]
            a2[i].start()
            part[mine, cols[i]] = part[mine, cols[i]] + r1[mine_r1, cols[i]]

        for i in range(4):
            produce(i)
            a1[i].start()
            if i:
                over_x(i - 1)
        over_x(3)
        after()
        for i in range(4):
            a2[i].wait_recv()
            total = part[mine, cols[i]] + r2[:, cols[i]]
            buf[mine, cols[i]] = (resid[mine, cols[i]].astype(F32) + total).astype(BF16)
            a3[i].start()
            a4[i].start()
        last()
        for i in range(4):
            a3[i].wait_recv()
            a5[i].start()
        for i in range(4):
            a4[i].wait_recv()
            a5[i].wait_recv()
        for step in (a1, a2, a3, a4, a5):
            for i in range(4):
                step[i].wait_send()

    def w_o_cols(i):
        load_o(i).wait()
        part[:, i * QW:(i + 1) * QW] = dot32(att[...], buf_c[i * QW:(i + 1) * QW, QW:2 * QW])

    def after_w_o():
        load_u.start()

    def send_late():
        for i in range(N_GAP, 8):
            late_send(i).start()

    def keep_late():
        for i in range(8):
            late_send(i).wait_recv()

    reduce_all(0, w_o_cols, after_w_o, send_late, hid, x2)
    gain_m = g_mlp[...].astype(F32)

    def norm_x2(i, carry):
        rows = pl.ds(pl.multiple_of(i * 32, 32), 32)
        normed[rows, :] = norm_rows(x2[rows, :], gain_m)
        return carry

    lax.fori_loop(0, 4, norm_x2, 0)
    load_g.wait()
    load_u.wait()

    def mlp_cols(i, carry):
        cols = pl.ds(pl.multiple_of(i * 256, 256), 256)
        gate = dot32(normed[...], buf_b[:, cols])
        up = dot32(normed[...], buf_c[:, cols])
        mid[:, cols] = (gate * (1.0 / (1.0 + jnp.exp(-gate))) * up).astype(BF16)
        return carry

    lax.fori_loop(0, FF // 256, mlp_cols, 0)
    load_d.wait()

    def down_cols(i):
        def body(t, carry):
            cols = pl.ds(pl.multiple_of(i * QW + t * 256, 256), 256)
            part[:, cols] = dot32(mid[...], buf_a[:, cols])
            return carry
        lax.fori_loop(0, QW // 256, body, 0)

    reduce_all(1, down_cols, keep_late, lambda: None, x2, hid)
    for kind in range(3):
        for tn in range(2):
            for j in range(NCH if kind == 0 else LATE):
                if kind or tn:
                    kv_send(kind, tn, j).wait_send()
    for i in range(8):
        late_send(i).wait_send()
    for h in range(2):
        rb_send(h).wait_send()
    q_msg.wait_send()
    p_msg.wait_send()


def copy_out(kv, knv, hid, k_out, v_out, last_out, dec_out, buf, sem, row_sem):
    rows = [pltpu.make_async_copy(hid.at[pl.ds(i * NB, NB)], dst, row_sem.at[i]) for i, dst in enumerate((last_out, dec_out))]
    for r in rows:
        r.start()

    def store(h, g):
        dst = pl.ds(pl.multiple_of(g * 2064, 2064), 2064)
        slot = lax.rem(g, 2)
        return pltpu.make_async_copy(buf.at[h, slot, pl.ds(0, 2064)], (k_out, v_out)[h].at[dst], sem.at[h, slot])

    def lay_out(g, carry):
        slot = lax.rem(g, 2)
        for h in range(2):
            @pl.when(g > 1)
            def _():
                store(h, g - 2).wait()
            for t in range(8):
                buf[h, slot, t * 258:t * 258 + 256, :] = kv[h, g * 8 + t]
            new = knv[h, pl.ds(pl.multiple_of(g * 16, 16), 16), :]
            for t in range(8):
                buf[h, slot, t * 258 + 256:t * 258 + 258, :] = new[2 * t:2 * t + 2]
            store(h, g).start()
        return carry

    lax.fori_loop(0, NB // 8, lay_out, 0)
    for g in range(NB // 8 - 2, NB // 8):
        for h in range(2):
            store(h, g).wait()
    for r in rows:
        r.wait()


def solution(mesh):
    seq_spec = P('replica', 'model', None)
    col_spec = P(None, None, 'model')
    row_spec = P(None, 'model', None)
    gain_spec = P(None, None)
    tok_spec = P('replica', None)
    cache_spec = P(None, 'replica', None, 'model', None)
    in_specs = (seq_spec, P('replica'), tok_spec, gain_spec, col_spec, col_spec, col_spec, row_spec, gain_spec, col_spec, col_spec, row_spec)
    out_specs = (tok_spec, tok_spec, cache_spec, cache_spec)

    def per_device(prompt, lengths, new_tok, norm_attn, w_q, w_k, w_v, w_o, norm_mlp, w_gate, w_up, w_down):
        tab = jnp.asarray(rotate_tables(136))
        vmem = pl.BlockSpec(memory_space=pltpu.VMEM)
        hbm = pl.BlockSpec(memory_space=pl.ANY)
        smem = pl.BlockSpec(memory_space=pltpu.SMEM)
        dma = pltpu.SemaphoreType.DMA
        kv, knv, hid = pl.pallas_call(
            kernel,
            out_shape=(pltpu.VMEM((2, NB, 256, HEAD_DIM), BF16), pltpu.VMEM((2, 2 * NB, HEAD_DIM), BF16), pltpu.VMEM((2 * NB, D), BF16)),
            in_specs=[smem] + [vmem] * 3 + [hbm] * 9,
            out_specs=(vmem,) * 3,
            scratch_shapes=[
                pltpu.VMEM((NB * SEQ_LOC, D), BF16),
                pltpu.VMEM((D, FF), BF16),
                pltpu.VMEM((D, FF), BF16),
                pltpu.VMEM((2, 2, NCH, CH, 64, HEAD_DIM), BF16),
                pltpu.VMEM((NCH, CH, 64, HEAD_DIM), BF16),
                pltpu.VMEM((2 * ROWS, HEAD_DIM), F32),
                pltpu.VMEM((NB * 16, HEAD_DIM), F32),
                pltpu.VMEM((NB * 16, HEAD_DIM), F32),
                pltpu.VMEM((NB * 16, HEAD_DIM), F32),
                pltpu.VMEM((NB * 16, HEAD_DIM), F32),
                pltpu.VMEM((2 * NB, QW), BF16),
                pltpu.VMEM((NB, D), BF16),
                pltpu.VMEM((32, D), BF16),
                pltpu.VMEM((2 * NB, D), BF16),
                pltpu.VMEM((2 * NB, D), F32),
                pltpu.VMEM((NB, D), F32),
                pltpu.VMEM((32, D), F32),
                pltpu.VMEM((2 * NB, D), BF16),
                pltpu.VMEM((2 * NB, FF), BF16),
                pltpu.VMEM((NB * 16, 256), BF16),
                pltpu.VMEM((2, 2 * NB, HEAD_DIM), F32),
                pltpu.VMEM((2, CH, 128, HEAD_DIM), BF16),
                pltpu.VMEM((CH * 16, HEAD_DIM), BF16),
                pltpu.VMEM((CH * 16, HEAD_DIM), BF16),
                pltpu.VMEM((CH * 16, HEAD_DIM), F32),
                pltpu.VMEM((CH * 16, HEAD_DIM), F32),
                pltpu.VMEM((CH * 16, HEAD_DIM), F32),
                pltpu.VMEM((CH * 16, HEAD_DIM), F32),
                dma((NCH,)), dma((2,)), dma((9,)),
                dma, dma, dma((WCH,)), dma((WCH,)), dma((WCH,)), dma((WCH,)),
                dma((WCH,)), dma((WCH,)), dma((WCH,)), dma((WCH,)),
                dma((3,)), dma((3,)), dma((3, 2, NCH)), dma((3, 2, NCH)), dma((2, 5, 4)), dma((2, 5, 4)),
                dma((2,)), dma((2,)), dma((8,)), dma((8,)), dma((2,)), dma((2,)),
            ],
            compiler_params=pltpu.CompilerParams(collective_id=0, has_side_effects=True, vmem_limit_bytes=VMEM_LAYER),
            name="layer",
        )(lengths, tab, norm_attn, norm_mlp, new_tok,
          prompt.reshape(NB * SEQ_LOC, D), w_q[0], w_k[0], w_v[0], w_o[0], w_gate[0], w_up[0], w_down[0])
        rows, slots = jax.ShapeDtypeStruct((NB, D), BF16), jax.ShapeDtypeStruct((NB * 258, HEAD_DIM), BF16)
        o_k, o_v, o_last, o_dec = pl.pallas_call(
            copy_out,
            out_shape=(slots, slots, rows, rows),
            in_specs=[vmem] * 3,
            out_specs=(hbm,) * 4,
            scratch_shapes=[pltpu.VMEM((2, 2, 8 * 258 + 32, HEAD_DIM), BF16), dma((2, 2)), dma((2,))],
            compiler_params=pltpu.CompilerParams(vmem_limit_bytes=40 << 20),
            name="copy_out",
        )(kv, knv, hid)
        caches = [o.reshape(1, NB, 129, 2, HEAD_DIM) for o in (o_k, o_v)]
        return o_dec, o_last, caches[0], caches[1]

    return jax.shard_map(per_device, mesh=mesh, in_specs=in_specs, out_specs=out_specs, check_vma=False)
```

```python
import functools

import jax
import jax.numpy as jnp
import numpy as np
from jax import lax
from jax.experimental import pallas as pl
from jax.experimental.pallas import tpu as pltpu
from jax.sharding import PartitionSpec as P

HEAD_DIM = 128
NEG_BIG = -1e30
MESH = pl.DeviceIdType.MESH
F32 = jnp.float32
BF16 = jnp.bfloat16

NB = 64
SEQ_LOC = 32
D = 3072
FF = 2048
QW = 768
CH = 16
NCH = NB // CH
ROWS = CH * SEQ_LOC
VMEM_LAYER = 67043328 - (10 << 20)
LATE = NCH - 1
N_LATE = 16
N_GAP = 4
N_MID = 1
WCH = 4
WROWS = D // WCH


def dot32(lhs, rhs):
    return jnp.dot(lhs, rhs, preferred_element_type=F32)


def rotate_tables(n):
    half = HEAD_DIM // 2
    inv_freq = np.float32(10000.0) ** (np.float32(-2.0) * np.arange(half, dtype=np.float32) / np.float32(HEAD_DIM))
    angles = (np.arange(n, dtype=np.float32)[:, None] * inv_freq).astype(np.float32).astype(np.float64)
    cos_tab, sin_tab = np.cos(angles), np.sin(angles)
    return np.stack([np.concatenate([cos_tab, cos_tab], 1), np.concatenate([-sin_tab, sin_tab], 1)]).astype(np.float32)


def kernel(lens, tab_in, g_attn_in, g_mlp_in,
           new_tok, prompt, w_q, w_k, w_v, w_o, w_g, w_u, w_d,
           kv, knv, hid,
           buf_a, buf_b, buf_c, stage, stage_p, flat, q_buf, k_buf, v_buf, a_buf, att,
           sel_r1, sel_r2, normed, part, r1, r2, x2, mid, p_buf, rot,
           tab, g_attn, g_mlp, rb, qb, qb_r, m_buf, l_buf, pb, pb_r,
           ld_p, ld_w, ld_big, ld_small,
           wp_s, wp_r, wx_s, wx_r, wfx_s, wfx_r, wy_s, wy_r, wfy_s, wfy_r,
           sel_s, sel_r, kv_s, kv_r, ar_s, ar_r, rb_s, rb_r, late_s, late_r, qp_s, qp_r):
    y = lax.axis_index("replica")
    m = lax.axis_index("model")
    c = lax.rem(m, 2)
    x = m // 2
    xs_m = lax.rem(m + 2, 4)
    xo_m = 3 - m
    pt_m = m + 1 - 2 * c
    xs, xo, pt, yp = (y, xs_m), (y, xo_m), (y, pt_m), (1 - y, m)

    def remote(src, dst, ssem, rsem, dev):
        return pltpu.make_async_remote_copy(src_ref=src, dst_ref=dst, send_sem=ssem, recv_sem=rsem,
                                            device_id=dev, device_id_type=MESH)

    def load_w(i):
        src = (w_k, w_v)[i]
        return pltpu.make_async_copy(src, buf_b.at[:, pl.ds(pl.multiple_of(m * 512 + i * 256, 256), 256)], ld_w.at[i])

    def load_p(j):
        r = pl.ds(pl.multiple_of(j * ROWS, ROWS), ROWS)
        return pltpu.make_async_copy(prompt.at[r], buf_a.at[r], ld_p.at[j])

    for i in range(2):
        load_w(i).start()
    for j in range(NCH):
        load_p(j).start()
    load_q = pltpu.make_async_copy(w_q, buf_c.at[:, pl.ds(0, QW)], ld_big.at[0])
    load_q.start()
    load_t = pltpu.make_async_copy(new_tok, hid.at[pl.ds(NB, NB)], ld_big.at[8])
    load_t.start()
    small = [pltpu.make_async_copy(src, dst, ld_small.at[i])
             for i, (src, dst) in enumerate(((tab_in, tab), (g_attn_in, g_attn), (g_mlp_in, g_mlp)))]
    for cp in small:
        cp.start()

    def load_o(i):
        return pltpu.make_async_copy(w_o.at[:, pl.ds(i * QW, QW)], buf_c.at[pl.ds(i * QW, QW), pl.ds(QW, QW)], ld_big.at[1 + i])

    for i in range(4):
        load_o(i).start()
    load_g = pltpu.make_async_copy(w_g, buf_b, ld_big.at[5])
    load_u = pltpu.make_async_copy(w_u, buf_c, ld_big.at[6])
    load_d = pltpu.make_async_copy(w_d, buf_a, ld_big.at[7])

    barrier = pltpu.get_barrier_semaphore()
    for dev in (xs, xo, pt, yp):
        pl.semaphore_signal(barrier, inc=1, device_id=dev, device_id_type=MESH)
    pl.semaphore_wait(barrier, 4)

    def w_ref(owner, half, r):
        rows = pl.ds(pl.multiple_of(half * (D // 2) + (r % 2) * WROWS, WROWS), WROWS)
        return buf_b.at[rows, pl.ds(pl.multiple_of(owner * 512 + (r // 2) * 256, 256), 256)]

    def wx(r):
        src = (w_k, w_v)[r // 2].at[pl.ds(pl.multiple_of(y * (D // 2) + (r % 2) * WROWS, WROWS), WROWS)]
        return remote(src, w_ref(m, y, r), wx_s.at[r], wx_r.at[r], xs)

    def wfx(r):
        ref = w_ref(xs_m, y, r)
        return remote(ref, ref, wfx_s.at[r], wfx_r.at[r], pt)

    def wy(r):
        ref = w_ref(xs_m, y, r)
        return remote(ref, ref, wy_s.at[r], wy_r.at[r], yp)

    def wfy(r):
        ref = w_ref(xs_m, 1 - y, r)
        return remote(ref, ref, wfy_s.at[r], wfy_r.at[r], pt)

    own = buf_b.at[:, pl.ds(pl.multiple_of(m * 512, 512), 512)]
    wp = remote(own, own, wp_s, wp_r, pt)
    for r in range(WCH):
        wx(r).start()
    for i in range(2):
        load_w(i).wait()
    wp.start()

    def forward_x(r):
        wx(r).wait_recv()
        wfx(r).start()
        wy(r).start()

    def forward_y(r):
        wy(r).wait_recv()
        wfy(r).start()

    for cp in small:
        cp.wait()
    gain_a = g_attn[...].astype(F32)
    row_iota = lax.broadcasted_iota(jnp.int32, (SEQ_LOC, 1), 0)

    def norm_prompts(i, carry):
        parts = []
        for t in range(8):
            b = i * 8 + t
            rows = pl.ds(pl.multiple_of(b * SEQ_LOC, SEQ_LOC), SEQ_LOC)
            v = buf_a[rows, :].astype(F32)
            inv = lax.rsqrt(jnp.mean(v * v, axis=-1, keepdims=True) + 1e-5)
            hit = row_iota == lens[b] - 1 - m * SEQ_LOC
            parts.append(jnp.sum(jnp.where(hit, v, 0.0), axis=0, keepdims=True))
            buf_a[rows, :] = (buf_a[rows, :].astype(F32) * inv * gain_a).astype(BF16)
        part[pl.ds(pl.multiple_of(i * 8, 8), 8), :] = jnp.concatenate(parts, axis=0)
        return carry

    per = CH // 8
    for j in range(NCH):
        load_p(j).wait()
        lax.fori_loop(j * per, (j + 1) * per, norm_prompts, 0)

    sel_b = normed.at[pl.ds(0, NB)]
    sel_b[...] = part[0:NB, :].astype(BF16)
    s1 = remote(sel_b, sel_r1, sel_s.at[0], sel_r.at[0], pt)
    s1.start()

    def unit_chunk(owner, h, j):
        col = pl.ds(pl.multiple_of(owner * 512 + h * 256, 256), 256)
        acc = dot32(buf_a[pl.ds(pl.multiple_of(j * ROWS, ROWS), ROWS), :], buf_b[:, col])
        here = pl.ds(pl.multiple_of(m * SEQ_LOC, SEQ_LOC), SEQ_LOC)
        for hd in range(2):
            a = acc[:, hd * HEAD_DIM:(hd + 1) * HEAD_DIM]
            if h == 0:
                turned = pltpu.roll(a, HEAD_DIM // 2, 1).reshape(CH, SEQ_LOC, HEAD_DIM)
                a = a.reshape(CH, SEQ_LOC, HEAD_DIM) * tab[0, here, :][None] + turned * tab[1, here, :][None]
                a = a.reshape(ROWS, HEAD_DIM)
            flat[pl.ds(hd, ROWS, stride=2), :] = a
        return flat[...].astype(BF16).reshape(CH, 2 * SEQ_LOC, HEAD_DIM)

    def kv_ref(h, j):
        return kv.at[h, pl.ds(pl.multiple_of(j * CH, CH), CH), pl.ds(pl.multiple_of(m * 64, 64), 64)]

    def kv_send(kind, h, j):
        dev = (pt, xs, xo)[kind]
        return remote(stage_p.at[j] if kind == 0 else stage.at[kind - 1, h, j], kv_ref(h, j), kv_s.at[kind, h, j], kv_r.at[kind, h, j], dev)

    def late_send(i):
        kind, h, first = 1 + i % 2, (i // 2) % 2, i // 4 * 4
        src = stage.at[kind - 1, h, LATE, pl.ds(first, 4)]
        dst = kv.at[h, pl.ds(LATE * CH + first, 4), pl.ds(pl.multiple_of(m * 64, 64), 64)]
        return remote(src, dst, late_s.at[i], late_r.at[i], (xs, xo)[i % 2])

    my_rb = pl.ds(pl.multiple_of(c * 64, 64), 64)

    def rb_send(h):
        return remote(stage.at[1, h, LATE], rb.at[h, :, my_rb], rb_s.at[h], rb_r.at[h], pt)

    def late_unit(h):
        chunk = unit_chunk(xs_m, h, LATE)
        stage[0, h, LATE] = chunk
        rb[h, :, my_rb] = chunk
        stage[1, h, LATE] = unit_chunk(xo_m, h, LATE)
        rb_send(h).start()

    def run_unit(kind, h, j):
        owner = (pt_m, xs_m, xo_m)[kind]
        chunk = unit_chunk(owner, h, j)
        if kind == 0:
            if h == 1:
                kv_send(0, 0, j).wait_send()
            stage_p[j] = chunk
        else:
            stage[kind - 1, h, j] = chunk
        kv_send(kind, h, j).start()

    def own_unit(h):
        def body(j, carry):
            kv[h, pl.ds(pl.multiple_of(j * CH, CH), CH), pl.ds(pl.multiple_of(m * 64, 64), 64)] = unit_chunk(m, h, j)
            return carry
        lax.fori_loop(0, NCH, body, 0)

    def loop_unit(kind, h):
        def body(j, carry):
            run_unit(kind, h, j)
            return carry
        lax.fori_loop(0, NCH if kind == 0 else LATE, body, 0)

    forward_x(0)
    own_unit(0)
    s1.wait()
    sel_b[...] = (sel_b[...].astype(F32) + sel_r1[...].astype(F32)).astype(BF16)
    half = pl.ds(pl.multiple_of(c * 32, 32), 32)
    s2 = remote(normed.at[half], sel_r2, sel_s.at[1], sel_r.at[1], xs)
    s2.start()
    own_unit(1)
    forward_x(1)
    forward_y(0)
    wp.wait_recv()
    loop_unit(0, 0)
    forward_x(2)
    forward_y(1)
    loop_unit(1, 0)
    for r in range(2):
        wfx(r).wait_recv()
        wfy(r).wait_recv()
    loop_unit(2, 0)
    late_unit(0)
    forward_x(3)
    forward_y(2)
    loop_unit(0, 1)

    s2.wait()
    hid[half, :] = (normed[half, :].astype(F32) + sel_r2[...].astype(F32)).astype(BF16)
    s3 = remote(hid.at[half], hid.at[half], sel_s.at[2], sel_r.at[2], pt)
    s3.start()
    forward_y(3)
    s3.wait()
    load_t.wait()

    def norm_rows(src, gain):
        v = src.astype(F32)
        inv = lax.rsqrt(jnp.mean(v * v, axis=-1, keepdims=True) + 1e-5)
        return (v * inv * gain).astype(BF16)

    def norm_hid(i, carry):
        rows = pl.ds(pl.multiple_of(i * 32, 32), 32)
        normed[rows, :] = norm_rows(hid[rows, :], gain_a)
        return carry

    lax.fori_loop(0, 4, norm_hid, 0)
    load_q.wait()
    q_buf[...] = jnp.zeros_like(q_buf)
    k_buf[...] = jnp.zeros_like(k_buf)
    v_buf[...] = jnp.zeros_like(v_buf)

    def pick(b, carry):
        pos = jnp.clip(lens[b], 1, 128)
        for i in range(2):
            rot[i, pl.ds(b, 1), :] = tab[i, pl.ds(pos - 1, 1), :]
            rot[i, pl.ds(NB + b, 1), :] = tab[i, pl.ds(pos, 1), :]
        return carry

    lax.fori_loop(0, NB, pick, 0)

    def turn(a, ct, st):
        return (a * ct + pltpu.roll(a, HEAD_DIM // 2, 1) * st).astype(BF16).astype(F32)

    for pair in range(3):
        qs = dot32(normed[...], buf_c[:, pair * 256:(pair + 1) * 256])
        for i in range(2):
            hd = pair * 2 + i
            q_h = turn(qs[:, i * HEAD_DIM:(i + 1) * HEAD_DIM], rot[0], rot[1])
            for t in range(2):
                q_buf[pl.ds(t * 8 + hd, NB, stride=16), :] = q_h[t * NB:(t + 1) * NB]
    toks = normed[NB:2 * NB, :]
    k_new = dot32(toks, buf_b[:, pl.ds(pl.multiple_of(m * 512, 256), 256)])
    v_new = dot32(toks, buf_b[:, pl.ds(pl.multiple_of(m * 512 + 256, 256), 256)])
    for g in range(2):
        cols = slice(g * HEAD_DIM, (g + 1) * HEAD_DIM)
        k_g = turn(k_new[:, cols], rot[0, NB:, :], rot[1, NB:, :])
        v_g = v_new[:, cols].astype(BF16).astype(F32)
        flat[pl.ds(g, NB, stride=2), :] = k_g
        flat[pl.ds(2 * NB + g, NB, stride=2), :] = v_g
        for i in range(3):
            rows = pl.ds(8 + 3 * g + i, NB, stride=16)
            k_buf[rows, :] = k_g
            v_buf[rows, :] = v_g
    knv[0] = flat[0:2 * NB, :].astype(BF16)
    knv[1] = flat[2 * NB:4 * NB, :].astype(BF16)

    qb[...] = q_buf[LATE * CH * 16:, :].astype(BF16)
    q_msg = remote(qb, qb_r, qp_s.at[0], qp_r.at[0], xs)
    q_msg.start()

    for r in range(2, WCH):
        wfx(r).wait_recv()
        wfy(r).wait_recv()

    def last_units(j, carry):
        run_unit(1, 1, j)
        run_unit(2, 1, j)
        return carry

    lax.fori_loop(0, LATE, last_units, 0)
    late_unit(1)
    wp.wait_send()
    for r in range(WCH):
        wx(r).wait_send()
        wfx(r).wait_send()
        wy(r).wait_send()
        wfy(r).wait_send()
    load_g.start()
    load_d.start()

    r_io = lax.broadcasted_iota(jnp.int32, (16, 256), 0)
    c_io = lax.broadcasted_iota(jnp.int32, (16, 256), 1)
    same = ((r_io & 7) >= 3) == ((c_io & 1) == 1)
    k_pos = c_io >> 1
    is_new = lax.broadcasted_iota(jnp.int32, (16, 1), 0) >= 8
    scale = HEAD_DIM ** -0.5

    def score(b):
        rows = pl.ds(pl.multiple_of(b * 16, 16), 16)
        q = q_buf[rows, :]
        s = lax.dot_general(q.astype(BF16), kv[0, b], (((1,), (1,)), ((), ())), preferred_element_type=F32) * scale
        s = jnp.where(same & (k_pos < lens[b]), s, NEG_BIG)
        s_new = jnp.where(is_new, jnp.sum(q * k_buf[rows, :], axis=-1, keepdims=True) * scale, NEG_BIG)
        top = jnp.maximum(jnp.max(s, axis=-1, keepdims=True), s_new)
        p = jnp.exp(s - top)
        p_new = jnp.exp(s_new - top)
        inv = 1.0 / (jnp.sum(p, axis=-1, keepdims=True) + p_new)
        p_buf[rows, :] = (p * inv).astype(BF16)
        a_buf[rows, :] = (p_new * inv) * v_buf[rows, :]

    def score_four(i, carry):
        for t in range(4):
            score(i * 4 + t)
        return carry

    def weigh_eight(i, carry):
        for t in range(8):
            b = i * 8 + t
            rows = pl.ds(pl.multiple_of(b * 16, 16), 16)
            a_buf[rows, :] = a_buf[rows, :] + dot32(p_buf[rows, :], kv[1, b])
        return carry

    c_half = lax.broadcasted_iota(jnp.int32, (16, 128), 1)
    r_half = lax.broadcasted_iota(jnp.int32, (16, 128), 0)
    same_half = ((r_half & 7) >= 3) == ((c_half & 1) == 1)
    pos_half = x * 64 + (c_half >> 1)
    on_diag = c_half == r_half
    chip_rows = pl.ds(pl.multiple_of(x * 128, 128), 128)

    def partial_scores(q, keys, b):
        s = lax.dot_general(q, keys, (((1,), (1,)), ((), ())), preferred_element_type=F32) * scale
        return jnp.where(same_half & (pos_half < lens[b]), s, NEG_BIG)

    def late_local(p):
        b = LATE * CH + p
        rows = pl.ds(pl.multiple_of(b * 16, 16), 16)
        out = pl.ds(pl.multiple_of(p * 16, 16), 16)
        q = q_buf[rows, :]
        s = partial_scores(q.astype(BF16), kv[0, b, chip_rows, :], b)
        s_new = jnp.where(is_new, jnp.sum(q * k_buf[rows, :], axis=-1, keepdims=True) * scale, NEG_BIG)
        top = jnp.maximum(jnp.max(s, axis=-1, keepdims=True), s_new)
        w = jnp.exp(s - top)
        w_new = jnp.exp(s_new - top)
        m_buf[out, :] = jnp.broadcast_to(top, (16, HEAD_DIM))
        l_buf[out, :] = jnp.broadcast_to(jnp.sum(w, axis=-1, keepdims=True) + w_new, (16, HEAD_DIM))
        a_buf[rows, :] = dot32(w.astype(BF16), kv[1, b, chip_rows, :]) + w_new * v_buf[rows, :]

    def late_peer(p):
        out = pl.ds(pl.multiple_of(p * 16, 16), 16)
        s = partial_scores(qb_r[out, :], rb[0, p], LATE * CH + p)
        top = jnp.max(s, axis=-1, keepdims=True)
        w = jnp.exp(s - top)
        acc = dot32(w.astype(BF16), rb[1, p])
        tops = jnp.sum(jnp.where(on_diag, top, 0.0), axis=0, keepdims=True)
        sums = jnp.sum(jnp.where(on_diag, jnp.sum(w, axis=-1, keepdims=True), 0.0), axis=0, keepdims=True)
        pb[out, :] = jnp.where(r_half == 6, tops, jnp.where(r_half == 7, sums, acc))

    def late_merge(p):
        rows = pl.ds(pl.multiple_of((LATE * CH + p) * 16, 16), 16)
        out = pl.ds(pl.multiple_of(p * 16, 16), 16)
        other = pb_r[out, :]
        o_top = jnp.sum(jnp.where(on_diag, other[6:7, :], 0.0), axis=-1, keepdims=True)
        o_sum = jnp.sum(jnp.where(on_diag, other[7:8, :], 0.0), axis=-1, keepdims=True)
        top = jnp.maximum(m_buf[out, :], o_top)
        w, o_w = jnp.exp(m_buf[out, :] - top), jnp.exp(o_top - top)
        a_buf[rows, :] = (a_buf[rows, :] * w + other * o_w) / (l_buf[out, :] * w + o_sum * o_w)

    def by_four(f):
        def body(i, carry):
            for t in range(4):
                f(i * 4 + t)
            return carry
        lax.fori_loop(0, CH // 4, body, 0)

    for j in range(LATE):
        for kind in range(3):
            kv_send(kind, 0, j).wait_recv()
        lax.fori_loop(j * (CH // 4), (j + 1) * (CH // 4), score_four, 0)
    for h in range(2):
        kv_send(0, h, LATE).wait_recv()
        rb_send(h).wait_recv()
    by_four(late_local)
    q_msg.wait_recv()
    by_four(late_peer)
    p_msg = remote(pb, pb_r, qp_s.at[1], qp_r.at[1], xs)
    p_msg.start()
    for i in range(N_GAP):
        late_send(i).start()

    for j in range(LATE):
        for kind in range(3):
            kv_send(kind, 1, j).wait_recv()
        lax.fori_loop(j * (CH // 8), (j + 1) * (CH // 8), weigh_eight, 0)
    p_msg.wait_recv()
    by_four(late_merge)

    for hd in range(6):
        for t in range(2):
            att[t * NB:(t + 1) * NB, hd * HEAD_DIM:(hd + 1) * HEAD_DIM] = a_buf[pl.ds(t * 8 + hd, NB, stride=16), :].astype(BF16)
    ot_half = pl.ds(pl.multiple_of((1 - c) * 64, 64), 64)
    mine = pl.ds(pl.multiple_of(c * 64 + x * 32, 32), 32)
    away = pl.ds(pl.multiple_of(c * 64 + (1 - x) * 32, 32), 32)
    mine_r1 = pl.ds(pl.multiple_of(x * 32, 32), 32)
    away_r1 = pl.ds(pl.multiple_of((1 - x) * 32, 32), 32)

    def reduce_all(k, produce, after, last, resid, buf):
        def msg(step, i, src, dst, dev):
            return remote(src, dst, ar_s.at[k, step, i], ar_r.at[k, step, i], dev)

        cols = [pl.ds(i * QW, QW) for i in range(4)]
        a1 = [msg(0, i, part.at[ot_half, cols[i]], r1.at[:, cols[i]], pt) for i in range(4)]
        a2 = [msg(1, i, part.at[away, cols[i]], r2.at[:, cols[i]], xs) for i in range(4)]
        a3 = [msg(2, i, buf.at[mine, cols[i]], buf.at[mine, cols[i]], xs) for i in range(4)]
        a4 = [msg(3, i, buf.at[mine, cols[i]], buf.at[mine, cols[i]], pt) for i in range(4)]
        a5 = [msg(4, i, buf.at[away, cols[i]], buf.at[away, cols[i]], pt) for i in range(4)]

        def over_x(i):
            a1[i].wait_recv()
            part[away, cols[i]] = part[away, cols[i]] + r1[away_r1, cols[i]]
            a2[i].start()
            part[mine, cols[i]] = part[mine, cols[i]] + r1[mine_r1, cols[i]]

        for i in range(4):
            produce(i)
            a1[i].start()
            if i:
                over_x(i - 1)
        over_x(3)
        after()
        for i in range(4):
            if i == 3:
                for t in range(N_MID):
                    late_send((N_GAP, N_LATE - N_MID)[k] + t).start()
            a2[i].wait_recv()
            total = part[mine, cols[i]] + r2[:, cols[i]]
            buf[mine, cols[i]] = (resid[mine, cols[i]].astype(F32) + total).astype(BF16)
            a3[i].start()
            a4[i].start()
        last()
        for i in range(4):
            a3[i].wait_recv()
            a5[i].start()
        for i in range(4):
            a4[i].wait_recv()
            a5[i].wait_recv()
        for step in (a1, a2, a3, a4, a5):
            for i in range(4):
                step[i].wait_send()

    def w_o_cols(i):
        load_o(i).wait()
        part[:, i * QW:(i + 1) * QW] = dot32(att[...], buf_c[i * QW:(i + 1) * QW, QW:2 * QW])

    def after_w_o():
        load_u.start()

    def send_late():
        for i in range(N_GAP + N_MID, N_LATE - N_MID):
            late_send(i).start()

    def keep_late():
        for i in range(N_LATE - N_MID):
            late_send(i).wait_recv()

    reduce_all(0, w_o_cols, after_w_o, send_late, hid, x2)
    gain_m = g_mlp[...].astype(F32)

    def norm_x2(i, carry):
        rows = pl.ds(pl.multiple_of(i * 32, 32), 32)
        normed[rows, :] = norm_rows(x2[rows, :], gain_m)
        return carry

    lax.fori_loop(0, 4, norm_x2, 0)
    load_g.wait()
    load_u.wait()

    def mlp_cols(i, carry):
        cols = pl.ds(pl.multiple_of(i * 256, 256), 256)
        gate = dot32(normed[...], buf_b[:, cols])
        up = dot32(normed[...], buf_c[:, cols])
        mid[:, cols] = (gate * (1.0 / (1.0 + jnp.exp(-gate))) * up).astype(BF16)
        return carry

    lax.fori_loop(0, FF // 256, mlp_cols, 0)
    load_d.wait()

    def down_cols(i):
        def body(t, carry):
            cols = pl.ds(pl.multiple_of(i * QW + t * 256, 256), 256)
            part[:, cols] = dot32(mid[...], buf_a[:, cols])
            return carry
        lax.fori_loop(0, QW // 256, body, 0)

    reduce_all(1, down_cols, keep_late, lambda: None, x2, hid)
    for kind in range(3):
        for tn in range(2):
            for j in range(NCH if kind == 0 else LATE):
                if kind or tn:
                    kv_send(kind, tn, j).wait_send()
    for i in range(N_LATE):
        late_send(i).wait_send()
    for i in range(N_LATE - N_MID, N_LATE):
        late_send(i).wait_recv()
    for h in range(2):
        rb_send(h).wait_send()
    q_msg.wait_send()
    p_msg.wait_send()


def copy_out(kv, knv, hid, k_out, v_out, last_out, dec_out, buf, sem, row_sem):
    rows = [pltpu.make_async_copy(hid.at[pl.ds(i * NB, NB)], dst, row_sem.at[i]) for i, dst in enumerate((last_out, dec_out))]
    for r in rows:
        r.start()

    def store(h, g):
        dst = pl.ds(pl.multiple_of(g * 2064, 2064), 2064)
        slot = lax.rem(g, 2)
        return pltpu.make_async_copy(buf.at[h, slot, pl.ds(0, 2064)], (k_out, v_out)[h].at[dst], sem.at[h, slot])

    def lay_out(g, carry):
        slot = lax.rem(g, 2)
        for h in range(2):
            @pl.when(g > 1)
            def _():
                store(h, g - 2).wait()
            for t in range(8):
                buf[h, slot, t * 258:t * 258 + 256, :] = kv[h, g * 8 + t]
            new = knv[h, pl.ds(pl.multiple_of(g * 16, 16), 16), :]
            for t in range(8):
                buf[h, slot, t * 258 + 256:t * 258 + 258, :] = new[2 * t:2 * t + 2]
            store(h, g).start()
        return carry

    lax.fori_loop(0, NB // 8, lay_out, 0)
    for g in range(NB // 8 - 2, NB // 8):
        for h in range(2):
            store(h, g).wait()
    for r in rows:
        r.wait()


def solution(mesh):
    seq_spec = P('replica', 'model', None)
    col_spec = P(None, None, 'model')
    row_spec = P(None, 'model', None)
    gain_spec = P(None, None)
    tok_spec = P('replica', None)
    cache_spec = P(None, 'replica', None, 'model', None)
    in_specs = (seq_spec, P('replica'), tok_spec, gain_spec, col_spec, col_spec, col_spec, row_spec, gain_spec, col_spec, col_spec, row_spec)
    out_specs = (tok_spec, tok_spec, cache_spec, cache_spec)

    def per_device(prompt, lengths, new_tok, norm_attn, w_q, w_k, w_v, w_o, norm_mlp, w_gate, w_up, w_down):
        tab = jnp.asarray(rotate_tables(136))
        vmem = pl.BlockSpec(memory_space=pltpu.VMEM)
        hbm = pl.BlockSpec(memory_space=pl.ANY)
        smem = pl.BlockSpec(memory_space=pltpu.SMEM)
        dma = pltpu.SemaphoreType.DMA
        kv, knv, hid = pl.pallas_call(
            kernel,
            out_shape=(pltpu.VMEM((2, NB, 256, HEAD_DIM), BF16), pltpu.VMEM((2, 2 * NB, HEAD_DIM), BF16), pltpu.VMEM((2 * NB, D), BF16)),
            in_specs=[smem] + [hbm] * 12,
            out_specs=(vmem,) * 3,
            scratch_shapes=[
                pltpu.VMEM((NB * SEQ_LOC, D), BF16),
                pltpu.VMEM((D, FF), BF16),
                pltpu.VMEM((D, FF), BF16),
                pltpu.VMEM((2, 2, NCH, CH, 64, HEAD_DIM), BF16),
                pltpu.VMEM((NCH, CH, 64, HEAD_DIM), BF16),
                pltpu.VMEM((2 * ROWS, HEAD_DIM), F32),
                pltpu.VMEM((NB * 16, HEAD_DIM), F32),
                pltpu.VMEM((NB * 16, HEAD_DIM), F32),
                pltpu.VMEM((NB * 16, HEAD_DIM), F32),
                pltpu.VMEM((NB * 16, HEAD_DIM), F32),
                pltpu.VMEM((2 * NB, QW), BF16),
                pltpu.VMEM((NB, D), BF16),
                pltpu.VMEM((32, D), BF16),
                pltpu.VMEM((2 * NB, D), BF16),
                pltpu.VMEM((2 * NB, D), F32),
                pltpu.VMEM((NB, D), F32),
                pltpu.VMEM((32, D), F32),
                pltpu.VMEM((2 * NB, D), BF16),
                pltpu.VMEM((2 * NB, FF), BF16),
                pltpu.VMEM((NB * 16, 256), BF16),
                pltpu.VMEM((2, 2 * NB, HEAD_DIM), F32),
                pltpu.VMEM((2, 136, HEAD_DIM), F32),
                pltpu.VMEM((1, D), BF16),
                pltpu.VMEM((1, D), BF16),
                pltpu.VMEM((2, CH, 128, HEAD_DIM), BF16),
                pltpu.VMEM((CH * 16, HEAD_DIM), BF16),
                pltpu.VMEM((CH * 16, HEAD_DIM), BF16),
                pltpu.VMEM((CH * 16, HEAD_DIM), F32),
                pltpu.VMEM((CH * 16, HEAD_DIM), F32),
                pltpu.VMEM((CH * 16, HEAD_DIM), F32),
                pltpu.VMEM((CH * 16, HEAD_DIM), F32),
                dma((NCH,)), dma((2,)), dma((9,)), dma((3,)),
                dma, dma, dma((WCH,)), dma((WCH,)), dma((WCH,)), dma((WCH,)),
                dma((WCH,)), dma((WCH,)), dma((WCH,)), dma((WCH,)),
                dma((3,)), dma((3,)), dma((3, 2, NCH)), dma((3, 2, NCH)), dma((2, 5, 4)), dma((2, 5, 4)),
                dma((2,)), dma((2,)), dma((N_LATE,)), dma((N_LATE,)), dma((2,)), dma((2,)),
            ],
            compiler_params=pltpu.CompilerParams(collective_id=0, has_side_effects=True, vmem_limit_bytes=VMEM_LAYER),
            name="layer",
        )(lengths, tab, norm_attn, norm_mlp, new_tok,
          prompt.reshape(NB * SEQ_LOC, D), w_q[0], w_k[0], w_v[0], w_o[0], w_gate[0], w_up[0], w_down[0])
        rows, slots = jax.ShapeDtypeStruct((NB, D), BF16), jax.ShapeDtypeStruct((NB * 258, HEAD_DIM), BF16)
        o_k, o_v, o_last, o_dec = pl.pallas_call(
            copy_out,
            out_shape=(slots, slots, rows, rows),
            in_specs=[vmem] * 3,
            out_specs=(hbm,) * 4,
            scratch_shapes=[pltpu.VMEM((2, 2, 8 * 258 + 32, HEAD_DIM), BF16), dma((2, 2)), dma((2,))],
            compiler_params=pltpu.CompilerParams(vmem_limit_bytes=40 << 20),
            name="copy_out",
        )(kv, knv, hid)
        caches = [o.reshape(1, NB, 129, 2, HEAD_DIM) for o in (o_k, o_v)]
        return o_dec, o_last, caches[0], caches[1]

    return jax.shard_map(per_device, mesh=mesh, in_specs=in_specs, out_specs=out_specs, check_vma=False)
```

```python
import functools

import jax
import jax.numpy as jnp
import numpy as np
from jax import lax
from jax.experimental import pallas as pl
from jax.experimental.pallas import tpu as pltpu
from jax.sharding import PartitionSpec as P

HEAD_DIM = 128
NEG_BIG = -1e30
MESH = pl.DeviceIdType.MESH
F32 = jnp.float32
BF16 = jnp.bfloat16

NB = 64
SEQ_LOC = 32
D = 3072
FF = 2048
QW = 768
CH = 16
NCH = NB // CH
ROWS = CH * SEQ_LOC
VMEM_LAYER = 67043328 - (10 << 20)
LATE = NCH - 1
N_EARLY = 1
N_LATE = 16
N_GAP = 4
N_MID = 0
N_FIRST = 4 * N_EARLY + N_GAP
WCH = 4
WROWS = D // WCH


def dot32(lhs, rhs):
    return jnp.dot(lhs, rhs, preferred_element_type=F32)


def rotate_tables(n):
    half = HEAD_DIM // 2
    inv_freq = np.float32(10000.0) ** (np.float32(-2.0) * np.arange(half, dtype=np.float32) / np.float32(HEAD_DIM))
    angles = (np.arange(n, dtype=np.float32)[:, None] * inv_freq).astype(np.float32).astype(np.float64)
    cos_tab, sin_tab = np.cos(angles), np.sin(angles)
    return np.stack([np.concatenate([cos_tab, cos_tab], 1), np.concatenate([-sin_tab, sin_tab], 1)]).astype(np.float32)


def kernel(lens, tab_in, g_attn_in, g_mlp_in,
           new_tok, prompt, w_q, w_k, w_v, w_o, w_g, w_u, w_d,
           kv, knv, hid,
           buf_a, buf_b, buf_c, stage, stage_p, flat, q_buf, k_buf, v_buf, a_buf, att,
           sel_r1, sel_r2, normed, part, r1, r2, x2, mid, p_buf, rot,
           tab, g_attn, g_mlp, rb, qb, qb_r, m_buf, l_buf, pb, pb_r,
           ld_p, ld_w, ld_big, ld_small,
           wp_s, wp_r, wx_s, wx_r, wfx_s, wfx_r, wy_s, wy_r, wfy_s, wfy_r,
           sel_s, sel_r, kv_s, kv_r, ar_s, ar_r, rb_s, rb_r, late_s, late_r, qp_s, qp_r):
    y = lax.axis_index("replica")
    m = lax.axis_index("model")
    c = lax.rem(m, 2)
    x = m // 2
    xs_m = lax.rem(m + 2, 4)
    xo_m = 3 - m
    pt_m = m + 1 - 2 * c
    xs, xo, pt, yp = (y, xs_m), (y, xo_m), (y, pt_m), (1 - y, m)

    def remote(src, dst, ssem, rsem, dev):
        return pltpu.make_async_remote_copy(src_ref=src, dst_ref=dst, send_sem=ssem, recv_sem=rsem,
                                            device_id=dev, device_id_type=MESH)

    def load_w(i):
        src = (w_k, w_v)[i]
        return pltpu.make_async_copy(src, buf_b.at[:, pl.ds(pl.multiple_of(m * 512 + i * 256, 256), 256)], ld_w.at[i])

    def load_p(j):
        r = pl.ds(pl.multiple_of(j * ROWS, ROWS), ROWS)
        return pltpu.make_async_copy(prompt.at[r], buf_a.at[r], ld_p.at[j])

    for i in range(2):
        load_w(i).start()
    for j in range(NCH):
        load_p(j).start()
    load_q = pltpu.make_async_copy(w_q, buf_c.at[:, pl.ds(0, QW)], ld_big.at[0])
    load_q.start()
    load_t = pltpu.make_async_copy(new_tok, hid.at[pl.ds(NB, NB)], ld_big.at[8])
    load_t.start()
    small = [pltpu.make_async_copy(src, dst, ld_small.at[i])
             for i, (src, dst) in enumerate(((tab_in, tab), (g_attn_in, g_attn), (g_mlp_in, g_mlp)))]
    for cp in small:
        cp.start()

    def load_o(i):
        return pltpu.make_async_copy(w_o.at[:, pl.ds(i * QW, QW)], buf_c.at[pl.ds(i * QW, QW), pl.ds(QW, QW)], ld_big.at[1 + i])

    for i in range(4):
        load_o(i).start()
    load_g = pltpu.make_async_copy(w_g, buf_b, ld_big.at[5])
    load_u = pltpu.make_async_copy(w_u, buf_c, ld_big.at[6])
    load_d = pltpu.make_async_copy(w_d, buf_a, ld_big.at[7])

    barrier = pltpu.get_barrier_semaphore()
    for dev in (xs, xo, pt, yp):
        pl.semaphore_signal(barrier, inc=1, device_id=dev, device_id_type=MESH)
    pl.semaphore_wait(barrier, 4)

    def w_ref(owner, half, r):
        rows = pl.ds(pl.multiple_of(half * (D // 2) + (r % 2) * WROWS, WROWS), WROWS)
        return buf_b.at[rows, pl.ds(pl.multiple_of(owner * 512 + (r // 2) * 256, 256), 256)]

    def wx(r):
        src = (w_k, w_v)[r // 2].at[pl.ds(pl.multiple_of(y * (D // 2) + (r % 2) * WROWS, WROWS), WROWS)]
        return remote(src, w_ref(m, y, r), wx_s.at[r], wx_r.at[r], xs)

    def wfx(r):
        ref = w_ref(xs_m, y, r)
        return remote(ref, ref, wfx_s.at[r], wfx_r.at[r], pt)

    def wy(r):
        ref = w_ref(xs_m, y, r)
        return remote(ref, ref, wy_s.at[r], wy_r.at[r], yp)

    def wfy(r):
        ref = w_ref(xs_m, 1 - y, r)
        return remote(ref, ref, wfy_s.at[r], wfy_r.at[r], pt)

    own = buf_b.at[:, pl.ds(pl.multiple_of(m * 512, 512), 512)]
    wp = remote(own, own, wp_s, wp_r, pt)
    for r in range(WCH):
        wx(r).start()
    for i in range(2):
        load_w(i).wait()
    wp.start()

    def forward_x(r):
        wx(r).wait_recv()
        wfx(r).start()
        wy(r).start()

    def forward_y(r):
        wy(r).wait_recv()
        wfy(r).start()

    for cp in small:
        cp.wait()
    gain_a = g_attn[...].astype(F32)
    row_iota = lax.broadcasted_iota(jnp.int32, (SEQ_LOC, 1), 0)

    def norm_prompts(i, carry):
        parts = []
        for t in range(8):
            b = i * 8 + t
            rows = pl.ds(pl.multiple_of(b * SEQ_LOC, SEQ_LOC), SEQ_LOC)
            v = buf_a[rows, :].astype(F32)
            inv = lax.rsqrt(jnp.mean(v * v, axis=-1, keepdims=True) + 1e-5)
            hit = row_iota == lens[b] - 1 - m * SEQ_LOC
            parts.append(jnp.sum(jnp.where(hit, v, 0.0), axis=0, keepdims=True))
            buf_a[rows, :] = (buf_a[rows, :].astype(F32) * inv * gain_a).astype(BF16)
        part[pl.ds(pl.multiple_of(i * 8, 8), 8), :] = jnp.concatenate(parts, axis=0)
        return carry

    per = CH // 8
    for j in range(NCH):
        load_p(j).wait()
        lax.fori_loop(j * per, (j + 1) * per, norm_prompts, 0)

    sel_b = normed.at[pl.ds(0, NB)]
    sel_b[...] = part[0:NB, :].astype(BF16)
    s1 = remote(sel_b, sel_r1, sel_s.at[0], sel_r.at[0], pt)
    s1.start()

    def unit_chunk(owner, h, j):
        col = pl.ds(pl.multiple_of(owner * 512 + h * 256, 256), 256)
        acc = dot32(buf_a[pl.ds(pl.multiple_of(j * ROWS, ROWS), ROWS), :], buf_b[:, col])
        here = pl.ds(pl.multiple_of(m * SEQ_LOC, SEQ_LOC), SEQ_LOC)
        for hd in range(2):
            a = acc[:, hd * HEAD_DIM:(hd + 1) * HEAD_DIM]
            if h == 0:
                turned = pltpu.roll(a, HEAD_DIM // 2, 1).reshape(CH, SEQ_LOC, HEAD_DIM)
                a = a.reshape(CH, SEQ_LOC, HEAD_DIM) * tab[0, here, :][None] + turned * tab[1, here, :][None]
                a = a.reshape(ROWS, HEAD_DIM)
            flat[pl.ds(hd, ROWS, stride=2), :] = a
        return flat[...].astype(BF16).reshape(CH, 2 * SEQ_LOC, HEAD_DIM)

    def kv_ref(h, j):
        return kv.at[h, pl.ds(pl.multiple_of(j * CH, CH), CH), pl.ds(pl.multiple_of(m * 64, 64), 64)]

    def kv_send(kind, h, j):
        dev = (pt, xs, xo)[kind]
        return remote(stage_p.at[j] if kind == 0 else stage.at[kind - 1, h, j], kv_ref(h, j), kv_s.at[kind, h, j], kv_r.at[kind, h, j], dev)

    def late_send(i):
        kind, h, first = 1 + i % 2, (i // 2) % 2, i // 4 * 4
        src = stage.at[kind - 1, h, LATE, pl.ds(first, 4)]
        dst = kv.at[h, pl.ds(LATE * CH + first, 4), pl.ds(pl.multiple_of(m * 64, 64), 64)]
        return remote(src, dst, late_s.at[i], late_r.at[i], (xs, xo)[i % 2])

    my_rb = pl.ds(pl.multiple_of(c * 64, 64), 64)

    def rb_send(h):
        return remote(stage.at[1, h, LATE], rb.at[h, :, my_rb], rb_s.at[h], rb_r.at[h], pt)

    def late_unit(h):
        chunk = unit_chunk(xs_m, h, LATE)
        stage[0, h, LATE] = chunk
        rb[h, :, my_rb] = chunk
        stage[1, h, LATE] = unit_chunk(xo_m, h, LATE)
        rb_send(h).start()
        for t in range(N_EARLY):
            for i in range(2):
                late_send(4 * t + 2 * h + i).start()

    def run_unit(kind, h, j):
        owner = (pt_m, xs_m, xo_m)[kind]
        chunk = unit_chunk(owner, h, j)
        if kind == 0:
            if h == 1:
                kv_send(0, 0, j).wait_send()
            stage_p[j] = chunk
        else:
            stage[kind - 1, h, j] = chunk
        kv_send(kind, h, j).start()

    def own_unit(h):
        def body(j, carry):
            kv[h, pl.ds(pl.multiple_of(j * CH, CH), CH), pl.ds(pl.multiple_of(m * 64, 64), 64)] = unit_chunk(m, h, j)
            return carry
        lax.fori_loop(0, NCH, body, 0)

    def loop_unit(kind, h):
        def body(j, carry):
            run_unit(kind, h, j)
            return carry
        lax.fori_loop(0, NCH if kind == 0 else LATE, body, 0)

    forward_x(0)
    own_unit(0)
    s1.wait()
    sel_b[...] = (sel_b[...].astype(F32) + sel_r1[...].astype(F32)).astype(BF16)
    half = pl.ds(pl.multiple_of(c * 32, 32), 32)
    s2 = remote(normed.at[half], sel_r2, sel_s.at[1], sel_r.at[1], xs)
    s2.start()
    own_unit(1)
    forward_x(1)
    forward_y(0)
    wp.wait_recv()
    loop_unit(0, 0)
    forward_x(2)
    forward_y(1)
    loop_unit(1, 0)
    for r in range(2):
        wfx(r).wait_recv()
        wfy(r).wait_recv()
    loop_unit(2, 0)
    late_unit(0)
    forward_x(3)
    forward_y(2)
    loop_unit(0, 1)

    s2.wait()
    hid[half, :] = (normed[half, :].astype(F32) + sel_r2[...].astype(F32)).astype(BF16)
    s3 = remote(hid.at[half], hid.at[half], sel_s.at[2], sel_r.at[2], pt)
    s3.start()
    forward_y(3)
    s3.wait()
    load_t.wait()

    def norm_rows(src, gain):
        v = src.astype(F32)
        inv = lax.rsqrt(jnp.mean(v * v, axis=-1, keepdims=True) + 1e-5)
        return (v * inv * gain).astype(BF16)

    def norm_hid(i, carry):
        rows = pl.ds(pl.multiple_of(i * 32, 32), 32)
        normed[rows, :] = norm_rows(hid[rows, :], gain_a)
        return carry

    lax.fori_loop(0, 4, norm_hid, 0)
    load_q.wait()
    q_buf[...] = jnp.zeros_like(q_buf)
    k_buf[...] = jnp.zeros_like(k_buf)
    v_buf[...] = jnp.zeros_like(v_buf)

    def pick(b, carry):
        pos = jnp.clip(lens[b], 1, 128)
        for i in range(2):
            rot[i, pl.ds(b, 1), :] = tab[i, pl.ds(pos - 1, 1), :]
            rot[i, pl.ds(NB + b, 1), :] = tab[i, pl.ds(pos, 1), :]
        return carry

    lax.fori_loop(0, NB, pick, 0)

    def turn(a, ct, st):
        return (a * ct + pltpu.roll(a, HEAD_DIM // 2, 1) * st).astype(BF16).astype(F32)

    for pair in range(3):
        qs = dot32(normed[...], buf_c[:, pair * 256:(pair + 1) * 256])
        for i in range(2):
            hd = pair * 2 + i
            q_h = turn(qs[:, i * HEAD_DIM:(i + 1) * HEAD_DIM], rot[0], rot[1])
            for t in range(2):
                q_buf[pl.ds(t * 8 + hd, NB, stride=16), :] = q_h[t * NB:(t + 1) * NB]
    toks = normed[NB:2 * NB, :]
    k_new = dot32(toks, buf_b[:, pl.ds(pl.multiple_of(m * 512, 256), 256)])
    v_new = dot32(toks, buf_b[:, pl.ds(pl.multiple_of(m * 512 + 256, 256), 256)])
    for g in range(2):
        cols = slice(g * HEAD_DIM, (g + 1) * HEAD_DIM)
        k_g = turn(k_new[:, cols], rot[0, NB:, :], rot[1, NB:, :])
        v_g = v_new[:, cols].astype(BF16).astype(F32)
        flat[pl.ds(g, NB, stride=2), :] = k_g
        flat[pl.ds(2 * NB + g, NB, stride=2), :] = v_g
        for i in range(3):
            rows = pl.ds(8 + 3 * g + i, NB, stride=16)
            k_buf[rows, :] = k_g
            v_buf[rows, :] = v_g
    knv[0] = flat[0:2 * NB, :].astype(BF16)
    knv[1] = flat[2 * NB:4 * NB, :].astype(BF16)

    qb[...] = q_buf[LATE * CH * 16:, :].astype(BF16)
    late_rows = pl.ds(N_EARLY * 64, CH * 16 - N_EARLY * 64)
    q_msg = remote(qb.at[late_rows], qb_r.at[late_rows], qp_s.at[0], qp_r.at[0], xs)
    q_msg.start()

    for r in range(2, WCH):
        wfx(r).wait_recv()
        wfy(r).wait_recv()

    def last_units(j, carry):
        run_unit(1, 1, j)
        run_unit(2, 1, j)
        return carry

    lax.fori_loop(0, LATE, last_units, 0)
    late_unit(1)
    wp.wait_send()
    for r in range(WCH):
        wx(r).wait_send()
        wfx(r).wait_send()
        wy(r).wait_send()
        wfy(r).wait_send()
    load_g.start()
    load_d.start()

    r_io = lax.broadcasted_iota(jnp.int32, (16, 256), 0)
    c_io = lax.broadcasted_iota(jnp.int32, (16, 256), 1)
    same = ((r_io & 7) >= 3) == ((c_io & 1) == 1)
    k_pos = c_io >> 1
    is_new = lax.broadcasted_iota(jnp.int32, (16, 1), 0) >= 8
    scale = HEAD_DIM ** -0.5

    def score(b):
        rows = pl.ds(pl.multiple_of(b * 16, 16), 16)
        q = q_buf[rows, :]
        s = lax.dot_general(q.astype(BF16), kv[0, b], (((1,), (1,)), ((), ())), preferred_element_type=F32) * scale
        s = jnp.where(same & (k_pos < lens[b]), s, NEG_BIG)
        s_new = jnp.where(is_new, jnp.sum(q * k_buf[rows, :], axis=-1, keepdims=True) * scale, NEG_BIG)
        top = jnp.maximum(jnp.max(s, axis=-1, keepdims=True), s_new)
        p = jnp.exp(s - top)
        p_new = jnp.exp(s_new - top)
        inv = 1.0 / (jnp.sum(p, axis=-1, keepdims=True) + p_new)
        p_buf[rows, :] = (p * inv).astype(BF16)
        a_buf[rows, :] = (p_new * inv) * v_buf[rows, :]

    def score_four(i, carry):
        for t in range(4):
            score(i * 4 + t)
        return carry

    def weigh(b):
        rows = pl.ds(pl.multiple_of(b * 16, 16), 16)
        a_buf[rows, :] = a_buf[rows, :] + dot32(p_buf[rows, :], kv[1, b])

    def weigh_eight(i, carry):
        for t in range(8):
            weigh(i * 8 + t)
        return carry

    c_half = lax.broadcasted_iota(jnp.int32, (16, 128), 1)
    r_half = lax.broadcasted_iota(jnp.int32, (16, 128), 0)
    same_half = ((r_half & 7) >= 3) == ((c_half & 1) == 1)
    pos_half = x * 64 + (c_half >> 1)
    on_diag = c_half == r_half
    chip_rows = pl.ds(pl.multiple_of(x * 128, 128), 128)

    def partial_scores(q, keys, b):
        s = lax.dot_general(q, keys, (((1,), (1,)), ((), ())), preferred_element_type=F32) * scale
        return jnp.where(same_half & (pos_half < lens[b]), s, NEG_BIG)

    def late_local(p):
        b = LATE * CH + p
        rows = pl.ds(pl.multiple_of(b * 16, 16), 16)
        out = pl.ds(pl.multiple_of(p * 16, 16), 16)
        q = q_buf[rows, :]
        s = partial_scores(q.astype(BF16), kv[0, b, chip_rows, :], b)
        s_new = jnp.where(is_new, jnp.sum(q * k_buf[rows, :], axis=-1, keepdims=True) * scale, NEG_BIG)
        top = jnp.maximum(jnp.max(s, axis=-1, keepdims=True), s_new)
        w = jnp.exp(s - top)
        w_new = jnp.exp(s_new - top)
        m_buf[out, :] = jnp.broadcast_to(top, (16, HEAD_DIM))
        l_buf[out, :] = jnp.broadcast_to(jnp.sum(w, axis=-1, keepdims=True) + w_new, (16, HEAD_DIM))
        a_buf[rows, :] = dot32(w.astype(BF16), kv[1, b, chip_rows, :]) + w_new * v_buf[rows, :]

    def late_peer(p):
        out = pl.ds(pl.multiple_of(p * 16, 16), 16)
        s = partial_scores(qb_r[out, :], rb[0, p], LATE * CH + p)
        top = jnp.max(s, axis=-1, keepdims=True)
        w = jnp.exp(s - top)
        acc = dot32(w.astype(BF16), rb[1, p])
        tops = jnp.sum(jnp.where(on_diag, top, 0.0), axis=0, keepdims=True)
        sums = jnp.sum(jnp.where(on_diag, jnp.sum(w, axis=-1, keepdims=True), 0.0), axis=0, keepdims=True)
        pb[out, :] = jnp.where(r_half == 6, tops, jnp.where(r_half == 7, sums, acc))

    def late_merge(p):
        rows = pl.ds(pl.multiple_of((LATE * CH + p) * 16, 16), 16)
        out = pl.ds(pl.multiple_of(p * 16, 16), 16)
        other = pb_r[out, :]
        o_top = jnp.sum(jnp.where(on_diag, other[6:7, :], 0.0), axis=-1, keepdims=True)
        o_sum = jnp.sum(jnp.where(on_diag, other[7:8, :], 0.0), axis=-1, keepdims=True)
        top = jnp.maximum(m_buf[out, :], o_top)
        w, o_w = jnp.exp(m_buf[out, :] - top), jnp.exp(o_top - top)
        a_buf[rows, :] = (a_buf[rows, :] * w + other * o_w) / (l_buf[out, :] * w + o_sum * o_w)

    def by_four(f):
        def body(i, carry):
            for t in range(4):
                f(i * 4 + t)
            return carry
        lax.fori_loop(N_EARLY, CH // 4, body, 0)

    for j in range(LATE):
        for kind in range(3):
            kv_send(kind, 0, j).wait_recv()
        lax.fori_loop(j * (CH // 4), (j + 1) * (CH // 4), score_four, 0)
    for h in range(2):
        kv_send(0, h, LATE).wait_recv()
        rb_send(h).wait_recv()
    for t in range(N_EARLY):
        for i in range(2):
            late_send(4 * t + i).wait_recv()
        score_four(LATE * (CH // 4) + t, 0)
    by_four(late_local)
    q_msg.wait_recv()
    by_four(late_peer)
    p_msg = remote(pb.at[late_rows], pb_r.at[late_rows], qp_s.at[1], qp_r.at[1], xs)
    p_msg.start()
    for i in range(4 * N_EARLY, N_FIRST):
        late_send(i).start()

    for j in range(LATE):
        for kind in range(3):
            kv_send(kind, 1, j).wait_recv()
        lax.fori_loop(j * (CH // 8), (j + 1) * (CH // 8), weigh_eight, 0)
    for t in range(N_EARLY):
        for i in range(2):
            late_send(4 * t + 2 + i).wait_recv()
        for b in range(LATE * CH + 4 * t, LATE * CH + 4 * t + 4):
            weigh(b)
    p_msg.wait_recv()
    by_four(late_merge)

    for hd in range(6):
        for t in range(2):
            att[t * NB:(t + 1) * NB, hd * HEAD_DIM:(hd + 1) * HEAD_DIM] = a_buf[pl.ds(t * 8 + hd, NB, stride=16), :].astype(BF16)
    ot_half = pl.ds(pl.multiple_of((1 - c) * 64, 64), 64)
    mine = pl.ds(pl.multiple_of(c * 64 + x * 32, 32), 32)
    away = pl.ds(pl.multiple_of(c * 64 + (1 - x) * 32, 32), 32)
    mine_r1 = pl.ds(pl.multiple_of(x * 32, 32), 32)
    away_r1 = pl.ds(pl.multiple_of((1 - x) * 32, 32), 32)

    def reduce_all(k, produce, after, last, resid, buf):
        def msg(step, i, src, dst, dev):
            return remote(src, dst, ar_s.at[k, step, i], ar_r.at[k, step, i], dev)

        cols = [pl.ds(i * QW, QW) for i in range(4)]
        a1 = [msg(0, i, part.at[ot_half, cols[i]], r1.at[:, cols[i]], pt) for i in range(4)]
        a2 = [msg(1, i, part.at[away, cols[i]], r2.at[:, cols[i]], xs) for i in range(4)]
        a3 = [msg(2, i, buf.at[mine, cols[i]], buf.at[mine, cols[i]], xs) for i in range(4)]
        a4 = [msg(3, i, buf.at[mine, cols[i]], buf.at[mine, cols[i]], pt) for i in range(4)]
        a5 = [msg(4, i, buf.at[away, cols[i]], buf.at[away, cols[i]], pt) for i in range(4)]

        def over_x(i):
            a1[i].wait_recv()
            part[away, cols[i]] = part[away, cols[i]] + r1[away_r1, cols[i]]
            a2[i].start()
            part[mine, cols[i]] = part[mine, cols[i]] + r1[mine_r1, cols[i]]

        for i in range(4):
            produce(i)
            a1[i].start()
            if i:
                over_x(i - 1)
        over_x(3)
        after()
        for i in range(4):
            if i == 3:
                for t in range(N_MID):
                    late_send((N_FIRST, N_LATE - N_MID)[k] + t).start()
            a2[i].wait_recv()
            total = part[mine, cols[i]] + r2[:, cols[i]]
            buf[mine, cols[i]] = (resid[mine, cols[i]].astype(F32) + total).astype(BF16)
            a3[i].start()
            a4[i].start()
        last()
        for i in range(4):
            a3[i].wait_recv()
            a5[i].start()
        for i in range(4):
            a4[i].wait_recv()
            a5[i].wait_recv()
        for step in (a1, a2, a3, a4, a5):
            for i in range(4):
                step[i].wait_send()

    def w_o_cols(i):
        load_o(i).wait()
        part[:, i * QW:(i + 1) * QW] = dot32(att[...], buf_c[i * QW:(i + 1) * QW, QW:2 * QW])

    def after_w_o():
        load_u.start()

    def send_late():
        for i in range(N_FIRST + N_MID, N_LATE - N_MID):
            late_send(i).start()

    def keep_late():
        for i in range(4 * N_EARLY, N_LATE - N_MID):
            late_send(i).wait_recv()

    reduce_all(0, w_o_cols, after_w_o, send_late, hid, x2)
    gain_m = g_mlp[...].astype(F32)

    def norm_x2(i, carry):
        rows = pl.ds(pl.multiple_of(i * 32, 32), 32)
        normed[rows, :] = norm_rows(x2[rows, :], gain_m)
        return carry

    lax.fori_loop(0, 4, norm_x2, 0)
    load_g.wait()
    load_u.wait()

    def mlp_cols(i, carry):
        cols = pl.ds(pl.multiple_of(i * 256, 256), 256)
        gate = dot32(normed[...], buf_b[:, cols])
        up = dot32(normed[...], buf_c[:, cols])
        mid[:, cols] = (gate * (1.0 / (1.0 + jnp.exp(-gate))) * up).astype(BF16)
        return carry

    lax.fori_loop(0, FF // 256, mlp_cols, 0)
    load_d.wait()

    def down_cols(i):
        def body(t, carry):
            cols = pl.ds(pl.multiple_of(i * QW + t * 256, 256), 256)
            part[:, cols] = dot32(mid[...], buf_a[:, cols])
            return carry
        lax.fori_loop(0, QW // 256, body, 0)

    reduce_all(1, down_cols, keep_late, lambda: None, x2, hid)
    for kind in range(3):
        for tn in range(2):
            for j in range(NCH if kind == 0 else LATE):
                if kind or tn:
                    kv_send(kind, tn, j).wait_send()
    for i in range(N_LATE):
        late_send(i).wait_send()
    for i in range(N_LATE - N_MID, N_LATE):
        late_send(i).wait_recv()
    for h in range(2):
        rb_send(h).wait_send()
    q_msg.wait_send()
    p_msg.wait_send()


def copy_out(kv, knv, hid, k_out, v_out, last_out, dec_out, buf, sem, row_sem):
    rows = [pltpu.make_async_copy(hid.at[pl.ds(i * NB, NB)], dst, row_sem.at[i]) for i, dst in enumerate((last_out, dec_out))]
    for r in rows:
        r.start()

    def store(h, g):
        dst = pl.ds(pl.multiple_of(g * 2064, 2064), 2064)
        slot = lax.rem(g, 2)
        return pltpu.make_async_copy(buf.at[h, slot, pl.ds(0, 2064)], (k_out, v_out)[h].at[dst], sem.at[h, slot])

    def lay_out(g, carry):
        slot = lax.rem(g, 2)
        for h in range(2):
            @pl.when(g > 1)
            def _():
                store(h, g - 2).wait()
            for t in range(8):
                buf[h, slot, t * 258:t * 258 + 256, :] = kv[h, g * 8 + t]
            new = knv[h, pl.ds(pl.multiple_of(g * 16, 16), 16), :]
            for t in range(8):
                buf[h, slot, t * 258 + 256:t * 258 + 258, :] = new[2 * t:2 * t + 2]
            store(h, g).start()
        return carry

    lax.fori_loop(0, NB // 8, lay_out, 0)
    for g in range(NB // 8 - 2, NB // 8):
        for h in range(2):
            store(h, g).wait()
    for r in rows:
        r.wait()


def solution(mesh):
    seq_spec = P('replica', 'model', None)
    col_spec = P(None, None, 'model')
    row_spec = P(None, 'model', None)
    gain_spec = P(None, None)
    tok_spec = P('replica', None)
    cache_spec = P(None, 'replica', None, 'model', None)
    in_specs = (seq_spec, P('replica'), tok_spec, gain_spec, col_spec, col_spec, col_spec, row_spec, gain_spec, col_spec, col_spec, row_spec)
    out_specs = (tok_spec, tok_spec, cache_spec, cache_spec)

    def per_device(prompt, lengths, new_tok, norm_attn, w_q, w_k, w_v, w_o, norm_mlp, w_gate, w_up, w_down):
        tab = jnp.asarray(rotate_tables(136))
        vmem = pl.BlockSpec(memory_space=pltpu.VMEM)
        hbm = pl.BlockSpec(memory_space=pl.ANY)
        smem = pl.BlockSpec(memory_space=pltpu.SMEM)
        dma = pltpu.SemaphoreType.DMA
        kv, knv, hid = pl.pallas_call(
            kernel,
            out_shape=(pltpu.VMEM((2, NB, 256, HEAD_DIM), BF16), pltpu.VMEM((2, 2 * NB, HEAD_DIM), BF16), pltpu.VMEM((2 * NB, D), BF16)),
            in_specs=[smem] + [hbm] * 12,
            out_specs=(vmem,) * 3,
            scratch_shapes=[
                pltpu.VMEM((NB * SEQ_LOC, D), BF16),
                pltpu.VMEM((D, FF), BF16),
                pltpu.VMEM((D, FF), BF16),
                pltpu.VMEM((2, 2, NCH, CH, 64, HEAD_DIM), BF16),
                pltpu.VMEM((NCH, CH, 64, HEAD_DIM), BF16),
                pltpu.VMEM((2 * ROWS, HEAD_DIM), F32),
                pltpu.VMEM((NB * 16, HEAD_DIM), F32),
                pltpu.VMEM((NB * 16, HEAD_DIM), F32),
                pltpu.VMEM((NB * 16, HEAD_DIM), F32),
                pltpu.VMEM((NB * 16, HEAD_DIM), F32),
                pltpu.VMEM((2 * NB, QW), BF16),
                pltpu.VMEM((NB, D), BF16),
                pltpu.VMEM((32, D), BF16),
                pltpu.VMEM((2 * NB, D), BF16),
                pltpu.VMEM((2 * NB, D), F32),
                pltpu.VMEM((NB, D), F32),
                pltpu.VMEM((32, D), F32),
                pltpu.VMEM((2 * NB, D), BF16),
                pltpu.VMEM((2 * NB, FF), BF16),
                pltpu.VMEM((NB * 16, 256), BF16),
                pltpu.VMEM((2, 2 * NB, HEAD_DIM), F32),
                pltpu.VMEM((2, 136, HEAD_DIM), F32),
                pltpu.VMEM((1, D), BF16),
                pltpu.VMEM((1, D), BF16),
                pltpu.VMEM((2, CH, 128, HEAD_DIM), BF16),
                pltpu.VMEM((CH * 16, HEAD_DIM), BF16),
                pltpu.VMEM((CH * 16, HEAD_DIM), BF16),
                pltpu.VMEM((CH * 16, HEAD_DIM), F32),
                pltpu.VMEM((CH * 16, HEAD_DIM), F32),
                pltpu.VMEM((CH * 16, HEAD_DIM), F32),
                pltpu.VMEM((CH * 16, HEAD_DIM), F32),
                dma((NCH,)), dma((2,)), dma((9,)), dma((3,)),
                dma, dma, dma((WCH,)), dma((WCH,)), dma((WCH,)), dma((WCH,)),
                dma((WCH,)), dma((WCH,)), dma((WCH,)), dma((WCH,)),
                dma((3,)), dma((3,)), dma((3, 2, NCH)), dma((3, 2, NCH)), dma((2, 5, 4)), dma((2, 5, 4)),
                dma((2,)), dma((2,)), dma((N_LATE,)), dma((N_LATE,)), dma((2,)), dma((2,)),
            ],
            compiler_params=pltpu.CompilerParams(collective_id=0, has_side_effects=True, vmem_limit_bytes=VMEM_LAYER),
            name="layer",
        )(lengths, tab, norm_attn, norm_mlp, new_tok,
          prompt.reshape(NB * SEQ_LOC, D), w_q[0], w_k[0], w_v[0], w_o[0], w_gate[0], w_up[0], w_down[0])
        rows, slots = jax.ShapeDtypeStruct((NB, D), BF16), jax.ShapeDtypeStruct((NB * 258, HEAD_DIM), BF16)
        o_k, o_v, o_last, o_dec = pl.pallas_call(
            copy_out,
            out_shape=(slots, slots, rows, rows),
            in_specs=[vmem] * 3,
            out_specs=(hbm,) * 4,
            scratch_shapes=[pltpu.VMEM((2, 2, 8 * 258 + 32, HEAD_DIM), BF16), dma((2, 2)), dma((2,))],
            compiler_params=pltpu.CompilerParams(vmem_limit_bytes=40 << 20),
            name="copy_out",
        )(kv, knv, hid)
        caches = [o.reshape(1, NB, 129, 2, HEAD_DIM) for o in (o_k, o_v)]
        return o_dec, o_last, caches[0], caches[1]

    return jax.shard_map(per_device, mesh=mesh, in_specs=in_specs, out_specs=out_specs, check_vma=False)
```

```python
import functools

import jax
import jax.numpy as jnp
import numpy as np
from jax import lax
from jax.experimental import pallas as pl
from jax.experimental.pallas import tpu as pltpu
from jax.sharding import PartitionSpec as P

HEAD_DIM = 128
NEG_BIG = -1e30
MESH = pl.DeviceIdType.MESH
F32 = jnp.float32
BF16 = jnp.bfloat16

NB = 64
SEQ_LOC = 32
D = 3072
FF = 2048
QW = 768
CH = 16
NCH = NB // CH
ROWS = CH * SEQ_LOC
VMEM_LAYER = 67043328 - (10 << 20)
LATE = NCH - 1
N_EARLY = 1
N_LATE = 16
N_GAP = 4
N_MID = 0
N_FIRST = 4 * N_EARLY + N_GAP
WCH = 4
WROWS = D // WCH


def dot32(lhs, rhs):
    return jnp.dot(lhs, rhs, preferred_element_type=F32)


def rotate_tables(n):
    half = HEAD_DIM // 2
    inv_freq = np.float32(10000.0) ** (np.float32(-2.0) * np.arange(half, dtype=np.float32) / np.float32(HEAD_DIM))
    angles = (np.arange(n, dtype=np.float32)[:, None] * inv_freq).astype(np.float32).astype(np.float64)
    cos_tab, sin_tab = np.cos(angles), np.sin(angles)
    return np.stack([np.concatenate([cos_tab, cos_tab], 1), np.concatenate([-sin_tab, sin_tab], 1)]).astype(np.float32)


def kernel(lens, tab_in, g_attn_in, g_mlp_in,
           new_tok, prompt, w_q, w_k, w_v, w_o, w_g, w_u, w_d,
           kv, knv, hid,
           buf_a, buf_b, buf_c, stage, stage_p, flat, q_buf, k_buf, v_buf, a_buf, att,
           sel_r1, sel_r2, normed, part, r1, r2, x2, mid, p_buf, rot,
           tab, g_attn, g_mlp, rb, qb, qb_r, m_buf, l_buf, pb, pb_r,
           ld_p, ld_w, ld_big, ld_small,
           wp_s, wp_r, wx_s, wx_r, wfx_s, wfx_r, wy_s, wy_r, wfy_s, wfy_r,
           sel_s, sel_r, kv_s, kv_r, ar_s, ar_r, rb_s, rb_r, late_s, late_r, qp_s, qp_r):
    y = lax.axis_index("replica")
    m = lax.axis_index("model")
    c = lax.rem(m, 2)
    x = m // 2
    xs_m = lax.rem(m + 2, 4)
    xo_m = 3 - m
    pt_m = m + 1 - 2 * c
    xs, xo, pt, yp = (y, xs_m), (y, xo_m), (y, pt_m), (1 - y, m)

    def remote(src, dst, ssem, rsem, dev):
        return pltpu.make_async_remote_copy(src_ref=src, dst_ref=dst, send_sem=ssem, recv_sem=rsem,
                                            device_id=dev, device_id_type=MESH)

    def load_w(i):
        src = (w_k, w_v)[i]
        return pltpu.make_async_copy(src, buf_b.at[:, pl.ds(pl.multiple_of(m * 512 + i * 256, 256), 256)], ld_w.at[i])

    def load_p(j):
        r = pl.ds(pl.multiple_of(j * ROWS, ROWS), ROWS)
        return pltpu.make_async_copy(prompt.at[r], buf_a.at[r], ld_p.at[j])

    for i in range(2):
        load_w(i).start()
    for j in range(NCH):
        load_p(j).start()
    load_q = pltpu.make_async_copy(w_q, buf_c.at[:, pl.ds(0, QW)], ld_big.at[0])
    load_q.start()
    load_t = pltpu.make_async_copy(new_tok, hid.at[pl.ds(NB, NB)], ld_big.at[8])
    load_t.start()
    small = [pltpu.make_async_copy(src, dst, ld_small.at[i])
             for i, (src, dst) in enumerate(((tab_in, tab), (g_attn_in, g_attn), (g_mlp_in, g_mlp)))]
    for cp in small:
        cp.start()

    def load_o(i):
        return pltpu.make_async_copy(w_o.at[:, pl.ds(i * QW, QW)], buf_c.at[pl.ds(i * QW, QW), pl.ds(QW, QW)], ld_big.at[1 + i])

    for i in range(4):
        load_o(i).start()
    load_g = pltpu.make_async_copy(w_g, buf_b, ld_big.at[5])
    load_u = pltpu.make_async_copy(w_u, buf_c, ld_big.at[6])
    load_d = pltpu.make_async_copy(w_d, buf_a, ld_big.at[7])

    barrier = pltpu.get_barrier_semaphore()
    for dev in (xs, xo, pt, yp):
        pl.semaphore_signal(barrier, inc=1, device_id=dev, device_id_type=MESH)
    pl.semaphore_wait(barrier, 4)

    def w_ref(owner, half, r):
        rows = pl.ds(pl.multiple_of(half * (D // 2) + (r % 2) * WROWS, WROWS), WROWS)
        return buf_b.at[rows, pl.ds(pl.multiple_of(owner * 512 + (r // 2) * 256, 256), 256)]

    def wx(r):
        src = (w_k, w_v)[r // 2].at[pl.ds(pl.multiple_of(y * (D // 2) + (r % 2) * WROWS, WROWS), WROWS)]
        return remote(src, w_ref(m, y, r), wx_s.at[r], wx_r.at[r], xs)

    def wfx(r):
        ref = w_ref(xs_m, y, r)
        return remote(ref, ref, wfx_s.at[r], wfx_r.at[r], pt)

    def wy(r):
        ref = w_ref(xs_m, y, r)
        return remote(ref, ref, wy_s.at[r], wy_r.at[r], yp)

    def wfy(r):
        ref = w_ref(xs_m, 1 - y, r)
        return remote(ref, ref, wfy_s.at[r], wfy_r.at[r], pt)

    own = buf_b.at[:, pl.ds(pl.multiple_of(m * 512, 512), 512)]
    wp = remote(own, own, wp_s, wp_r, pt)
    for r in range(WCH):
        wx(r).start()
    for i in range(2):
        load_w(i).wait()
    wp.start()

    def forward_x(r):
        wx(r).wait_recv()
        wfx(r).start()
        wy(r).start()

    def forward_y(r):
        wy(r).wait_recv()
        wfy(r).start()

    for cp in small:
        cp.wait()
    gain_a = g_attn[...].astype(F32)
    row_iota = lax.broadcasted_iota(jnp.int32, (SEQ_LOC, 1), 0)

    def norm_prompts(i, carry):
        parts = []
        for t in range(8):
            b = i * 8 + t
            rows = pl.ds(pl.multiple_of(b * SEQ_LOC, SEQ_LOC), SEQ_LOC)
            v = buf_a[rows, :].astype(F32)
            inv = lax.rsqrt(jnp.mean(v * v, axis=-1, keepdims=True) + 1e-5)
            hit = row_iota == lens[b] - 1 - m * SEQ_LOC
            parts.append(jnp.sum(jnp.where(hit, v, 0.0), axis=0, keepdims=True))
            buf_a[rows, :] = (buf_a[rows, :].astype(F32) * inv * gain_a).astype(BF16)
        part[pl.ds(pl.multiple_of(i * 8, 8), 8), :] = jnp.concatenate(parts, axis=0)
        return carry

    per = CH // 8
    for j in range(NCH):
        load_p(j).wait()
        lax.fori_loop(j * per, (j + 1) * per, norm_prompts, 0)

    sel_b = normed.at[pl.ds(0, NB)]
    sel_b[...] = part[0:NB, :].astype(BF16)
    s1 = remote(sel_b, sel_r1, sel_s.at[0], sel_r.at[0], pt)
    s1.start()

    def unit_chunk(owner, h, j):
        col = pl.ds(pl.multiple_of(owner * 512 + h * 256, 256), 256)
        acc = dot32(buf_a[pl.ds(pl.multiple_of(j * ROWS, ROWS), ROWS), :], buf_b[:, col])
        here = pl.ds(pl.multiple_of(m * SEQ_LOC, SEQ_LOC), SEQ_LOC)
        for hd in range(2):
            a = acc[:, hd * HEAD_DIM:(hd + 1) * HEAD_DIM]
            if h == 0:
                turned = pltpu.roll(a, HEAD_DIM // 2, 1).reshape(CH, SEQ_LOC, HEAD_DIM)
                a = a.reshape(CH, SEQ_LOC, HEAD_DIM) * tab[0, here, :][None] + turned * tab[1, here, :][None]
                a = a.reshape(ROWS, HEAD_DIM)
            flat[pl.ds(hd, ROWS, stride=2), :] = a
        return flat[...].astype(BF16).reshape(CH, 2 * SEQ_LOC, HEAD_DIM)

    def kv_ref(h, j):
        return kv.at[h, pl.ds(pl.multiple_of(j * CH, CH), CH), pl.ds(pl.multiple_of(m * 64, 64), 64)]

    def kv_send(kind, h, j):
        dev = (pt, xs, xo)[kind]
        return remote(stage_p.at[j] if kind == 0 else stage.at[kind - 1, h, j], kv_ref(h, j), kv_s.at[kind, h, j], kv_r.at[kind, h, j], dev)

    def late_send(i):
        kind, h, first = 1 + i % 2, (i // 2) % 2, i // 4 * 4
        src = stage.at[kind - 1, h, LATE, pl.ds(first, 4)]
        dst = kv.at[h, pl.ds(LATE * CH + first, 4), pl.ds(pl.multiple_of(m * 64, 64), 64)]
        return remote(src, dst, late_s.at[i], late_r.at[i], (xs, xo)[i % 2])

    my_rb = pl.ds(pl.multiple_of(c * 64, 64), 64)

    def rb_send(h):
        return remote(stage.at[1, h, LATE], rb.at[h, :, my_rb], rb_s.at[h], rb_r.at[h], pt)

    def late_unit(h):
        chunk = unit_chunk(xs_m, h, LATE)
        stage[0, h, LATE] = chunk
        rb[h, :, my_rb] = chunk
        stage[1, h, LATE] = unit_chunk(xo_m, h, LATE)
        rb_send(h).start()
        for t in range(N_EARLY):
            for i in range(2):
                late_send(4 * t + 2 * h + i).start()

    def run_unit(kind, h, j):
        owner = (pt_m, xs_m, xo_m)[kind]
        chunk = unit_chunk(owner, h, j)
        if kind == 0:
            if h == 1:
                kv_send(0, 0, j).wait_send()
            stage_p[j] = chunk
        else:
            stage[kind - 1, h, j] = chunk
        kv_send(kind, h, j).start()

    def own_unit(h):
        def body(j, carry):
            kv[h, pl.ds(pl.multiple_of(j * CH, CH), CH), pl.ds(pl.multiple_of(m * 64, 64), 64)] = unit_chunk(m, h, j)
            return carry
        lax.fori_loop(0, NCH, body, 0)

    def loop_unit(kind, h):
        def body(j, carry):
            run_unit(kind, h, j)
            return carry
        lax.fori_loop(0, NCH if kind == 0 else LATE, body, 0)

    forward_x(0)
    own_unit(0)
    s1.wait()
    sel_b[...] = (sel_b[...].astype(F32) + sel_r1[...].astype(F32)).astype(BF16)
    half = pl.ds(pl.multiple_of(c * 32, 32), 32)
    s2 = remote(normed.at[half], sel_r2, sel_s.at[1], sel_r.at[1], xs)
    s2.start()
    own_unit(1)
    forward_x(1)
    forward_y(0)
    wp.wait_recv()
    loop_unit(0, 0)
    forward_x(2)
    forward_y(1)
    loop_unit(1, 0)
    for r in range(2):
        wfx(r).wait_recv()
        wfy(r).wait_recv()
    loop_unit(2, 0)
    late_unit(0)
    forward_x(3)
    forward_y(2)
    loop_unit(0, 1)

    s2.wait()
    hid[half, :] = (normed[half, :].astype(F32) + sel_r2[...].astype(F32)).astype(BF16)
    s3 = remote(hid.at[half], hid.at[half], sel_s.at[2], sel_r.at[2], pt)
    s3.start()
    forward_y(3)
    s3.wait()
    load_t.wait()

    def norm_rows(src, gain):
        v = src.astype(F32)
        inv = lax.rsqrt(jnp.mean(v * v, axis=-1, keepdims=True) + 1e-5)
        return (v * inv * gain).astype(BF16)

    def norm_hid(i, carry):
        rows = pl.ds(pl.multiple_of(i * 32, 32), 32)
        normed[rows, :] = norm_rows(hid[rows, :], gain_a)
        return carry

    lax.fori_loop(0, 4, norm_hid, 0)
    load_q.wait()
    q_buf[...] = jnp.zeros_like(q_buf)
    k_buf[...] = jnp.zeros_like(k_buf)
    v_buf[...] = jnp.zeros_like(v_buf)

    def pick(b, carry):
        pos = jnp.clip(lens[b], 1, 128)
        for i in range(2):
            rot[i, pl.ds(b, 1), :] = tab[i, pl.ds(pos - 1, 1), :]
            rot[i, pl.ds(NB + b, 1), :] = tab[i, pl.ds(pos, 1), :]
        return carry

    lax.fori_loop(0, NB, pick, 0)

    def turn(a, ct, st):
        return (a * ct + pltpu.roll(a, HEAD_DIM // 2, 1) * st).astype(BF16).astype(F32)

    for pair in range(3):
        qs = dot32(normed[...], buf_c[:, pair * 256:(pair + 1) * 256])
        for i in range(2):
            hd = pair * 2 + i
            q_h = turn(qs[:, i * HEAD_DIM:(i + 1) * HEAD_DIM], rot[0], rot[1])
            for t in range(2):
                q_buf[pl.ds(t * 8 + hd, NB, stride=16), :] = q_h[t * NB:(t + 1) * NB]
    toks = normed[NB:2 * NB, :]
    k_new = dot32(toks, buf_b[:, pl.ds(pl.multiple_of(m * 512, 256), 256)])
    v_new = dot32(toks, buf_b[:, pl.ds(pl.multiple_of(m * 512 + 256, 256), 256)])
    for g in range(2):
        cols = slice(g * HEAD_DIM, (g + 1) * HEAD_DIM)
        k_g = turn(k_new[:, cols], rot[0, NB:, :], rot[1, NB:, :])
        v_g = v_new[:, cols].astype(BF16).astype(F32)
        flat[pl.ds(g, NB, stride=2), :] = k_g
        flat[pl.ds(2 * NB + g, NB, stride=2), :] = v_g
        for i in range(3):
            rows = pl.ds(8 + 3 * g + i, NB, stride=16)
            k_buf[rows, :] = k_g
            v_buf[rows, :] = v_g
    knv[0] = flat[0:2 * NB, :].astype(BF16)
    knv[1] = flat[2 * NB:4 * NB, :].astype(BF16)

    qb[...] = q_buf[LATE * CH * 16:, :].astype(BF16)
    late_rows = pl.ds(N_EARLY * 64, CH * 16 - N_EARLY * 64)
    q_msg = remote(qb.at[late_rows], qb_r.at[late_rows], qp_s.at[0], qp_r.at[0], xs)
    q_msg.start()

    for r in range(2, WCH):
        wfx(r).wait_recv()
        wfy(r).wait_recv()

    def last_units(j, carry):
        run_unit(1, 1, j)
        run_unit(2, 1, j)
        return carry

    lax.fori_loop(0, LATE, last_units, 0)
    late_unit(1)
    wp.wait_send()
    for r in range(WCH):
        wx(r).wait_send()
        wfx(r).wait_send()
        wy(r).wait_send()
        wfy(r).wait_send()
    load_g.start()
    load_d.start()

    r_io = lax.broadcasted_iota(jnp.int32, (16, 256), 0)
    c_io = lax.broadcasted_iota(jnp.int32, (16, 256), 1)
    same = ((r_io & 7) >= 3) == ((c_io & 1) == 1)
    k_pos = c_io >> 1
    is_new = lax.broadcasted_iota(jnp.int32, (16, 1), 0) >= 8
    scale = HEAD_DIM ** -0.5

    def score(b):
        rows = pl.ds(pl.multiple_of(b * 16, 16), 16)
        q = q_buf[rows, :]
        s = lax.dot_general(q.astype(BF16), kv[0, b], (((1,), (1,)), ((), ())), preferred_element_type=F32) * scale
        s = jnp.where(same & (k_pos < lens[b]), s, NEG_BIG)
        s_new = jnp.where(is_new, jnp.sum(q * k_buf[rows, :], axis=-1, keepdims=True) * scale, NEG_BIG)
        top = jnp.maximum(jnp.max(s, axis=-1, keepdims=True), s_new)
        p = jnp.exp(s - top)
        p_new = jnp.exp(s_new - top)
        inv = 1.0 / (jnp.sum(p, axis=-1, keepdims=True) + p_new)
        p_buf[rows, :] = (p * inv).astype(BF16)
        a_buf[rows, :] = (p_new * inv) * v_buf[rows, :]

    def score_four(i, carry):
        for t in range(4):
            score(i * 4 + t)
        return carry

    def weigh(b):
        rows = pl.ds(pl.multiple_of(b * 16, 16), 16)
        a_buf[rows, :] = a_buf[rows, :] + dot32(p_buf[rows, :], kv[1, b])

    def weigh_eight(i, carry):
        for t in range(8):
            weigh(i * 8 + t)
        return carry

    c_half = lax.broadcasted_iota(jnp.int32, (16, 128), 1)
    r_half = lax.broadcasted_iota(jnp.int32, (16, 128), 0)
    same_half = ((r_half & 7) >= 3) == ((c_half & 1) == 1)
    pos_half = x * 64 + (c_half >> 1)
    on_diag = c_half == r_half
    chip_rows = pl.ds(pl.multiple_of(x * 128, 128), 128)

    def partial_scores(q, keys, b):
        s = lax.dot_general(q, keys, (((1,), (1,)), ((), ())), preferred_element_type=F32) * scale
        return jnp.where(same_half & (pos_half < lens[b]), s, NEG_BIG)

    def late_local(p):
        b = LATE * CH + p
        rows = pl.ds(pl.multiple_of(b * 16, 16), 16)
        out = pl.ds(pl.multiple_of(p * 16, 16), 16)
        q = q_buf[rows, :]
        s = partial_scores(q.astype(BF16), kv[0, b, chip_rows, :], b)
        s_new = jnp.where(is_new, jnp.sum(q * k_buf[rows, :], axis=-1, keepdims=True) * scale, NEG_BIG)
        top = jnp.maximum(jnp.max(s, axis=-1, keepdims=True), s_new)
        w = jnp.exp(s - top)
        w_new = jnp.exp(s_new - top)
        m_buf[out, :] = jnp.broadcast_to(top, (16, HEAD_DIM))
        l_buf[out, :] = jnp.broadcast_to(jnp.sum(w, axis=-1, keepdims=True) + w_new, (16, HEAD_DIM))
        a_buf[rows, :] = dot32(w.astype(BF16), kv[1, b, chip_rows, :]) + w_new * v_buf[rows, :]

    def late_peer(p):
        out = pl.ds(pl.multiple_of(p * 16, 16), 16)
        s = partial_scores(qb_r[out, :], rb[0, p], LATE * CH + p)
        top = jnp.max(s, axis=-1, keepdims=True)
        w = jnp.exp(s - top)
        acc = dot32(w.astype(BF16), rb[1, p])
        tops = jnp.sum(jnp.where(on_diag, top, 0.0), axis=0, keepdims=True)
        sums = jnp.sum(jnp.where(on_diag, jnp.sum(w, axis=-1, keepdims=True), 0.0), axis=0, keepdims=True)
        pb[out, :] = jnp.where(r_half == 6, tops, jnp.where(r_half == 7, sums, acc))

    def late_merge(p):
        rows = pl.ds(pl.multiple_of((LATE * CH + p) * 16, 16), 16)
        out = pl.ds(pl.multiple_of(p * 16, 16), 16)
        other = pb_r[out, :]
        o_top = jnp.sum(jnp.where(on_diag, other[6:7, :], 0.0), axis=-1, keepdims=True)
        o_sum = jnp.sum(jnp.where(on_diag, other[7:8, :], 0.0), axis=-1, keepdims=True)
        top = jnp.maximum(m_buf[out, :], o_top)
        w, o_w = jnp.exp(m_buf[out, :] - top), jnp.exp(o_top - top)
        a_buf[rows, :] = (a_buf[rows, :] * w + other * o_w) / (l_buf[out, :] * w + o_sum * o_w)

    def by_four(f):
        def body(i, carry):
            for t in range(4):
                f(i * 4 + t)
            return carry
        lax.fori_loop(N_EARLY, CH // 4, body, 0)

    for j in range(LATE):
        for kind in range(3):
            kv_send(kind, 0, j).wait_recv()
        lax.fori_loop(j * (CH // 4), (j + 1) * (CH // 4), score_four, 0)
    for h in range(2):
        kv_send(0, h, LATE).wait_recv()
        rb_send(h).wait_recv()
    for t in range(N_EARLY):
        for i in range(2):
            late_send(4 * t + i).wait_recv()
        score_four(LATE * (CH // 4) + t, 0)
    by_four(late_local)
    q_msg.wait_recv()
    by_four(late_peer)
    p_msg = remote(pb.at[late_rows], pb_r.at[late_rows], qp_s.at[1], qp_r.at[1], xs)
    p_msg.start()
    for i in range(4 * N_EARLY, N_FIRST):
        late_send(i).start()

    for j in range(LATE):
        for kind in range(3):
            kv_send(kind, 1, j).wait_recv()
        lax.fori_loop(j * (CH // 8), (j + 1) * (CH // 8), weigh_eight, 0)
    for t in range(N_EARLY):
        for i in range(2):
            late_send(4 * t + 2 + i).wait_recv()
        for b in range(LATE * CH + 4 * t, LATE * CH + 4 * t + 4):
            weigh(b)
    p_msg.wait_recv()
    by_four(late_merge)

    for hd in range(6):
        for t in range(2):
            att[t * NB:(t + 1) * NB, hd * HEAD_DIM:(hd + 1) * HEAD_DIM] = a_buf[pl.ds(t * 8 + hd, NB, stride=16), :].astype(BF16)
    ot_half = pl.ds(pl.multiple_of((1 - c) * 64, 64), 64)
    mine = pl.ds(pl.multiple_of(c * 64 + x * 32, 32), 32)
    away = pl.ds(pl.multiple_of(c * 64 + (1 - x) * 32, 32), 32)
    mine_r1 = pl.ds(pl.multiple_of(x * 32, 32), 32)
    away_r1 = pl.ds(pl.multiple_of((1 - x) * 32, 32), 32)

    def reduce_all(k, produce, after, last, resid, buf):
        def msg(step, i, src, dst, dev):
            return remote(src, dst, ar_s.at[k, step, i], ar_r.at[k, step, i], dev)

        cols = [pl.ds(i * QW, QW) for i in range(4)]
        a1 = [msg(0, i, part.at[ot_half, cols[i]], r1.at[:, cols[i]], pt) for i in range(4)]
        a2 = [msg(1, i, part.at[away, cols[i]], r2.at[:, cols[i]], xs) for i in range(4)]
        a3 = [msg(2, i, buf.at[mine, cols[i]], buf.at[mine, cols[i]], xs) for i in range(4)]
        a4 = [msg(3, i, buf.at[mine, cols[i]], buf.at[mine, cols[i]], pt) for i in range(4)]
        a5 = [msg(4, i, buf.at[away, cols[i]], buf.at[away, cols[i]], pt) for i in range(4)]

        def over_x(i):
            a1[i].wait_recv()
            part[away, cols[i]] = part[away, cols[i]] + r1[away_r1, cols[i]]
            a2[i].start()
            part[mine, cols[i]] = part[mine, cols[i]] + r1[mine_r1, cols[i]]

        for i in range(4):
            produce(i)
            a1[i].start()
            if i:
                over_x(i - 1)
        over_x(3)
        after()
        for i in range(4):
            if i == 3:
                for t in range(N_MID):
                    late_send((N_FIRST, N_LATE - N_MID)[k] + t).start()
            a2[i].wait_recv()
            total = part[mine, cols[i]] + r2[:, cols[i]]
            buf[mine, cols[i]] = (resid[mine, cols[i]].astype(F32) + total).astype(BF16)
            a3[i].start()
            a4[i].start()
        last()
        for i in range(4):
            a3[i].wait_recv()
            a5[i].start()
        for i in range(4):
            a4[i].wait_recv()
            a5[i].wait_recv()
        for step in (a1, a2, a3, a4, a5):
            for i in range(4):
                step[i].wait_send()

    def w_o_cols(i):
        load_o(i).wait()
        part[:, i * QW:(i + 1) * QW] = dot32(att[...], buf_c[i * QW:(i + 1) * QW, QW:2 * QW])

    def after_w_o():
        load_u.start()

    def send_late():
        for i in range(N_FIRST + N_MID, N_LATE - N_MID):
            late_send(i).start()

    def keep_late():
        for i in range(4 * N_EARLY, N_LATE - N_MID):
            late_send(i).wait_recv()

    reduce_all(0, w_o_cols, after_w_o, send_late, hid, x2)
    gain_m = g_mlp[...].astype(F32)

    def norm_x2(i, carry):
        rows = pl.ds(pl.multiple_of(i * 32, 32), 32)
        normed[rows, :] = norm_rows(x2[rows, :], gain_m)
        return carry

    lax.fori_loop(0, 4, norm_x2, 0)
    load_g.wait()
    load_u.wait()

    def mlp_cols(i, carry):
        cols = pl.ds(pl.multiple_of(i * 256, 256), 256)
        gate = dot32(normed[...], buf_b[:, cols])
        up = dot32(normed[...], buf_c[:, cols])
        mid[:, cols] = (gate * (1.0 / (1.0 + jnp.exp(-gate))) * up).astype(BF16)
        return carry

    lax.fori_loop(0, FF // 256, mlp_cols, 0)
    load_d.wait()

    def down_cols(i):
        def body(t, carry):
            cols = pl.ds(pl.multiple_of(i * QW + t * 256, 256), 256)
            part[:, cols] = dot32(mid[...], buf_a[:, cols])
            return carry
        lax.fori_loop(0, QW // 256, body, 0)

    reduce_all(1, down_cols, keep_late, lambda: None, x2, hid)
    for kind in range(3):
        for tn in range(2):
            for j in range(NCH if kind == 0 else LATE):
                if kind or tn:
                    kv_send(kind, tn, j).wait_send()
    for i in range(N_LATE):
        late_send(i).wait_send()
    for i in range(N_LATE - N_MID, N_LATE):
        late_send(i).wait_recv()
    for h in range(2):
        rb_send(h).wait_send()
    q_msg.wait_send()
    p_msg.wait_send()


def copy_out(kv, knv, hid, k_out, v_out, last_out, dec_out, buf, sem, row_sem):
    rows = [pltpu.make_async_copy(hid.at[pl.ds(i * NB, NB)], dst, row_sem.at[i]) for i, dst in enumerate((last_out, dec_out))]
    for r in rows:
        r.start()

    def store(h, g):
        dst = pl.ds(pl.multiple_of(g * 1032, 8), 1032)
        slot = lax.rem(g, 4)
        return pltpu.make_async_copy(buf.at[h, slot, pl.ds(0, 1032)], (k_out, v_out)[h].at[dst], sem.at[h, slot])

    def lay_out(g, carry):
        slot = lax.rem(g, 4)
        for h in range(2):
            @pl.when(g > 3)
            def _():
                store(h, g - 4).wait()
            for t in range(4):
                buf[h, slot, t * 258:t * 258 + 256, :] = kv[h, g * 4 + t]
            new = knv[h, pl.ds(pl.multiple_of(g * 8, 8), 8), :]
            for t in range(4):
                buf[h, slot, t * 258 + 256:t * 258 + 258, :] = new[2 * t:2 * t + 2]
            store(h, g).start()
        return carry

    lax.fori_loop(0, NB // 4, lay_out, 0)
    for g in range(NB // 4 - 4, NB // 4):
        for h in range(2):
            store(h, g).wait()
    for r in rows:
        r.wait()


def solution(mesh):
    seq_spec = P('replica', 'model', None)
    col_spec = P(None, None, 'model')
    row_spec = P(None, 'model', None)
    gain_spec = P(None, None)
    tok_spec = P('replica', None)
    cache_spec = P(None, 'replica', None, 'model', None)
    in_specs = (seq_spec, P('replica'), tok_spec, gain_spec, col_spec, col_spec, col_spec, row_spec, gain_spec, col_spec, col_spec, row_spec)
    out_specs = (tok_spec, tok_spec, cache_spec, cache_spec)

    def per_device(prompt, lengths, new_tok, norm_attn, w_q, w_k, w_v, w_o, norm_mlp, w_gate, w_up, w_down):
        tab = jnp.asarray(rotate_tables(136))
        vmem = pl.BlockSpec(memory_space=pltpu.VMEM)
        hbm = pl.BlockSpec(memory_space=pl.ANY)
        smem = pl.BlockSpec(memory_space=pltpu.SMEM)
        dma = pltpu.SemaphoreType.DMA
        kv, knv, hid = pl.pallas_call(
            kernel,
            out_shape=(pltpu.VMEM((2, NB, 256, HEAD_DIM), BF16), pltpu.VMEM((2, 2 * NB, HEAD_DIM), BF16), pltpu.VMEM((2 * NB, D), BF16)),
            in_specs=[smem] + [hbm] * 12,
            out_specs=(vmem,) * 3,
            scratch_shapes=[
                pltpu.VMEM((NB * SEQ_LOC, D), BF16),
                pltpu.VMEM((D, FF), BF16),
                pltpu.VMEM((D, FF), BF16),
                pltpu.VMEM((2, 2, NCH, CH, 64, HEAD_DIM), BF16),
                pltpu.VMEM((NCH, CH, 64, HEAD_DIM), BF16),
                pltpu.VMEM((2 * ROWS, HEAD_DIM), F32),
                pltpu.VMEM((NB * 16, HEAD_DIM), F32),
                pltpu.VMEM((NB * 16, HEAD_DIM), F32),
                pltpu.VMEM((NB * 16, HEAD_DIM), F32),
                pltpu.VMEM((NB * 16, HEAD_DIM), F32),
                pltpu.VMEM((2 * NB, QW), BF16),
                pltpu.VMEM((NB, D), BF16),
                pltpu.VMEM((32, D), BF16),
                pltpu.VMEM((2 * NB, D), BF16),
                pltpu.VMEM((2 * NB, D), F32),
                pltpu.VMEM((NB, D), F32),
                pltpu.VMEM((32, D), F32),
                pltpu.VMEM((2 * NB, D), BF16),
                pltpu.VMEM((2 * NB, FF), BF16),
                pltpu.VMEM((NB * 16, 256), BF16),
                pltpu.VMEM((2, 2 * NB, HEAD_DIM), F32),
                pltpu.VMEM((2, 136, HEAD_DIM), F32),
                pltpu.VMEM((1, D), BF16),
                pltpu.VMEM((1, D), BF16),
                pltpu.VMEM((2, CH, 128, HEAD_DIM), BF16),
                pltpu.VMEM((CH * 16, HEAD_DIM), BF16),
                pltpu.VMEM((CH * 16, HEAD_DIM), BF16),
                pltpu.VMEM((CH * 16, HEAD_DIM), F32),
                pltpu.VMEM((CH * 16, HEAD_DIM), F32),
                pltpu.VMEM((CH * 16, HEAD_DIM), F32),
                pltpu.VMEM((CH * 16, HEAD_DIM), F32),
                dma((NCH,)), dma((2,)), dma((9,)), dma((3,)),
                dma, dma, dma((WCH,)), dma((WCH,)), dma((WCH,)), dma((WCH,)),
                dma((WCH,)), dma((WCH,)), dma((WCH,)), dma((WCH,)),
                dma((3,)), dma((3,)), dma((3, 2, NCH)), dma((3, 2, NCH)), dma((2, 5, 4)), dma((2, 5, 4)),
                dma((2,)), dma((2,)), dma((N_LATE,)), dma((N_LATE,)), dma((2,)), dma((2,)),
            ],
            compiler_params=pltpu.CompilerParams(collective_id=0, has_side_effects=True, vmem_limit_bytes=VMEM_LAYER),
            name="layer",
        )(lengths, tab, norm_attn, norm_mlp, new_tok,
          prompt.reshape(NB * SEQ_LOC, D), w_q[0], w_k[0], w_v[0], w_o[0], w_gate[0], w_up[0], w_down[0])
        rows, slots = jax.ShapeDtypeStruct((NB, D), BF16), jax.ShapeDtypeStruct((NB * 258, HEAD_DIM), BF16)
        o_k, o_v, o_last, o_dec = pl.pallas_call(
            copy_out,
            out_shape=(slots, slots, rows, rows),
            in_specs=[vmem] * 3,
            out_specs=(hbm,) * 4,
            scratch_shapes=[pltpu.VMEM((2, 4, 4 * 258 + 40, HEAD_DIM), BF16), dma((2, 4)), dma((2,))],
            compiler_params=pltpu.CompilerParams(vmem_limit_bytes=40 << 20),
            name="copy_out",
        )(kv, knv, hid)
        caches = [o.reshape(1, NB, 129, 2, HEAD_DIM) for o in (o_k, o_v)]
        return o_dec, o_last, caches[0], caches[1]

    return jax.shard_map(per_device, mesh=mesh, in_specs=in_specs, out_specs=out_specs, check_vma=False)
```
